32 devices in a mesh: wt: 16 (over z, x, core), seq: 2 (over y).
Axes of the slice: x: 2, y: 2, z: 4, core: 2. Of those that a mesh axis runs over, the one named last changes fastest.
Arguments:
- tokens: bfloat16 [16, 1024, 1536], P('wt', 'seq'), may hold values from -6 to 6
- lengths: int32 [16], P('wt'), may hold values from 512 to 1024, as said below
- attn_gain: float32 [1536], P('wt'), may hold values from 0.5 to 1.5
- w_query: float32 [1536, 1536], P('wt'), may hold values from -0.15625 to 0.15625
- b_query: float32 [1536], P('wt'), may hold values from -3 to 3
- w_key: float32 [1536, 256], P('wt'), may hold values from -0.15625 to 0.15625
- b_key: float32 [256], P('wt'), may hold values from -3 to 3
- w_value: float32 [1536, 256], P('wt'), may hold values from -0.15625 to 0.15625
- b_value: float32 [256], P('wt'), may hold values from -0.6 to 0.6
- w_out: float32 [1536, 1536], P('wt'), may hold values from -0.625 to 0.625
- ffn_gain: float32 [1536], P('wt'), may hold values from 0.5 to 1.5
- w_gate: float32 [1536, 8960], P('wt'), may hold values from -0.15625 to 0.15625
- w_up: float32 [1536, 8960], P('wt'), may hold values from -0.15625 to 0.15625
- w_down: float32 [8960, 1536], P('wt'), may hold values from -0.0625 to 0.0625
- cotangent: bfloat16 [16, 1024, 1536], P('wt', 'seq'), may hold values from -6 to 6
Outputs:
- layer_out: bfloat16 [16, 1024, 1536], P('wt', 'seq')
- input_grad: bfloat16 [16, 1024, 1536], P('wt', 'seq')
- attn_gain_grad: float32 [1536], P('wt')
- w_query_grad: float32 [1536, 1536], P('wt')
- b_query_grad: float32 [1536], P('wt')
- w_key_grad: float32 [1536, 256], P('wt')
- b_key_grad: float32 [256], P('wt')
- w_value_grad: float32 [1536, 256], P('wt')
- b_value_grad: float32 [256], P('wt')
- w_out_grad: float32 [1536, 1536], P('wt')
- ffn_gain_grad: float32 [1536], P('wt')
- w_gate_grad: float32 [1536, 8960], P('wt')
- w_up_grad: float32 [1536, 8960], P('wt')
- w_down_grad: float32 [8960, 1536], P('wt')
The draws below stay inside these ranges and needn't reach their ends.
Inputs may be any that keep to these rules, and one draw needn't show every extreme that they name: `lengths`: some slot has exactly 1024 valid tokens and some exactly 512.
All inputs are finite; a program needn't handle non-finite values.
Results may differ from the reference program's by a relative error of at most 0.028.
Values may be sent and summed in bfloat16 or wider, within the bound.
A program may use at most 384 MiB of HBM per device.

```python
import math
import jax
import jax.numpy as jnp
from jax import lax

D = 1536
HEADS = 12
KV_HEADS = 2
HEAD_DIM = 128
FF = 8960
SLOT = 1024
SLOTS = 16
QW = 1536
KVW = 256


def draw_lengths(key, part):
    base_key = jax.random.fold_in(key, 11)
    draw_key, long_key, shift_key = jax.random.split(base_key, 3)
    values = jax.random.randint(draw_key, (SLOTS,), SLOT // 2, SLOT + 1)
    longest = jax.random.randint(long_key, (), 0, SLOTS)
    offset = jax.random.randint(shift_key, (), 1, SLOTS)
    shortest = (longest + offset) % SLOTS
    values = values.at[longest].set(SLOT)
    values = values.at[shortest].set(SLOT // 2)
    return values.astype(jnp.int32)


def block_levels(stream_key, shape, pieces, least, top_value):
    level, own = 1.0, jax.random.fold_in(stream_key, 6)
    for dim, parts in pieces:
        heights = jnp.exp(jax.random.uniform(jax.random.fold_in(own, dim), (parts,), jnp.float32, least / len(pieces), top_value / len(pieces)))
        level = level * jnp.repeat(heights, shape[dim] // parts).reshape([-1 if axis == dim else 1 for axis in range(len(shape))])
    return level


def normal_values(own_key, extent, width, most, shards=(), kind=jnp.bfloat16):
    level = block_levels(own_key, extent, shards, -0.22, 0.18) if shards else 1.0
    drawn = jax.random.normal(own_key, extent, jnp.float32) * width * level
    return jnp.minimum(jnp.maximum(drawn, -most), most).astype(kind)


def setup_inputs(seed: int = 0) -> dict:
    key_of = jax.random.split(jax.random.key(seed), 16)
    tokens = normal_values(key_of[0], (SLOTS, SLOT, D), 1.0, 6.0, ((0, 16), (1, 2)))
    lengths = draw_lengths(jax.random.fold_in(key_of[15], 71), 0)
    attn_gain = jnp.clip(1.0 + 0.1 * jax.random.normal(key_of[2], (D,), jnp.float32), 0.5, 1.5)
    w_query = normal_values(key_of[3], (D, QW), D ** -0.5, 0.15625, ((0, 16),), jnp.float32)
    b_query = normal_values(key_of[4], (QW,), 0.5, 3.0, ((0, 16),), jnp.float32)
    w_key = normal_values(key_of[5], (D, KVW), D ** -0.5, 0.15625, ((0, 16),), jnp.float32)
    b_key = normal_values(key_of[6], (KVW,), 0.5, 3.0, ((0, 16),), jnp.float32)
    w_value = normal_values(key_of[7], (D, KVW), D ** -0.5, 0.15625, ((0, 16),), jnp.float32)
    b_value = normal_values(key_of[8], (KVW,), 0.1, 0.6, ((0, 16),), jnp.float32)
    w_out = normal_values(key_of[9], (QW, D), (QW // 16) ** -0.5, 0.625, ((0, 16),), jnp.float32)
    ffn_gain = jnp.clip(1.0 + 0.1 * jax.random.normal(key_of[10], (D,), jnp.float32), 0.5, 1.5)
    w_gate = normal_values(key_of[11], (D, FF), D ** -0.5, 0.15625, ((0, 16),), jnp.float32)
    w_up = normal_values(key_of[12], (D, FF), D ** -0.5, 0.15625, ((0, 16),), jnp.float32)
    w_down = normal_values(key_of[13], (FF, D), FF ** -0.5, 0.0625, ((0, 16),), jnp.float32)
    cotangent = normal_values(key_of[14], (SLOTS, SLOT, D), 1.0, 6.0, ((0, 16), (1, 2)))
    return {"tokens": tokens, "lengths": lengths, "attn_gain": attn_gain, "w_query": w_query, "b_query": b_query, "w_key": w_key, "b_key": b_key, "w_value": w_value, "b_value": b_value, "w_out": w_out, "ffn_gain": ffn_gain, "w_gate": w_gate, "w_up": w_up, "w_down": w_down, "cotangent": cotangent}


epsilon = 1e-06
masked_score = -1e+30
highest = lax.Precision.HIGHEST

@jax.custom_vjp
def low(v):
    return lax.optimization_barrier(v.astype(jnp.bfloat16)).astype(jnp.float32)

@jax.custom_vjp
def low_back(v):
    return v

def low_keep(v):
    return (low(v), None)

def low_pass(kept, grad):
    return (grad,)

def back_keep(v):
    return (v, None)

def back_low(kept, grad):
    return (low(grad),)
low.defvjp(low_keep, low_pass)
low_back.defvjp(back_keep, back_low)

def product(left, right):
    return jnp.dot(left, right, precision=highest, preferred_element_type=jnp.float32)

def rms_norm(values, gain):
    return values * lax.rsqrt(lax.optimization_barrier(jnp.mean(values * values, axis=-1, keepdims=True)) + epsilon) * gain

def rope_tables(count):
    half = HEAD_DIM // 2
    inverse = 10000.0 ** (-jnp.arange(half, dtype=jnp.float32) / half)
    places = jnp.arange(count, dtype=jnp.float32)
    angle = places[:, None] * inverse[None, :]
    return (jnp.cos(angle), jnp.sin(angle))

def rotate(values, cosine, sine):
    half = values.shape[-1] // 2
    first_half = values[..., :half]
    second_half = values[..., half:]
    cosine = cosine[:, None, :]
    sine = sine[:, None, :]
    return jnp.concatenate([first_half * cosine - second_half * sine, second_half * cosine + first_half * sine], axis=-1)

def attend_slot(item):
    queries, keys, values, length = item
    group = HEADS // KV_HEADS
    keys = jnp.repeat(keys, group, axis=1)
    values = jnp.repeat(values, group, axis=1)
    scores = jnp.einsum('qhd,khd->hqk', queries, keys, precision=highest) * (1.0 / math.sqrt(HEAD_DIM))
    scores = low_back(scores)
    places = jnp.arange(SLOT, dtype=jnp.int32)
    valid = (places[None, :] <= places[:, None]) & (places[None, :] < length)
    scores = jnp.where(valid[None], scores, masked_score)
    probs = low(jax.nn.softmax(scores, axis=-1))
    return jnp.einsum('hqk,khd->qhd', probs, values, precision=highest)

def layer(inputs, lengths, attn_gain, w_query, b_query, w_key, b_key, w_value, b_value, w_out, ffn_gain, w_gate, w_up, w_down):
    count = inputs.shape[0]
    rows = count * SLOT
    flat = inputs.reshape(rows, D)
    normed = low(rms_norm(flat, low(attn_gain)))
    query = low_back(product(normed, low(w_query)) + low(b_query))
    key = low_back(product(normed, low(w_key)) + low(b_key))
    value = low_back(product(normed, low(w_value)) + low(b_value))
    cosine, sine = rope_tables(SLOT)
    query = low(rotate(query.reshape(count, SLOT, HEADS, HEAD_DIM), cosine, sine))
    key = low(rotate(key.reshape(count, SLOT, KV_HEADS, HEAD_DIM), cosine, sine))
    value = low(value.reshape(count, SLOT, KV_HEADS, HEAD_DIM))
    mixed = lax.map(jax.checkpoint(attend_slot), (query, key, value, lengths))
    mixed = low_back(low(mixed.reshape(rows, HEADS * HEAD_DIM)))
    attn = low_back(product(mixed, low(w_out)))
    resid = flat + attn
    normed_two = low(rms_norm(resid, low(ffn_gain)))
    gate = low_back(product(normed_two, low(w_gate)))
    upper = low_back(product(normed_two, low(w_up)))
    hidden = low(jax.nn.silu(gate) * upper)
    result = resid + product(hidden, low(w_down))
    places = jnp.arange(SLOT, dtype=jnp.int32)
    keep = (places[None, :] < lengths[:, None]).astype(jnp.float32)
    return result.reshape(count, SLOT, D) * keep[:, :, None]

def reference(tokens, lengths, attn_gain, w_query, b_query, w_key, b_key, w_value, b_value, w_out, ffn_gain, w_gate, w_up, w_down, cotangent):
    weights = (attn_gain, w_query, b_query, w_key, b_key, w_value, b_value, w_out, ffn_gain, w_gate, w_up, w_down)
    total = tokens.shape[0]
    per_group = 4 if total % 4 == 0 else 1
    groups = total // per_group
    inputs = tokens.astype(jnp.float32).reshape(groups, per_group, SLOT, D)
    grads_in = cotangent.astype(jnp.float32).reshape(groups, per_group, SLOT, D)
    group_lengths = lengths.reshape(groups, per_group)

    def step(carry, item):
        group_in, group_len, group_grad = item

        def forward(values, *params):
            return layer(values, group_len, *params)
        result, pull = jax.vjp(forward, group_in, *weights)
        grads = pull(group_grad)
        carry = tuple((acc + part for acc, part in zip(carry, grads[1:])))
        return (carry, (result.astype(jnp.bfloat16), grads[0].astype(jnp.bfloat16)))
    start = tuple((jnp.zeros_like(weight) for weight in weights))
    sums, (results, input_grads) = lax.scan(step, start, (inputs, group_lengths, grads_in))
    layer_out = results.reshape(total, SLOT, D)
    input_grad = input_grads.reshape(total, SLOT, D)
    return (layer_out, input_grad, sums[0], sums[1], sums[2], sums[3], sums[4], sums[5], sums[6], sums[7], sums[8], sums[9], sums[10], sums[11])
```

```python
import functools
import math

import jax
import jax.numpy as jnp
from jax import lax
from jax.experimental import pallas as pl
from jax.experimental.pallas import tpu as pltpu
from jax.sharding import PartitionSpec as P

HEADS = 12
KV_HEADS = 2
HEAD_DIM = 128
SLOT = 1024
INNER = 4
EXTRA = 8

epsilon = 1e-06
masked_score = -1e30
far_place = 1 << 30
scale = 1.0 / math.sqrt(HEAD_DIM)
low = jnp.bfloat16
full = jnp.float32


def product(left, right):
    return jnp.dot(left, right, preferred_element_type=full)


def product_left(left, right):
    return lax.dot_general(left, right, (((0,), (0,)), ((), ())), preferred_element_type=full)


def product_right(left, right):
    return lax.dot_general(left, right, (((1,), (1,)), ((), ())), preferred_element_type=full)


def norm_rows(values, gain):
    factor = lax.rsqrt(jnp.mean(values * values, axis=-1, keepdims=True) + epsilon)
    return (values * factor * gain, factor)


def norm_back(values, factor, gain, upstream):
    weighted = upstream * gain
    inner = jnp.mean(weighted * values, axis=-1, keepdims=True)
    grad_in = factor * weighted - values * (factor * factor * factor) * inner
    grad_gain = jnp.sum(upstream * values * factor, axis=0)
    return (grad_in, grad_gain)


def swap(value, hop):
    axis, bit = hop
    count = lax.axis_size(axis)
    return lax.ppermute(value, axis, [(i, i ^ bit) for i in range(count)])


def gather_hops(block, hops):
    held = block[None]
    for hop in hops:
        held = jnp.concatenate([held, swap(held, hop)], axis=0)
    return held


def reduce_hops(held, hops):
    for hop in reversed(hops):
        half = held.shape[0] // 2
        other = swap(held[half:].astype(low), hop)
        held = held[:half] + other.astype(full)
    return held[0]


def bits_of(axis, count):
    found, bit = [], 1
    while bit < count:
        found.append((axis, bit))
        bit *= 2
    return found


def plane_hops(seq_count):
    inner = bits_of("wt", INNER)
    seq = bits_of("seq", seq_count)
    slow = inner[1:] + seq
    return (slow + inner[:1], slow[::-1] + inner[:1])


def rank_of(hops):
    place = jnp.int32(0)
    for k, (axis, bit) in enumerate(hops):
        here = (lax.axis_index(axis) // bit) % 2
        place = place + here * (1 << k)
    return place


def plane_order(hops, count):
    order = []
    for inner in range(INNER):
        for seq in range(count):
            place = 0
            for k, (axis, bit) in enumerate(hops):
                source = inner if axis == "wt" else seq
                place |= ((source // bit) % 2) << k
            order.append(place)
    return order


def gather_plane(block, seq_count):
    hops_a, hops_b = plane_hops(seq_count)
    half = block.shape[0] // 2
    part_a = gather_hops(block[:half], hops_a)
    part_b = gather_hops(block[half:], hops_b)
    return (part_a, part_b)


def reduce_plane(part_a, part_b, seq_count):
    hops_a, hops_b = plane_hops(seq_count)
    return jnp.concatenate([reduce_hops(part_a, hops_a), reduce_hops(part_b, hops_b)], axis=0)


def to_place(stacked, place):
    return lax.dynamic_index_in_dim(stacked, place, 0, keepdims=False)


def qkv_kernel(n_ref, w_ref, b_ref, cos_ref, sin_ref, o_ref):
    step = pl.program_id(0)
    out = jnp.dot(n_ref[...], w_ref[...], preferred_element_type=full) + b_ref[...]
    cosine = cos_ref[...]
    sine = sin_ref[...]

    @pl.when(step < pl.num_programs(0) - 1)
    def _():
        for k in range(2):
            part = out[:, k * HEAD_DIM : (k + 1) * HEAD_DIM]
            turned = part * cosine + pltpu.roll(part, HEAD_DIM // 2, 1) * sine
            o_ref[:, k * HEAD_DIM : (k + 1) * HEAD_DIM] = turned.astype(low)

    @pl.when(step == pl.num_programs(0) - 1)
    def _():
        o_ref[...] = out.astype(low)


def project_heads(normed, weights, bias, cosine, sine):
    rows, width = normed.shape
    total = weights.shape[1]
    wide = 2 * HEAD_DIM
    return pl.pallas_call(
        qkv_kernel,
        grid=(total // wide,),
        in_specs=[
            pl.BlockSpec((rows, width), lambda i: (0, 0)),
            pl.BlockSpec((width, wide), lambda i: (0, i)),
            pl.BlockSpec((1, wide), lambda i: (0, i)),
            pl.BlockSpec((rows, HEAD_DIM), lambda i: (0, 0)),
            pl.BlockSpec((rows, HEAD_DIM), lambda i: (0, 0)),
        ],
        out_specs=pl.BlockSpec((rows, wide), lambda i: (0, i)),
        out_shape=jax.ShapeDtypeStruct((rows, total), low),
        cost_estimate=pl.CostEstimate(
            flops=2 * rows * width * total,
            bytes_accessed=2 * (width * total + rows * (width + total)),
            transcendentals=0,
        ),
        name="project_heads",
    )(normed, weights, bias, cosine, sine)


def shown(kpos_ref, rows, keys):
    places = lax.broadcasted_iota(jnp.int32, (rows, keys), 0)
    return kpos_ref[...] <= places


def fwd_kernel(kpos_ref, q_ref, k_ref, v_ref, o_ref):
    rows, keys = q_ref.shape[0], k_ref.shape[0]
    scores = (
        lax.dot_general(
            q_ref[...], k_ref[...], (((1,), (1,)), ((), ())), preferred_element_type=full
        )
        * scale
    )
    scores = jnp.where(shown(kpos_ref, rows, keys), scores, masked_score)
    top = jnp.max(scores, axis=-1, keepdims=True)
    weights = jnp.exp(scores - top)
    total = jnp.sum(weights, axis=-1, keepdims=True)
    probs = (weights * (1.0 / total)).astype(low)
    o_ref[...] = jnp.dot(probs, v_ref[...], preferred_element_type=full).astype(low)


def attend_forward(kpos, qkv, pairs):
    rows = qkv.shape[0]
    keys = pairs.shape[0]
    group = HEADS // KV_HEADS
    return pl.pallas_call(
        fwd_kernel,
        grid=(HEADS,),
        in_specs=[
            pl.BlockSpec((1, keys), lambda h: (0, 0)),
            pl.BlockSpec((rows, HEAD_DIM), lambda h: (0, h)),
            pl.BlockSpec((keys, HEAD_DIM), lambda h: (0, h // group)),
            pl.BlockSpec((keys, HEAD_DIM), lambda h: (0, KV_HEADS + h // group)),
        ],
        out_specs=pl.BlockSpec((rows, HEAD_DIM), lambda h: (0, h)),
        out_shape=jax.ShapeDtypeStruct((rows, HEADS * HEAD_DIM), low),
        cost_estimate=pl.CostEstimate(
            flops=4 * rows * keys * HEADS * HEAD_DIM * 3,
            bytes_accessed=4 * rows * HEADS * HEAD_DIM + 4 * keys * KV_HEADS * HEAD_DIM,
            transcendentals=rows * keys * HEADS,
        ),
        name="attend_forward",
    )(kpos, qkv, pairs, pairs)


def bwd_kernel(kpos_ref, cos_ref, sin_ref, q_ref, k_ref, v_ref, g_ref, dq_ref, dk_ref, dv_ref):
    rows, keys = q_ref.shape[0], k_ref.shape[0]
    group = HEADS // KV_HEADS
    head = pl.program_id(0)
    queries, key, value, grad = q_ref[...], k_ref[...], v_ref[...], g_ref[...]
    scores = (
        lax.dot_general(queries, key, (((1,), (1,)), ((), ())), preferred_element_type=full)
        * scale
    )
    scores = jnp.where(shown(kpos_ref, rows, keys), scores, masked_score)
    top = jnp.max(scores, axis=-1, keepdims=True)
    weights = jnp.exp(scores - top)
    total = jnp.sum(weights, axis=-1, keepdims=True)
    probs = weights * (1.0 / total)
    prob_grad = lax.dot_general(
        grad, value, (((1,), (1,)), ((), ())), preferred_element_type=full
    )
    inner = jnp.sum(probs * prob_grad, axis=-1, keepdims=True)
    score_grad = (probs * (prob_grad - inner)).astype(low)
    dv = lax.dot_general(
        probs.astype(low), grad, (((0,), (0,)), ((), ())), preferred_element_type=full
    )
    dk = (
        lax.dot_general(
            score_grad, queries, (((0,), (0,)), ((), ())), preferred_element_type=full
        )
        * scale
    )
    dq = jnp.dot(score_grad, key, preferred_element_type=full) * scale
    turned = dq * cos_ref[...] - pltpu.roll(dq, HEAD_DIM // 2, 1) * sin_ref[...]
    dq_ref[...] = turned.astype(low)

    @pl.when(head % group == 0)
    def _():
        dk_ref[...] = dk
        dv_ref[...] = dv

    @pl.when(head % group != 0)
    def _():
        dk_ref[...] += dk
        dv_ref[...] += dv


def attend_backward(kpos, cosine, sine, qkv, pairs, grad):
    rows = qkv.shape[0]
    keys = pairs.shape[0]
    group = HEADS // KV_HEADS
    width = KV_HEADS * HEAD_DIM
    return pl.pallas_call(
        bwd_kernel,
        grid=(HEADS,),
        in_specs=[
            pl.BlockSpec((1, keys), lambda h: (0, 0)),
            pl.BlockSpec((rows, HEAD_DIM), lambda h: (0, 0)),
            pl.BlockSpec((rows, HEAD_DIM), lambda h: (0, 0)),
            pl.BlockSpec((rows, HEAD_DIM), lambda h: (0, h)),
            pl.BlockSpec((keys, HEAD_DIM), lambda h: (0, h // group)),
            pl.BlockSpec((keys, HEAD_DIM), lambda h: (0, KV_HEADS + h // group)),
            pl.BlockSpec((rows, HEAD_DIM), lambda h: (0, h)),
        ],
        out_specs=[
            pl.BlockSpec((rows, HEAD_DIM), lambda h: (0, h)),
            pl.BlockSpec((keys, HEAD_DIM), lambda h: (0, h // group)),
            pl.BlockSpec((keys, HEAD_DIM), lambda h: (0, h // group)),
        ],
        out_shape=[
            jax.ShapeDtypeStruct((rows, HEADS * HEAD_DIM), low),
            jax.ShapeDtypeStruct((keys, width), full),
            jax.ShapeDtypeStruct((keys, width), full),
        ],
        cost_estimate=pl.CostEstimate(
            flops=10 * rows * keys * HEADS * HEAD_DIM * 3,
            bytes_accessed=8 * rows * HEADS * HEAD_DIM + 12 * keys * width,
            transcendentals=rows * keys * HEADS,
        ),
        name="attend_backward",
    )(kpos, cosine, sine, qkv, pairs, pairs, grad)


def body(
    tokens, lengths, attn_gain, w_query, b_query, w_key, b_key, w_value, b_value, w_out,
    ffn_gain, w_gate, w_up, w_down, cotangent,
):
    slot_count, rows, width = tokens.shape
    seq_count = lax.axis_size("seq")
    wt_count = lax.axis_size("wt")
    outer = wt_count // INNER
    seq_here = lax.axis_index("seq")
    inner_here = lax.axis_index("wt") % INNER
    line = [[o * INNER + i for o in range(outer)] for i in range(INNER)]
    hops_a, hops_b = plane_hops(seq_count)
    plane = INNER * seq_count
    share = w_query.shape[0]
    bias_q, bias_k = b_query.shape[0], b_key.shape[0]
    query_width = HEADS * HEAD_DIM
    pair_width = KV_HEADS * HEAD_DIM
    head_width = query_width + 2 * pair_width
    ff_own = w_down.shape[0] // seq_count
    ff_here = outer * ff_own
    ff_pad = -(-ff_here // 128) * 128

    flat = tokens.astype(full).reshape(rows, width)
    places = seq_here * rows + jnp.arange(rows, dtype=jnp.int32)
    keep = (places < lengths[0])[:, None]
    upstream_low = jnp.where(keep, cotangent.reshape(rows, width), jnp.zeros((), low))

    def own_columns(value):
        wide = value.shape[1] // seq_count
        return lax.dynamic_slice_in_dim(value, seq_here * wide, wide, axis=1)

    def line_gather(value):
        return lax.all_gather(value, "wt", axis=0, axis_index_groups=line, tiled=False)

    def line_reduce(value):
        return lax.psum_scatter(
            value, "wt", scatter_dimension=0, axis_index_groups=line, tiled=False
        )

    def gather_weight(value):
        count, wide = value.shape
        lined = line_gather(own_columns(value))
        part = wide // seq_count
        half = part // 2
        got = []
        for hops, piece in ((hops_a, lined[..., :half]), (hops_b, lined[..., half:])):
            stacked = gather_hops(piece, hops)
            me = rank_of(hops)
            placed = [to_place(stacked, me ^ p) for p in plane_order(hops, seq_count)]
            ordered = jnp.stack(placed).reshape(INNER, seq_count, outer, count, half)
            got.append(ordered.transpose(2, 0, 3, 1, 4))
        return jnp.stack(got, axis=4).reshape(wt_count, count, wide)

    def reduce_weight(value):
        count, wide = value.shape[1:]
        half = wide // seq_count // 2
        split = value.reshape(outer, INNER, count, seq_count, 2, half)
        done = []
        for k, hops in enumerate((hops_a, hops_b)):
            piece = split[:, :, :, :, k].transpose(1, 3, 0, 2, 4)
            piece = piece.reshape(plane, outer, count, half)
            order = plane_order(hops, seq_count)
            back = [order.index(p) for p in range(plane)]
            table = jnp.asarray(back, dtype=jnp.int32)
            me = rank_of(hops)
            placed = [to_place(piece, table[me ^ p]) for p in range(plane)]
            done.append(reduce_hops(jnp.stack(placed).astype(full), hops))
        lined = jnp.concatenate(done, axis=-1).astype(low)
        mine = line_reduce(lined)
        return seq_columns(mine)

    def seq_gather(value):
        stacked = gather_hops(value, bits_of("seq", seq_count))
        return jnp.stack([to_place(stacked, seq_here ^ p) for p in range(seq_count)])

    def seq_columns(value):
        got = seq_gather(value)
        return got.transpose(1, 0, 2).reshape(value.shape[0], -1)

    small = jnp.concatenate([attn_gain, b_query, b_key, b_value, ffn_gain]).astype(low)
    small_rows = jnp.zeros((EXTRA, head_width), low).at[0, : small.shape[0]].set(small)
    packed = jnp.concatenate(
        [jnp.concatenate([w_query, w_key, w_value], axis=1).astype(low), small_rows], axis=0
    )
    heads_all = gather_weight(packed)
    head_w = heads_all[:, :share].reshape(width, head_width)
    small_all = heads_all[:, share, : small.shape[0]].astype(full)
    edges = [0, share, share + bias_q]
    edges += [edges[-1] + bias_k, edges[-1] + 2 * bias_k]
    gain_one = small_all[:, : edges[1]].reshape(-1)
    head_b = jnp.concatenate(
        [
            small_all[:, edges[1] : edges[2]].reshape(-1),
            small_all[:, edges[2] : edges[3]].reshape(-1),
            small_all[:, edges[3] : edges[4]].reshape(-1),
        ]
    )
    gain_two = small_all[:, edges[4] :].reshape(-1)
    out_w = gather_weight(w_out.astype(low)).reshape(query_width, width)

    down_own = lax.dynamic_slice_in_dim(w_down, seq_here * ff_own, ff_own, axis=0).astype(low)
    down_w = line_gather(down_own).reshape(ff_here, width)
    down_w = jnp.pad(down_w, ((0, ff_pad - ff_here), (0, 0)))

    def to_units(value):
        split = value.reshape(share, outer, INNER, seq_count, ff_own)
        split = lax.dynamic_index_in_dim(split, seq_here, 3, keepdims=False).astype(low)
        split = split.transpose(2, 0, 1, 3).reshape(INNER, share, ff_here)
        return jnp.pad(split, ((0, 0), (0, 0), (0, ff_pad - ff_here)))

    def inner_swap(value, distance):
        count = lax.axis_size("wt")
        return lax.ppermute(value, "wt", [(i, i ^ distance) for i in range(count)])

    def inner_exchange(value):
        got = [to_place(value, inner_here)]
        got += [inner_swap(to_place(value, inner_here ^ d), d) for d in range(1, INNER)]
        stacked = jnp.stack(got)
        return jnp.stack([to_place(stacked, inner_here ^ p) for p in range(INNER)])

    def gather_units(value):
        block = inner_exchange(to_units(value)).reshape(INNER * share, ff_pad)
        return line_gather(block).reshape(width, ff_pad)

    gate_w = gather_units(w_gate)
    up_w = gather_units(w_up)

    normed, factor_one = norm_rows(flat, gain_one)
    normed_low = normed.astype(low)
    half = HEAD_DIM // 2
    inverse = 10000.0 ** (-jnp.arange(half, dtype=full) / half)
    angle = places.astype(full)[:, None] * inverse[None, :]
    cosine = jnp.cos(angle)
    sine = jnp.sin(angle)
    cosine = jnp.concatenate([cosine, cosine], axis=1)
    sine = jnp.concatenate([-sine, sine], axis=1)
    qkv = project_heads(normed_low, head_w, head_b[None, :], cosine, sine)
    seq_hops = bits_of("seq", seq_count)
    pairs = gather_hops(qkv[:, query_width:], seq_hops).reshape(SLOT, 2 * pair_width)
    distance = jnp.arange(SLOT, dtype=jnp.int32)
    key_place = (seq_here ^ (distance // rows)) * rows + distance % rows
    kpos = jnp.where(key_place < lengths[0], key_place - seq_here * rows, far_place)[None, :]
    mixed = attend_forward(kpos, qkv, pairs)
    resid = flat + product(mixed, out_w)
    normed_two, factor_two = norm_rows(resid, gain_two)
    normed_two_low = normed_two.astype(low)

    def spread(block):
        part_a, part_b = gather_plane(block, seq_count)
        return jnp.stack([part_a, part_b]).reshape(plane * rows, width)

    def collect(partial):
        both = partial.reshape(2, plane, rows // 2, width)
        return reduce_plane(both[0], both[1], seq_count)

    grad_all = spread(upstream_low)
    hidden_grad = product_right(grad_all, down_w)
    rows_all = spread(normed_two_low)
    gate = product(rows_all, gate_w)
    upper = product(rows_all, up_w)
    sigma = jax.nn.sigmoid(gate)
    hidden = (gate * sigma * upper).astype(low)
    gate_grad = (hidden_grad * upper * sigma * (1.0 + gate * (1.0 - sigma))).astype(low)
    up_grad = (hidden_grad * gate * sigma).astype(low)
    normed_two_grad = collect(product_right(gate_grad, gate_w) + product_right(up_grad, up_w))
    down_grad = product_left(hidden, grad_all).astype(low)[:ff_here]
    down_line = line_reduce(down_grad.reshape(outer, ff_own, width))
    gate_w_grad = product_left(rows_all, gate_grad).astype(low)
    up_w_grad = product_left(rows_all, up_grad).astype(low)
    gate_line = line_reduce(gate_w_grad.reshape(outer, INNER * share, ff_pad))
    up_line = line_reduce(up_w_grad.reshape(outer, INNER * share, ff_pad))
    result = resid + collect(product(hidden, down_w))
    layer_out = jnp.where(keep, result, 0.0).astype(low).reshape(slot_count, rows, width)

    def units_back(lined):
        got = inner_exchange(lined.reshape(INNER, share, ff_pad))[:, :, :ff_here]
        both = seq_gather(got.reshape(INNER * share, ff_here))
        both = both.reshape(seq_count, INNER, share, outer, ff_own)
        return both.transpose(2, 3, 1, 0, 4).reshape(share, -1).astype(full)

    down_out = seq_gather(down_line).reshape(seq_count * ff_own, width).astype(full)
    gate_out = units_back(gate_line)
    up_out = units_back(up_line)

    upstream = upstream_low.astype(full)
    resid_norm_grad, gain_two_grad = norm_back(resid, factor_two, gain_two, normed_two_grad)
    resid_grad = upstream + resid_norm_grad
    attn_grad = resid_grad.astype(low)
    mixed_grad = product_right(attn_grad, out_w).astype(low)
    out_w_grad = product_left(mixed, attn_grad).astype(low)
    out_w_out = reduce_weight(out_w_grad.reshape(wt_count, -1, width)).astype(full)
    query_grad, key_part, value_part = attend_backward(
        kpos, cosine, sine, qkv, pairs, mixed_grad
    )
    pair_part = jnp.concatenate([key_part, value_part], axis=1)
    pair_sum = reduce_hops(pair_part.reshape(seq_count, rows, 2 * pair_width), seq_hops)
    key_rot_grad = pair_sum[:, :pair_width].reshape(rows, KV_HEADS, HEAD_DIM)
    turned = jnp.concatenate([key_rot_grad[..., half:], key_rot_grad[..., :half]], axis=-1)
    key_grad = key_rot_grad * cosine[:, None, :] - turned * sine[:, None, :]
    head_grad = jnp.concatenate(
        [query_grad, key_grad.reshape(rows, pair_width).astype(low),
         pair_sum[:, pair_width:].astype(low)],
        axis=1,
    )
    head_w_grad = product_left(normed_low, head_grad).astype(low)
    head_b_grad = jnp.sum(head_grad.astype(full), axis=0)
    normed_grad = product_right(head_grad, head_w)
    input_norm_grad, gain_one_grad = norm_back(flat, factor_one, gain_one, normed_grad)
    input_grad = (resid_grad + input_norm_grad).astype(low).reshape(slot_count, rows, width)

    def parts(vector):
        return vector.reshape(wt_count, -1)

    small_grad = jnp.concatenate(
        [
            parts(gain_one_grad),
            parts(head_b_grad[:query_width]),
            parts(head_b_grad[query_width : query_width + pair_width]),
            parts(head_b_grad[query_width + pair_width :]),
            parts(gain_two_grad),
        ],
        axis=1,
    ).astype(low)
    extra = jnp.pad(
        small_grad[:, None, :],
        ((0, 0), (0, EXTRA - 1), (0, head_width - small_grad.shape[1])),
    )
    head_sum = reduce_weight(
        jnp.concatenate([head_w_grad.reshape(wt_count, share, head_width), extra], axis=1)
    ).astype(full)
    heads_out = head_sum[:share]
    small_out = head_sum[share]
    return (
        layer_out,
        input_grad,
        small_out[: edges[1]],
        heads_out[:, :query_width],
        small_out[edges[1] : edges[2]],
        heads_out[:, query_width : query_width + pair_width],
        small_out[edges[2] : edges[3]],
        heads_out[:, query_width + pair_width :],
        small_out[edges[3] : edges[4]],
        out_w_out,
        small_out[edges[4] : edges[4] + ffn_gain.shape[0]],
        gate_out,
        up_out,
        down_out,
    )


def solution(mesh):
    by_wt = P("wt")
    by_row = P("wt", None)
    by_token = P("wt", "seq", None)
    return jax.shard_map(
        body,
        mesh=mesh,
        in_specs=(
            by_token, by_wt, by_wt, by_row, by_wt, by_row, by_wt, by_row, by_wt, by_row,
            by_wt, by_row, by_row, by_row, by_token,
        ),
        out_specs=(
            by_token, by_token, by_wt, by_row, by_wt, by_row, by_wt, by_row, by_wt, by_row,
            by_wt, by_row, by_row, by_row,
        ),
        check_vma=False,
    )
```

```python
import functools
import math

import jax
import jax.numpy as jnp
from jax import lax
from jax.experimental import pallas as pl
from jax.experimental.pallas import tpu as pltpu
from jax.sharding import PartitionSpec as P


HEADS = 12
KV_HEADS = 2
HEAD_DIM = 128
SLOT = 1024
INNER = 4
EXTRA = 8

epsilon = 1e-06
masked_score = -1e30
far_place = 1 << 30
scale = 1.0 / math.sqrt(HEAD_DIM)
low = jnp.bfloat16
full = jnp.float32


def product(left, right):
    return jnp.dot(left, right, preferred_element_type=full)


def product_left(left, right):
    return lax.dot_general(left, right, (((0,), (0,)), ((), ())), preferred_element_type=full)


def product_right(left, right):
    return lax.dot_general(left, right, (((1,), (1,)), ((), ())), preferred_element_type=full)


def norm_rows(values, gain):
    factor = lax.rsqrt(jnp.mean(values * values, axis=-1, keepdims=True) + epsilon)
    return (values * factor * gain, factor)


def norm_back(values, factor, gain, upstream):
    weighted = upstream * gain
    inner = jnp.mean(weighted * values, axis=-1, keepdims=True)
    grad_in = factor * weighted - values * (factor * factor * factor) * inner
    grad_gain = jnp.sum(upstream * values * factor, axis=0)
    return (grad_in, grad_gain)


def swap(value, hop):
    axis, bit = hop
    count = lax.axis_size(axis)
    return lax.ppermute(value, axis, [(i, i ^ bit) for i in range(count)])


def gather_hops(block, hops):
    held = block[None]
    for hop in hops:
        held = jnp.concatenate([held, swap(held, hop)], axis=0)
    return held


def reduce_hop(held, hop):
    half = held.shape[0] // 2
    other = swap(held[half:], hop)
    return (held[:half].astype(full) + other.astype(full)).astype(low)


def reduce_hops(held, hops):
    for hop in hops[:0:-1]:
        held = reduce_hop(held, hop)
    return held[0].astype(full) + swap(held[1], hops[0]).astype(full)


def bits_of(axis, count):
    found, bit = [], 1
    while bit < count:
        found.append((axis, bit))
        bit *= 2
    return found


def plane_hops(seq_count):
    inner = bits_of("wt", INNER)
    seq = bits_of("seq", seq_count)
    slow = inner[1:] + seq
    return (slow + inner[:1], slow[::-1] + inner[:1])


def rank_of(hops):
    place = jnp.int32(0)
    for k, (axis, bit) in enumerate(hops):
        here = (lax.axis_index(axis) // bit) % 2
        place = place + here * (1 << k)
    return place


def plane_order(hops, count):
    order = []
    for inner in range(INNER):
        for seq in range(count):
            place = 0
            for k, (axis, bit) in enumerate(hops):
                source = inner if axis == "wt" else seq
                place |= ((source // bit) % 2) << k
            order.append(place)
    return order


def gather_plane(block, seq_count):
    hops_a, hops_b = plane_hops(seq_count)
    half = block.shape[0] // 2
    part_a = gather_hops(block[:half], hops_a)
    part_b = gather_hops(block[half:], hops_b)
    return (part_a, part_b)


def to_place(stacked, place):
    return lax.dynamic_index_in_dim(stacked, place, 0, keepdims=False)


def flip(index, bit):
    return index + bit - 2 * bit * ((index // bit) % 2)


def flip_all(index, distance):
    bit = 1
    while bit <= distance:
        if distance & bit:
            index = flip(index, bit)
        bit *= 2
    return index


def inner_bits():
    return [bit for _, bit in bits_of("wt", INNER)]


def meet(peers):
    barrier = pltpu.get_barrier_semaphore()
    for peer in peers:
        pl.semaphore_signal(
            barrier, inc=1, device_id=peer, device_id_type=pl.DeviceIdType.MESH
        )
    pl.semaphore_wait(barrier, len(peers))


class Sender:
    def __init__(self, send_sems, recv_sems):
        self.sems = (send_sems, recv_sems)
        self.copies = []

    def start(self, source, target, peer):
        at = len(self.copies)
        copy = pltpu.make_async_remote_copy(
            src_ref=source,
            dst_ref=target,
            send_sem=self.sems[0].at[at],
            recv_sem=self.sems[1].at[at],
            device_id=peer,
            device_id_type=pl.DeviceIdType.MESH,
        )
        copy.start()
        self.copies.append(copy)
        return copy


def subsets(hops):
    found = [(0, 0)]
    for axis, bit in hops:
        more = [(a ^ bit, b) if axis == "wt" else (a, b ^ bit) for a, b in found]
        found = found + more
    return found


def plane_copies(seq_count):
    hops_a, _ = plane_hops(seq_count)
    slow = len(hops_a) - 1
    return (2 * (2**slow - 1), len(set(a for a, _ in subsets(hops_a[:-1]))))


def gather_kernel(
    outer, seq_count, x_ref, p_ref, wo_ref, s_ref, cos_ref, sin_ref,
    normed_ref, qkv_ref, vec_ref, head_ref, out_ref,
    w_scr, o_scr, s_scr, send_sems, recv_sems, local_sems,
):
    share, head_width = p_ref.shape
    width = x_ref.shape[1]
    wt, seq = lax.axis_index("wt"), lax.axis_index("seq")
    line, inner = wt // INNER, wt % INNER
    hops = plane_hops(seq_count)
    slow = len(hops[0]) - 1
    peers = [(flip_all(line, d) * INNER + inner, seq) for d in range(1, outer)]
    peers += [(wt - inner + flip(inner, bit), seq) for bit in inner_bits()]
    peers += [(wt, flip(seq, bit)) for _, bit in bits_of("seq", seq_count)]

    def own_columns(total):
        wide = total // seq_count
        return pl.ds(pl.multiple_of(seq * wide, 128), wide)

    fill = [
        pltpu.make_async_copy(
            ref.at[:, own_columns(ref.shape[1])],
            scratch.at[line, inner, :, own_columns(ref.shape[1])],
            local_sems.at[k],
        )
        for k, (ref, scratch) in enumerate(((p_ref, w_scr), (wo_ref, o_scr)))
    ] + [
        pltpu.make_async_copy(s_ref, s_scr.at[line, inner], local_sems.at[2]),
    ]
    for copy in fill:
        copy.start()
    meet(peers)
    out = Sender(send_sems, recv_sems)

    def hop_peer(hop):
        axis, bit = hop
        if axis == "wt":
            return (wt - inner + flip(inner, bit), seq)
        return (wt, flip(seq, bit))

    def columns(total, part, half):
        wide = total // seq_count
        first = -(-wide // 256) * 128
        start = part * wide + half * first
        return pl.ds(pl.multiple_of(start, 128), wide - first if half else first)

    def start_line(source, scratch, narrow):
        total = source.shape[1]
        copies = [None]
        for d in range(1, outer):
            if narrow:
                part = own_columns(total)
                pair = (source.at[:, part], scratch.at[line, inner, :, part])
            else:
                pair = (source, scratch.at[line, inner])
            copies.append(out.start(*pair, (flip_all(line, d) * INNER + inner, seq)))
        return copies

    small_line = start_line(s_ref, s_scr, False)
    head_line = start_line(p_ref, w_scr, True)
    out_line = start_line(wo_ref, o_scr, True)

    def start_stage(scratch, at, stage):
        total = scratch.shape[-1]
        copies = []
        if stage < slow:
            for half in range(2):
                hop = hops[half][stage]
                for a, b in subsets(hops[half][:stage]):
                    place = scratch.at[
                        at, flip_all(inner, a), :, columns(total, flip_all(seq, b), half)
                    ]
                    copies.append(out.start(place, place, hop_peer(hop)))
            return copies
        for a in sorted(set(a for a, _ in subsets(hops[0][:slow]))):
            place = scratch.at[at, flip_all(inner, a)]
            copies.append(out.start(place, place, hop_peer(hops[0][slow])))
        return copies

    def arrive(copies):
        for copy in copies:
            if copy is not None:
                copy.wait_recv()

    for copy in fill:
        copy.wait()
    waiting = [[copy] for copy in head_line]
    small_wait = small_line
    for step in range(outer + slow + 1):
        for stage in range(slow + 1):
            d = step - stage
            if 0 <= d < outer:
                arrive(waiting[d])
                waiting[d] = start_stage(w_scr, flip_all(line, d), stage)
        if step == 0:
            arrive(small_wait)
            small_wait = []
        if step < len(inner_bits()):
            arrive(small_wait)
            bit = inner_bits()[::-1][step]
            small_wait = []
            for a, _ in subsets([("wt", b) for b in inner_bits()[::-1][:step]]):
                place = s_scr.at[:, flip_all(inner, a)]
                small_wait.append(out.start(place, place, hop_peer(("wt", bit))))
    arrive(small_wait)
    arrive(out_line)
    out_wait = start_stage(o_scr, slice(None), 0)

    count = outer * INNER
    bias_k = share * KV_HEADS * HEAD_DIM // (HEADS * HEAD_DIM)
    query_width = HEADS * HEAD_DIM
    pair_width = KV_HEADS * HEAD_DIM
    vec_ref[...] = jnp.zeros_like(vec_ref)
    for k in range(count):
        small = s_scr[k // INNER, k % INNER].astype(full)
        at = k * share
        vec_ref[0:1, at : at + share] = small[0:1, :share]
        vec_ref[1:2, at : at + share] = small[1:2, :share]
        at = query_width + k * bias_k
        vec_ref[1:2, at : at + bias_k] = small[2:3, :bias_k]
        at = query_width + pair_width + k * bias_k
        vec_ref[1:2, at : at + bias_k] = small[3:4, :bias_k]
        at = k * share
        vec_ref[2:3, at : at + share] = small[4:5, :share]

    values = x_ref[...].astype(full)
    factor = lax.rsqrt(jnp.mean(values * values, axis=-1, keepdims=True) + epsilon)
    normed_ref[...] = (values * factor * vec_ref[0:1, :width]).astype(low)
    for d in range(outer):
        arrive(waiting[d])
    keep_head = pltpu.make_async_copy(w_scr, head_ref, local_sems.at[0])
    keep_head.start()
    wide = 2 * HEAD_DIM
    blocks = head_width // wide

    def project(at):
        weights = w_scr[:, :, :, pl.ds(at, wide)].reshape(width, wide)
        return (
            jnp.dot(normed_ref[...], weights, preferred_element_type=full)
            + vec_ref[1:2, pl.ds(at, wide)]
        )

    def turn_block(k):
        at = pl.multiple_of(k * wide, wide)
        got = project(at)
        for j in range(2):
            part = got[:, j * HEAD_DIM : (j + 1) * HEAD_DIM]
            turned = part * cos_ref[...] + pltpu.roll(part, HEAD_DIM // 2, 1) * sin_ref[...]
            where = pl.multiple_of(at + j * HEAD_DIM, HEAD_DIM)
            qkv_ref[:, pl.ds(where, HEAD_DIM)] = turned.astype(low)

    turned_blocks = blocks - pair_width // wide
    marks = [turned_blocks * (k + 1) // (slow + 1) for k in range(slow + 1)]
    begin = 0
    for stage in range(slow + 1):
        @pl.loop(begin, marks[stage])
        def _(k):
            turn_block(k)

        begin = marks[stage]
        arrive(out_wait)
        out_wait = start_stage(o_scr, slice(None), stage + 1) if stage < slow else []
    for k in range(turned_blocks, blocks):
        qkv_ref[:, k * wide : (k + 1) * wide] = project(k * wide).astype(low)
    keep_out = pltpu.make_async_copy(o_scr, out_ref, local_sems.at[1])
    keep_out.start()
    for copy in out.copies:
        copy.wait_send()
    keep_head.wait()
    keep_out.wait()


def gather_project(tokens, packed, w_out, small, cosine, sine):
    outer = lax.axis_size("wt") // INNER
    seq_count = lax.axis_size("seq")
    rows, width = tokens.shape
    share, head_width = packed.shape
    slow_copies, last_copies = plane_copies(seq_count)
    each = slow_copies + last_copies
    small_copies = 2 ** len(inner_bits()) - 1
    copies = 3 * (outer - 1) + (outer + 1) * each + small_copies
    vmem = pl.BlockSpec(memory_space=pltpu.VMEM)
    anywhere = pl.BlockSpec(memory_space=pl.ANY)
    sent = 2 * outer * INNER * share * (head_width + w_out.shape[1])
    return pl.pallas_call(
        functools.partial(gather_kernel, outer, seq_count),
        in_specs=[vmem] * 6,
        out_specs=[vmem, vmem, vmem, anywhere, anywhere],
        out_shape=[
            jax.ShapeDtypeStruct((rows, width), low),
            jax.ShapeDtypeStruct((rows, head_width), low),
            jax.ShapeDtypeStruct((8, head_width), full),
            jax.ShapeDtypeStruct((outer, INNER, share, head_width), low),
            jax.ShapeDtypeStruct((outer, INNER, share, w_out.shape[1]), low),
        ],
        scratch_shapes=[
            pltpu.VMEM((outer, INNER, share, head_width), low),
            pltpu.VMEM((outer, INNER, share, w_out.shape[1]), low),
            pltpu.VMEM((outer, INNER, small.shape[0], small.shape[1]), low),
            pltpu.SemaphoreType.DMA((copies,)),
            pltpu.SemaphoreType.DMA((copies,)),
            pltpu.SemaphoreType.DMA((3,)),
        ],
        compiler_params=pltpu.CompilerParams(
            collective_id=1, has_side_effects=True, vmem_limit_bytes=48 << 20
        ),
        cost_estimate=pl.CostEstimate(
            flops=2 * rows * width * head_width * 8, bytes_accessed=2 * sent, transcendentals=0
        ),
        name="gather_project",
    )(tokens, packed, w_out, small, cosine, sine)


def split_kernel(outer, seq_count, own, info_ref, gate_ref, up_ref, o_ref):
    inner = info_ref[1]
    width = outer * own
    padded = o_ref.shape[2] // 2
    for s in range(seq_count):
        @pl.when(info_ref[0] == s)
        def _():
            for q in range(INNER):
                place = jnp.bitwise_xor(inner, q)
                for k, ref in enumerate((gate_ref, up_ref)):
                    for o in range(outer):
                        at = ((o * INNER + q) * seq_count + s) * own
                        to = k * padded + o * own
                        o_ref[place, :, to : to + own] = ref[:, at : at + own].astype(low)
                    if padded > width:
                        blank = jnp.zeros((o_ref.shape[1], padded - width), low)
                        o_ref[place, :, k * padded + width : (k + 1) * padded] = blank


def split_units(info, gate, up, outer, seq_count, own, padded):
    vmem = pl.BlockSpec(memory_space=pltpu.VMEM)
    return pl.pallas_call(
        functools.partial(split_kernel, outer, seq_count, own),
        in_specs=[pl.BlockSpec(memory_space=pltpu.SMEM), vmem, vmem],
        out_specs=vmem,
        out_shape=jax.ShapeDtypeStruct((INNER, gate.shape[0], 2 * padded), low),
        name="split_units",
    )(info, gate, up)


def join_kernel(outer, seq_count, own, info_ref, u_ref, gate_ref, up_ref):
    seq, inner = info_ref[0], info_ref[1]
    padded = u_ref.shape[3] // 2
    for s in range(seq_count):
        for q in range(INNER):
            block = u_ref[jnp.bitwise_xor(seq, s), jnp.bitwise_xor(inner, q)].astype(full)
            for k, ref in enumerate((gate_ref, up_ref)):
                for o in range(outer):
                    at = ((o * INNER + q) * seq_count + s) * own
                    source = k * padded + o * own
                    ref[:, at : at + own] = block[:, source : source + own]


def join_units(info, units, outer, own):
    seq_count, _, rows, _ = units.shape
    vmem = pl.BlockSpec(memory_space=pltpu.VMEM)
    shape = jax.ShapeDtypeStruct((rows, outer * INNER * seq_count * own), full)
    return pl.pallas_call(
        functools.partial(join_kernel, outer, seq_count, own),
        in_specs=[pl.BlockSpec(memory_space=pltpu.SMEM), vmem],
        out_specs=[vmem, vmem],
        out_shape=[shape, shape],
        name="join_units",
    )(info, units)


def after(value, *others):
    return lax.optimization_barrier((value, *others))[0]


def shown(kpos_ref, rows, keys):
    places = lax.broadcasted_iota(jnp.int32, (rows, keys), 0)
    return kpos_ref[...] <= places


def fwd_kernel(kpos_ref, q_ref, k_ref, v_ref, o_ref):
    rows, keys = q_ref.shape[0], k_ref.shape[0]
    scores = (
        lax.dot_general(
            q_ref[...], k_ref[...], (((1,), (1,)), ((), ())), preferred_element_type=full
        )
        * scale
    )
    scores = jnp.where(shown(kpos_ref, rows, keys), scores, masked_score)
    top = jnp.max(scores, axis=-1, keepdims=True)
    weights = jnp.exp(scores - top)
    total = jnp.sum(weights, axis=-1, keepdims=True)
    probs = (weights * (1.0 / total)).astype(low)
    o_ref[...] = jnp.dot(probs, v_ref[...], preferred_element_type=full).astype(low)


def attend_forward(kpos, qkv, pairs):
    rows = qkv.shape[0]
    keys = pairs.shape[0]
    group = HEADS // KV_HEADS
    return pl.pallas_call(
        fwd_kernel,
        grid=(HEADS,),
        in_specs=[
            pl.BlockSpec((1, keys), lambda h: (0, 0)),
            pl.BlockSpec((rows, HEAD_DIM), lambda h: (0, h)),
            pl.BlockSpec((keys, HEAD_DIM), lambda h: (0, h // group)),
            pl.BlockSpec((keys, HEAD_DIM), lambda h: (0, KV_HEADS + h // group)),
        ],
        out_specs=pl.BlockSpec((rows, HEAD_DIM), lambda h: (0, h)),
        out_shape=jax.ShapeDtypeStruct((rows, HEADS * HEAD_DIM), low),
        cost_estimate=pl.CostEstimate(
            flops=4 * rows * keys * HEADS * HEAD_DIM * 3,
            bytes_accessed=4 * rows * HEADS * HEAD_DIM + 4 * keys * KV_HEADS * HEAD_DIM,
            transcendentals=rows * keys * HEADS,
        ),
        name="attend_forward",
    )(kpos, qkv, pairs, pairs)


def bwd_kernel(kpos_ref, cos_ref, sin_ref, q_ref, k_ref, v_ref, g_ref, dq_ref, dk_ref, dv_ref):
    rows, keys = q_ref.shape[0], k_ref.shape[0]
    group = HEADS // KV_HEADS
    head = pl.program_id(0)
    queries, key, value, grad = q_ref[...], k_ref[...], v_ref[...], g_ref[...]
    scores = (
        lax.dot_general(queries, key, (((1,), (1,)), ((), ())), preferred_element_type=full)
        * scale
    )
    scores = jnp.where(shown(kpos_ref, rows, keys), scores, masked_score)
    top = jnp.max(scores, axis=-1, keepdims=True)
    weights = jnp.exp(scores - top)
    total = jnp.sum(weights, axis=-1, keepdims=True)
    probs = weights * (1.0 / total)
    prob_grad = lax.dot_general(
        grad, value, (((1,), (1,)), ((), ())), preferred_element_type=full
    )
    inner = jnp.sum(probs * prob_grad, axis=-1, keepdims=True)
    score_grad = (probs * (prob_grad - inner)).astype(low)
    dv = lax.dot_general(
        probs.astype(low), grad, (((0,), (0,)), ((), ())), preferred_element_type=full
    )
    dk = (
        lax.dot_general(
            score_grad, queries, (((0,), (0,)), ((), ())), preferred_element_type=full
        )
        * scale
    )
    dq = jnp.dot(score_grad, key, preferred_element_type=full) * scale
    turned = dq * cos_ref[...] - pltpu.roll(dq, HEAD_DIM // 2, 1) * sin_ref[...]
    dq_ref[...] = turned.astype(low)

    @pl.when(head % group == 0)
    def _():
        dk_ref[...] = dk
        dv_ref[...] = dv

    @pl.when(head % group != 0)
    def _():
        dk_ref[...] += dk
        dv_ref[...] += dv


def attend_backward(kpos, cosine, sine, qkv, pairs, grad):
    rows = qkv.shape[0]
    keys = pairs.shape[0]
    group = HEADS // KV_HEADS
    width = KV_HEADS * HEAD_DIM
    return pl.pallas_call(
        bwd_kernel,
        grid=(HEADS,),
        in_specs=[
            pl.BlockSpec((1, keys), lambda h: (0, 0)),
            pl.BlockSpec((rows, HEAD_DIM), lambda h: (0, 0)),
            pl.BlockSpec((rows, HEAD_DIM), lambda h: (0, 0)),
            pl.BlockSpec((rows, HEAD_DIM), lambda h: (0, h)),
            pl.BlockSpec((keys, HEAD_DIM), lambda h: (0, h // group)),
            pl.BlockSpec((keys, HEAD_DIM), lambda h: (0, KV_HEADS + h // group)),
            pl.BlockSpec((rows, HEAD_DIM), lambda h: (0, h)),
        ],
        out_specs=[
            pl.BlockSpec((rows, HEAD_DIM), lambda h: (0, h)),
            pl.BlockSpec((keys, HEAD_DIM), lambda h: (0, h // group)),
            pl.BlockSpec((keys, HEAD_DIM), lambda h: (0, h // group)),
        ],
        out_shape=[
            jax.ShapeDtypeStruct((rows, HEADS * HEAD_DIM), low),
            jax.ShapeDtypeStruct((keys, width), full),
            jax.ShapeDtypeStruct((keys, width), full),
        ],
        cost_estimate=pl.CostEstimate(
            flops=10 * rows * keys * HEADS * HEAD_DIM * 3,
            bytes_accessed=8 * rows * HEADS * HEAD_DIM + 12 * keys * width,
            transcendentals=rows * keys * HEADS,
        ),
        name="attend_backward",
    )(kpos, cosine, sine, qkv, pairs, pairs, grad)


def body(
    tokens, lengths, attn_gain, w_query, b_query, w_key, b_key, w_value, b_value, w_out,
    ffn_gain, w_gate, w_up, w_down, cotangent,
):
    slot_count, rows, width = tokens.shape
    seq_count = lax.axis_size("seq")
    wt_count = lax.axis_size("wt")
    outer = wt_count // INNER
    seq_here = lax.axis_index("seq")
    inner_here = lax.axis_index("wt") % INNER
    line = [[o * INNER + i for o in range(outer)] for i in range(INNER)]
    hops_a, hops_b = plane_hops(seq_count)
    plane = INNER * seq_count
    share = w_query.shape[0]
    bias_q, bias_k = b_query.shape[0], b_key.shape[0]
    query_width = HEADS * HEAD_DIM
    pair_width = KV_HEADS * HEAD_DIM
    head_width = query_width + 2 * pair_width
    ff_own = w_down.shape[0] // seq_count
    ff_here = outer * ff_own
    ff_pad = -(-ff_here // 128) * 128

    flat = tokens.astype(full).reshape(rows, width)
    places = seq_here * rows + jnp.arange(rows, dtype=jnp.int32)
    keep = (places < lengths[0])[:, None]
    upstream_low = jnp.where(keep, cotangent.reshape(rows, width), jnp.zeros((), low))

    def line_gather(value):
        return lax.all_gather(value, "wt", axis=0, axis_index_groups=line, tiled=False)

    def line_reduce(value):
        return lax.psum_scatter(
            value, "wt", scatter_dimension=0, axis_index_groups=line, tiled=False
        )

    def reduce_weight(value):
        count, wide = value.shape[1:]
        half = wide // seq_count // 2
        split = value.reshape(outer, INNER, count, seq_count, 2, half)
        done = []
        for k, hops in enumerate((hops_a, hops_b)):
            piece = split[:, :, :, :, k].transpose(1, 3, 0, 2, 4)
            piece = piece.reshape(plane, outer, count, half)
            order = plane_order(hops, seq_count)
            back = [order.index(p) for p in range(plane)]
            table = jnp.asarray(back, dtype=jnp.int32)
            me = rank_of(hops)
            placed = [to_place(piece, table[me ^ p]) for p in range(plane)]
            done.append(reduce_hops(jnp.stack(placed), hops))
        lined = jnp.concatenate(done, axis=-1).astype(low)
        mine = line_reduce(lined)
        return seq_columns(mine)

    def seq_gather(value):
        stacked = gather_hops(value, bits_of("seq", seq_count))
        return jnp.stack([to_place(stacked, seq_here ^ p) for p in range(seq_count)])

    def seq_columns(value):
        got = seq_gather(value)
        return got.transpose(1, 0, 2).reshape(value.shape[0], -1)

    info = jnp.stack([seq_here, inner_here]).astype(jnp.int32)
    down_own = lax.dynamic_slice_in_dim(w_down, seq_here * ff_own, ff_own, axis=0).astype(low)
    down_w = line_gather(down_own).reshape(ff_here, width)

    def inner_swap(value, distance):
        count = lax.axis_size("wt")
        return lax.ppermute(value, "wt", [(i, i ^ distance) for i in range(count)])

    def inner_exchange(value):
        got = [value[0]] + [inner_swap(value[d], d) for d in range(1, INNER)]
        return jnp.stack(got)

    stacked = inner_exchange(split_units(info, w_gate, w_up, outer, seq_count, ff_own, ff_pad))
    block = jnp.stack([to_place(stacked, inner_here ^ p) for p in range(INNER)])
    block = block.reshape(INNER * share, 2 * ff_pad)
    units_w = line_gather(block).reshape(width, 2 * ff_pad)
    down_w = jnp.pad(down_w, ((0, ff_pad - ff_here), (0, 0)))

    bias_q, bias_k = b_query.shape[0], b_key.shape[0]
    half = HEAD_DIM // 2
    inverse = 10000.0 ** (-jnp.arange(half, dtype=full) / half)
    angle = places.astype(full)[:, None] * inverse[None, :]
    cosine = jnp.cos(angle)
    sine = jnp.sin(angle)
    cosine = jnp.concatenate([cosine, cosine], axis=1)
    sine = jnp.concatenate([-sine, sine], axis=1)

    def line_of(vector):
        return jnp.pad(vector, (0, HEAD_DIM - vector.shape[0]))

    small = jnp.stack([line_of(v) for v in (attn_gain, b_query, b_key, b_value, ffn_gain)])
    small = jnp.pad(small.astype(low), ((0, 11), (0, 0)))
    packed = jnp.concatenate([w_query, w_key, w_value], axis=1).astype(low)
    normed_low, qkv, vectors, head_all, out_all = gather_project(
        after(tokens, block, down_own).reshape(rows, width),
        packed, w_out.astype(low), small, cosine, sine,
    )
    head_w = head_all.reshape(width, head_width)
    out_w = out_all.reshape(query_width, width)
    gain_one = vectors[0, :width]
    gain_two = vectors[2, :width]

    seq_hops = bits_of("seq", seq_count)
    pairs = gather_hops(qkv[:, query_width:], seq_hops).reshape(SLOT, 2 * pair_width)
    distance = jnp.arange(SLOT, dtype=jnp.int32)
    key_place = (seq_here ^ (distance // rows)) * rows + distance % rows
    kpos = jnp.where(key_place < lengths[0], key_place - seq_here * rows, far_place)[None, :]
    mixed = attend_forward(kpos, qkv, pairs)
    resid = flat + product(mixed, out_w)
    normed_two, factor_two = norm_rows(resid, gain_two)
    normed_two_low = normed_two.astype(low)

    def spread(block):
        part_a, part_b = gather_plane(block, seq_count)
        return jnp.stack([part_a, part_b]).reshape(plane * rows, width)

    def halves(partial):
        return list(partial.astype(low).reshape(2, plane, rows // 2, width))

    def hop_halves(parts, stage):
        return [reduce_hop(part, hops[stage]) for part, hops in zip(parts, (hops_a, hops_b))]

    def last_halves(parts):
        got = [reduce_hops(part, hops[:1]) for part, hops in zip(parts, (hops_a, hops_b))]
        return jnp.concatenate(got, axis=0)

    stages = list(range(len(hops_a)))[:0:-1]
    grad_all = spread(after(upstream_low, vectors))
    hidden_grad = product_right(grad_all, down_w)
    rows_all = spread(normed_two_low)
    both = product(rows_all, units_w)
    gate, upper = both[:, :ff_pad], both[:, ff_pad:]
    sigma = jax.nn.sigmoid(gate)
    hidden = (gate * sigma * upper).astype(low)
    gate_grad = (hidden_grad * upper * sigma * (1.0 + gate * (1.0 - sigma))).astype(low)
    up_grad = (hidden_grad * gate * sigma).astype(low)
    units_grad = jnp.concatenate([gate_grad, up_grad], axis=1)
    back = halves(product_right(units_grad, units_w))
    down_grad = product_left(after(hidden, back[0]), grad_all).astype(low)[:ff_here]
    down_line = line_reduce(down_grad.reshape(outer, ff_own, width))
    back = hop_halves(back, stages[0])
    rows_late, grad_late = lax.optimization_barrier((rows_all, units_grad, back, down_grad))[:2]
    units_w_grad = product_left(rows_late, grad_late).astype(low)
    units_line = line_reduce(units_w_grad.reshape(outer, INNER * share, 2 * ff_pad))
    for stage in stages[1:]:
        back = hop_halves(back, stage)
    hidden_late = after(hidden, back, units_w_grad)
    forth = halves(product(hidden_late, down_w))
    normed_two_grad = last_halves(back)
    forth[0] = after(forth[0], normed_two_grad)
    for stage in stages:
        forth = hop_halves(forth, stage)
    result = resid + last_halves(forth)
    layer_out = jnp.where(keep, result, 0.0).astype(low).reshape(slot_count, rows, width)

    blocks = units_line.reshape(INNER, share, 2 * ff_pad)
    sent = jnp.stack([to_place(blocks, inner_here ^ d) for d in range(INNER)])
    gate_out, up_out = join_units(
        info, gather_hops(inner_exchange(sent), seq_hops), outer, ff_own
    )
    down_out = seq_gather(down_line).reshape(seq_count * ff_own, width).astype(full)

    upstream = upstream_low.astype(full)
    resid_norm_grad, gain_two_grad = norm_back(resid, factor_two, gain_two, normed_two_grad)
    resid_grad = upstream + resid_norm_grad
    attn_grad = resid_grad.astype(low)
    mixed_grad = product_right(attn_grad, out_w).astype(low)
    out_w_grad = product_left(mixed, attn_grad).astype(low)
    out_w_out = reduce_weight(out_w_grad.reshape(wt_count, -1, width)).astype(full)
    query_grad, key_part, value_part = attend_backward(
        kpos, cosine, sine, qkv, pairs, mixed_grad
    )
    pair_part = jnp.concatenate([key_part, value_part], axis=1)
    pair_sum = reduce_hops(
        pair_part.reshape(seq_count, rows, 2 * pair_width).astype(low), seq_hops
    )
    key_rot_grad = pair_sum[:, :pair_width].reshape(rows, KV_HEADS, HEAD_DIM)
    turned = jnp.concatenate([key_rot_grad[..., half:], key_rot_grad[..., :half]], axis=-1)
    key_grad = key_rot_grad * cosine[:, None, :] - turned * sine[:, None, :]
    head_grad = jnp.concatenate(
        [query_grad, key_grad.reshape(rows, pair_width).astype(low),
         pair_sum[:, pair_width:].astype(low)],
        axis=1,
    )
    head_w_grad = product_left(normed_low, head_grad).astype(low)
    head_b_grad = jnp.sum(head_grad.astype(full), axis=0)
    normed_grad = product_right(head_grad, head_w)
    factor_one = lax.rsqrt(jnp.mean(flat * flat, axis=-1, keepdims=True) + epsilon)
    input_norm_grad, gain_one_grad = norm_back(flat, factor_one, gain_one, normed_grad)
    input_grad = (resid_grad + input_norm_grad).astype(low).reshape(slot_count, rows, width)

    edges = [0, share, share + bias_q]
    edges += [edges[-1] + bias_k, edges[-1] + 2 * bias_k]

    def parts(vector):
        return vector.reshape(wt_count, -1)

    small_grad = jnp.concatenate(
        [
            parts(gain_one_grad),
            parts(head_b_grad[:query_width]),
            parts(head_b_grad[query_width : query_width + pair_width]),
            parts(head_b_grad[query_width + pair_width :]),
            parts(gain_two_grad),
        ],
        axis=1,
    ).astype(low)
    extra = jnp.pad(
        small_grad[:, None, :],
        ((0, 0), (0, EXTRA - 1), (0, head_width - small_grad.shape[1])),
    )
    head_sum = reduce_weight(
        jnp.concatenate([head_w_grad.reshape(wt_count, share, head_width), extra], axis=1)
    ).astype(full)
    heads_out = head_sum[:share]
    small_out = head_sum[share]
    return (
        layer_out,
        input_grad,
        small_out[: edges[1]],
        heads_out[:, :query_width],
        small_out[edges[1] : edges[2]],
        heads_out[:, query_width : query_width + pair_width],
        small_out[edges[2] : edges[3]],
        heads_out[:, query_width + pair_width :],
        small_out[edges[3] : edges[4]],
        out_w_out,
        small_out[edges[4] : edges[4] + ffn_gain.shape[0]],
        gate_out,
        up_out,
        down_out,
    )


def solution(mesh):
    by_wt = P("wt")
    by_row = P("wt", None)
    by_token = P("wt", "seq", None)
    return jax.shard_map(
        body,
        mesh=mesh,
        in_specs=(
            by_token, by_wt, by_wt, by_row, by_wt, by_row, by_wt, by_row, by_wt, by_row,
            by_wt, by_row, by_row, by_row, by_token,
        ),
        out_specs=(
            by_token, by_token, by_wt, by_row, by_wt, by_row, by_wt, by_row, by_wt, by_row,
            by_wt, by_row, by_row, by_row,
        ),
        check_vma=False,
    )
```

```python
import functools
import math

import jax
import jax.numpy as jnp
from jax import lax
from jax.experimental import pallas as pl
from jax.experimental.pallas import tpu as pltpu
from jax.sharding import PartitionSpec as P


HEADS = 12
KV_HEADS = 2
HEAD_DIM = 128
SLOT = 1024
INNER = 4
EXTRA = 8

epsilon = 1e-06
masked_score = -1e30
far_place = 1 << 30
scale = 1.0 / math.sqrt(HEAD_DIM)
low = jnp.bfloat16
full = jnp.float32


def product(left, right):
    return jnp.dot(left, right, preferred_element_type=full)


def product_left(left, right):
    return lax.dot_general(left, right, (((0,), (0,)), ((), ())), preferred_element_type=full)


def product_right(left, right):
    return lax.dot_general(left, right, (((1,), (1,)), ((), ())), preferred_element_type=full)


def norm_rows(values, gain):
    factor = lax.rsqrt(jnp.mean(values * values, axis=-1, keepdims=True) + epsilon)
    return (values * factor * gain, factor)


def norm_back(values, factor, gain, upstream):
    weighted = upstream * gain
    inner = jnp.mean(weighted * values, axis=-1, keepdims=True)
    grad_in = factor * weighted - values * (factor * factor * factor) * inner
    grad_gain = jnp.sum(upstream * values * factor, axis=0)
    return (grad_in, grad_gain)


def swap(value, hop):
    axis, bit = hop
    count = lax.axis_size(axis)
    return lax.ppermute(value, axis, [(i, i ^ bit) for i in range(count)])


def gather_hops(block, hops):
    held = block[None]
    for hop in hops:
        held = jnp.concatenate([held, swap(held, hop)], axis=0)
    return held


def reduce_hop(held, hop):
    half = held.shape[0] // 2
    other = swap(held[half:], hop)
    return (held[:half].astype(full) + other.astype(full)).astype(low)


def reduce_hops(held, hops):
    for k in range(len(hops) - 1, 0, -1):
        held = reduce_hop(held, hops[k])
    return held[0].astype(full) + swap(held[1], hops[0]).astype(full)


def bits_of(axis, count):
    found, bit = [], 1
    while bit < count:
        found.append((axis, bit))
        bit *= 2
    return found


def plane_hops(seq_count):
    inner = bits_of("wt", INNER)
    seq = bits_of("seq", seq_count)
    slow = inner[1:] + seq
    return (slow + inner[:1], slow[::-1] + inner[:1])


def rank_of(hops):
    place = jnp.int32(0)
    for k, (axis, bit) in enumerate(hops):
        here = (lax.axis_index(axis) // bit) % 2
        place = place + here * (1 << k)
    return place


def plane_order(hops, count):
    order = []
    for inner in range(INNER):
        for seq in range(count):
            place = 0
            for k, (axis, bit) in enumerate(hops):
                source = inner if axis == "wt" else seq
                place |= ((source // bit) % 2) << k
            order.append(place)
    return order


def to_place(stacked, place):
    return lax.dynamic_index_in_dim(stacked, place, 0, keepdims=False)


def flip(index, bit):
    return index + bit - 2 * bit * ((index // bit) % 2)


def flip_all(index, distance):
    bit = 1
    while bit <= distance:
        if distance & bit:
            index = flip(index, bit)
        bit *= 2
    return index


def inner_bits():
    return [bit for _, bit in bits_of("wt", INNER)]


def meet(peers):
    barrier = pltpu.get_barrier_semaphore()
    for peer in peers:
        pl.semaphore_signal(
            barrier, inc=1, device_id=peer, device_id_type=pl.DeviceIdType.MESH
        )
    pl.semaphore_wait(barrier, len(peers))


class Sender:
    def __init__(self, send_sems, recv_sems):
        self.sems = (send_sems, recv_sems)
        self.copies = []

    def start(self, source, target, peer):
        at = len(self.copies)
        copy = pltpu.make_async_remote_copy(
            src_ref=source,
            dst_ref=target,
            send_sem=self.sems[0].at[at],
            recv_sem=self.sems[1].at[at],
            device_id=peer,
            device_id_type=pl.DeviceIdType.MESH,
        )
        copy.start()
        self.copies.append(copy)
        return copy


def subsets(hops):
    found = [(0, 0)]
    for axis, bit in hops:
        more = [(a ^ bit, b) if axis == "wt" else (a, b ^ bit) for a, b in found]
        found = found + more
    return found


def plane_copies(seq_count):
    hops_a, _ = plane_hops(seq_count)
    slow = len(hops_a) - 1
    return (2 * (2**slow - 1), len(set(a for a, _ in subsets(hops_a[:-1]))))


def gather_kernel(
    outer, seq_count, x_ref, p_ref, wo_ref, s_ref, cos_ref, sin_ref,
    normed_ref, qkv_ref, vec_ref, head_ref, out_ref,
    w_scr, o_scr, s_scr, send_sems, recv_sems, local_sems,
):
    share, head_width = p_ref.shape
    width = x_ref.shape[1]
    wt, seq = lax.axis_index("wt"), lax.axis_index("seq")
    line, inner = wt // INNER, wt % INNER
    hops = plane_hops(seq_count)
    slow = len(hops[0]) - 1
    peers = [(flip_all(line, d) * INNER + inner, seq) for d in range(1, outer)]
    peers += [(wt - inner + flip(inner, bit), seq) for bit in inner_bits()]
    peers += [(wt, flip(seq, bit)) for _, bit in bits_of("seq", seq_count)]

    def own_columns(total):
        wide = total // seq_count
        return pl.ds(pl.multiple_of(seq * wide, 128), wide)

    fill = [
        pltpu.make_async_copy(
            ref.at[:, own_columns(ref.shape[1])],
            scratch.at[line, inner, :, own_columns(ref.shape[1])],
            local_sems.at[k],
        )
        for k, (ref, scratch) in enumerate(((p_ref, w_scr), (wo_ref, o_scr)))
    ] + [
        pltpu.make_async_copy(s_ref, s_scr.at[line, inner], local_sems.at[2]),
    ]
    for copy in fill:
        copy.start()
    meet(peers)
    out = Sender(send_sems, recv_sems)

    def hop_peer(hop):
        axis, bit = hop
        if axis == "wt":
            return (wt - inner + flip(inner, bit), seq)
        return (wt, flip(seq, bit))

    def columns(total, part, half):
        wide = total // seq_count
        first = -(-wide // 256) * 128
        start = part * wide + half * first
        return pl.ds(pl.multiple_of(start, 128), wide - first if half else first)

    def start_line(source, scratch, narrow):
        total = source.shape[1]
        copies = [None]
        for d in range(1, outer):
            if narrow:
                part = own_columns(total)
                pair = (source.at[:, part], scratch.at[line, inner, :, part])
            else:
                pair = (source, scratch.at[line, inner])
            copies.append(out.start(*pair, (flip_all(line, d) * INNER + inner, seq)))
        return copies

    small_line = start_line(s_ref, s_scr, False)
    head_line = start_line(p_ref, w_scr, True)
    out_line = start_line(wo_ref, o_scr, True)

    def start_stage(scratch, at, stage):
        total = scratch.shape[-1]
        copies = []
        if stage < slow:
            for half in range(2):
                hop = hops[half][stage]
                for a, b in subsets(hops[half][:stage]):
                    place = scratch.at[
                        at, flip_all(inner, a), :, columns(total, flip_all(seq, b), half)
                    ]
                    copies.append(out.start(place, place, hop_peer(hop)))
            return copies
        for a in sorted(set(a for a, _ in subsets(hops[0][:slow]))):
            place = scratch.at[at, flip_all(inner, a)]
            copies.append(out.start(place, place, hop_peer(hops[0][slow])))
        return copies

    def arrive(copies):
        for copy in copies:
            if copy is not None:
                copy.wait_recv()

    for copy in fill:
        copy.wait()
    waiting = [[copy] for copy in head_line]
    small_wait = small_line
    for step in range(outer + slow + 1):
        for stage in range(slow + 1):
            d = step - stage
            if 0 <= d < outer:
                arrive(waiting[d])
                waiting[d] = start_stage(w_scr, flip_all(line, d), stage)
        if step == 0:
            arrive(small_wait)
            small_wait = []
        if step < len(inner_bits()):
            arrive(small_wait)
            bit = inner_bits()[::-1][step]
            small_wait = []
            for a, _ in subsets([("wt", b) for b in inner_bits()[::-1][:step]]):
                place = s_scr.at[:, flip_all(inner, a)]
                small_wait.append(out.start(place, place, hop_peer(("wt", bit))))
    arrive(small_wait)
    arrive(out_line)
    out_wait = start_stage(o_scr, slice(None), 0)

    count = outer * INNER
    bias_k = share * KV_HEADS * HEAD_DIM // (HEADS * HEAD_DIM)
    query_width = HEADS * HEAD_DIM
    pair_width = KV_HEADS * HEAD_DIM
    vec_ref[...] = jnp.zeros_like(vec_ref)
    for k in range(count):
        small = s_scr[k // INNER, k % INNER].astype(full)
        at = k * share
        vec_ref[0:1, at : at + share] = small[0:1, :share]
        vec_ref[1:2, at : at + share] = small[1:2, :share]
        at = query_width + k * bias_k
        vec_ref[1:2, at : at + bias_k] = small[2:3, :bias_k]
        at = query_width + pair_width + k * bias_k
        vec_ref[1:2, at : at + bias_k] = small[3:4, :bias_k]
        at = k * share
        vec_ref[2:3, at : at + share] = small[4:5, :share]

    values = x_ref[...].astype(full)
    factor = lax.rsqrt(jnp.mean(values * values, axis=-1, keepdims=True) + epsilon)
    normed_ref[...] = (values * factor * vec_ref[0:1, :width]).astype(low)
    for d in range(outer):
        arrive(waiting[d])
    keep_head = pltpu.make_async_copy(w_scr, head_ref, local_sems.at[0])
    keep_head.start()
    wide = 2 * HEAD_DIM
    blocks = head_width // wide

    def project(at):
        weights = w_scr[:, :, :, pl.ds(at, wide)].reshape(width, wide)
        return (
            jnp.dot(normed_ref[...], weights, preferred_element_type=full)
            + vec_ref[1:2, pl.ds(at, wide)]
        )

    def turn_block(k):
        at = pl.multiple_of(k * wide, wide)
        got = project(at)
        for j in range(2):
            part = got[:, j * HEAD_DIM : (j + 1) * HEAD_DIM]
            turned = part * cos_ref[...] + pltpu.roll(part, HEAD_DIM // 2, 1) * sin_ref[...]
            where = pl.multiple_of(at + j * HEAD_DIM, HEAD_DIM)
            qkv_ref[:, pl.ds(where, HEAD_DIM)] = turned.astype(low)

    turned_blocks = blocks - pair_width // wide
    marks = [turned_blocks * (k + 1) // (slow + 1) for k in range(slow + 1)]
    begin = 0
    for stage in range(slow + 1):
        @pl.loop(begin, marks[stage])
        def _(k):
            turn_block(k)

        begin = marks[stage]
        arrive(out_wait)
        out_wait = start_stage(o_scr, slice(None), stage + 1) if stage < slow else []
    for k in range(turned_blocks, blocks):
        qkv_ref[:, k * wide : (k + 1) * wide] = project(k * wide).astype(low)
    keep_out = pltpu.make_async_copy(o_scr, out_ref, local_sems.at[1])
    keep_out.start()
    for copy in out.copies:
        copy.wait_send()
    keep_head.wait()
    keep_out.wait()


def gather_project(tokens, packed, w_out, small, cosine, sine):
    outer = lax.axis_size("wt") // INNER
    seq_count = lax.axis_size("seq")
    rows, width = tokens.shape
    share, head_width = packed.shape
    slow_copies, last_copies = plane_copies(seq_count)
    each = slow_copies + last_copies
    small_copies = 2 ** len(inner_bits()) - 1
    copies = 3 * (outer - 1) + (outer + 1) * each + small_copies
    vmem = pl.BlockSpec(memory_space=pltpu.VMEM)
    anywhere = pl.BlockSpec(memory_space=pl.ANY)
    sent = 2 * outer * INNER * share * (head_width + w_out.shape[1])
    return pl.pallas_call(
        functools.partial(gather_kernel, outer, seq_count),
        in_specs=[vmem] * 6,
        out_specs=[vmem, vmem, vmem, anywhere, anywhere],
        out_shape=[
            jax.ShapeDtypeStruct((rows, width), low),
            jax.ShapeDtypeStruct((rows, head_width), low),
            jax.ShapeDtypeStruct((8, head_width), full),
            jax.ShapeDtypeStruct((outer, INNER, share, head_width), low),
            jax.ShapeDtypeStruct((outer, INNER, share, w_out.shape[1]), low),
        ],
        scratch_shapes=[
            pltpu.VMEM((outer, INNER, share, head_width), low),
            pltpu.VMEM((outer, INNER, share, w_out.shape[1]), low),
            pltpu.VMEM((outer, INNER, small.shape[0], small.shape[1]), low),
            pltpu.SemaphoreType.DMA((copies,)),
            pltpu.SemaphoreType.DMA((copies,)),
            pltpu.SemaphoreType.DMA((3,)),
        ],
        compiler_params=pltpu.CompilerParams(
            collective_id=1, has_side_effects=True, vmem_limit_bytes=48 << 20
        ),
        cost_estimate=pl.CostEstimate(
            flops=2 * rows * width * head_width * 8, bytes_accessed=2 * sent, transcendentals=0
        ),
        name="gather_project",
    )(tokens, packed, w_out, small, cosine, sine)


def split_kernel(outer, seq_count, own, info_ref, gate_ref, up_ref, o_ref):
    inner = info_ref[1]
    width = outer * own
    padded = o_ref.shape[2] // 2
    for s in range(seq_count):
        @pl.when(info_ref[0] == s)
        def _():
            for q in range(INNER):
                place = jnp.bitwise_xor(inner, q)
                for k, ref in enumerate((gate_ref, up_ref)):
                    for o in range(outer):
                        at = ((o * INNER + q) * seq_count + s) * own
                        to = k * padded + o * own
                        o_ref[place, :, to : to + own] = ref[:, at : at + own].astype(low)
                    if padded > width:
                        blank = jnp.zeros((o_ref.shape[1], padded - width), low)
                        o_ref[place, :, k * padded + width : (k + 1) * padded] = blank


def split_units(info, gate, up, outer, seq_count, own, padded):
    vmem = pl.BlockSpec(memory_space=pltpu.VMEM)
    return pl.pallas_call(
        functools.partial(split_kernel, outer, seq_count, own),
        in_specs=[pl.BlockSpec(memory_space=pltpu.SMEM), vmem, vmem],
        out_specs=vmem,
        out_shape=jax.ShapeDtypeStruct((INNER, gate.shape[0], 2 * padded), low),
        name="split_units",
    )(info, gate, up)


def join_kernel(outer, seq_count, own, info_ref, u_ref, gate_ref, up_ref):
    seq, inner = info_ref[0], info_ref[1]
    padded = u_ref.shape[3] // 2
    for s in range(seq_count):
        for q in range(INNER):
            block = u_ref[jnp.bitwise_xor(seq, s), jnp.bitwise_xor(inner, q)].astype(full)
            for k, ref in enumerate((gate_ref, up_ref)):
                for o in range(outer):
                    at = ((o * INNER + q) * seq_count + s) * own
                    source = k * padded + o * own
                    ref[:, at : at + own] = block[:, source : source + own]


def join_units(info, units, outer, own):
    seq_count, _, rows, _ = units.shape
    vmem = pl.BlockSpec(memory_space=pltpu.VMEM)
    shape = jax.ShapeDtypeStruct((rows, outer * INNER * seq_count * own), full)
    return pl.pallas_call(
        functools.partial(join_kernel, outer, seq_count, own),
        in_specs=[pl.BlockSpec(memory_space=pltpu.SMEM), vmem],
        out_specs=[vmem, vmem],
        out_shape=[shape, shape],
        name="join_units",
    )(info, units)


def after(value, *others):
    return lax.optimization_barrier((value, *others))[0]


def shown(kpos_ref, rows, keys):
    places = lax.broadcasted_iota(jnp.int32, (rows, keys), 0)
    return kpos_ref[...] <= places


def fwd_kernel(kpos_ref, q_ref, k_ref, v_ref, o_ref):
    rows, keys = q_ref.shape[0], k_ref.shape[0]
    scores = (
        lax.dot_general(
            q_ref[...], k_ref[...], (((1,), (1,)), ((), ())), preferred_element_type=full
        )
        * scale
    )
    scores = jnp.where(shown(kpos_ref, rows, keys), scores, masked_score)
    top = jnp.max(scores, axis=-1, keepdims=True)
    weights = jnp.exp(scores - top)
    total = jnp.sum(weights, axis=-1, keepdims=True)
    probs = (weights * (1.0 / total)).astype(low)
    o_ref[...] = jnp.dot(probs, v_ref[...], preferred_element_type=full).astype(low)


def attend_forward(kpos, qkv, pairs):
    rows = qkv.shape[0]
    keys = pairs.shape[0]
    group = HEADS // KV_HEADS
    return pl.pallas_call(
        fwd_kernel,
        grid=(HEADS,),
        in_specs=[
            pl.BlockSpec((1, keys), lambda h: (0, 0)),
            pl.BlockSpec((rows, HEAD_DIM), lambda h: (0, h)),
            pl.BlockSpec((keys, HEAD_DIM), lambda h: (0, h // group)),
            pl.BlockSpec((keys, HEAD_DIM), lambda h: (0, KV_HEADS + h // group)),
        ],
        out_specs=pl.BlockSpec((rows, HEAD_DIM), lambda h: (0, h)),
        out_shape=jax.ShapeDtypeStruct((rows, HEADS * HEAD_DIM), low),
        cost_estimate=pl.CostEstimate(
            flops=4 * rows * keys * HEADS * HEAD_DIM * 3,
            bytes_accessed=4 * rows * HEADS * HEAD_DIM + 4 * keys * KV_HEADS * HEAD_DIM,
            transcendentals=rows * keys * HEADS,
        ),
        name="attend_forward",
    )(kpos, qkv, pairs, pairs)


def bwd_kernel(kpos_ref, cos_ref, sin_ref, q_ref, k_ref, v_ref, g_ref, dq_ref, dk_ref, dv_ref):
    rows, keys = q_ref.shape[0], k_ref.shape[0]
    group = HEADS // KV_HEADS
    head = pl.program_id(0)
    queries, key, value, grad = q_ref[...], k_ref[...], v_ref[...], g_ref[...]
    scores = (
        lax.dot_general(queries, key, (((1,), (1,)), ((), ())), preferred_element_type=full)
        * scale
    )
    scores = jnp.where(shown(kpos_ref, rows, keys), scores, masked_score)
    top = jnp.max(scores, axis=-1, keepdims=True)
    weights = jnp.exp(scores - top)
    total = jnp.sum(weights, axis=-1, keepdims=True)
    probs = weights * (1.0 / total)
    prob_grad = lax.dot_general(
        grad, value, (((1,), (1,)), ((), ())), preferred_element_type=full
    )
    inner = jnp.sum(probs * prob_grad, axis=-1, keepdims=True)
    score_grad = (probs * (prob_grad - inner)).astype(low)
    dv = lax.dot_general(
        probs.astype(low), grad, (((0,), (0,)), ((), ())), preferred_element_type=full
    )
    dk = (
        lax.dot_general(
            score_grad, queries, (((0,), (0,)), ((), ())), preferred_element_type=full
        )
        * scale
    )
    dq = jnp.dot(score_grad, key, preferred_element_type=full) * scale
    turned = dq * cos_ref[...] - pltpu.roll(dq, HEAD_DIM // 2, 1) * sin_ref[...]
    dq_ref[...] = turned.astype(low)

    @pl.when(head % group == 0)
    def _():
        dk_ref[...] = dk
        dv_ref[...] = dv

    @pl.when(head % group != 0)
    def _():
        dk_ref[...] += dk
        dv_ref[...] += dv


def attend_backward(kpos, cosine, sine, qkv, pairs, grad):
    rows = qkv.shape[0]
    keys = pairs.shape[0]
    group = HEADS // KV_HEADS
    width = KV_HEADS * HEAD_DIM
    return pl.pallas_call(
        bwd_kernel,
        grid=(HEADS,),
        in_specs=[
            pl.BlockSpec((1, keys), lambda h: (0, 0)),
            pl.BlockSpec((rows, HEAD_DIM), lambda h: (0, 0)),
            pl.BlockSpec((rows, HEAD_DIM), lambda h: (0, 0)),
            pl.BlockSpec((rows, HEAD_DIM), lambda h: (0, h)),
            pl.BlockSpec((keys, HEAD_DIM), lambda h: (0, h // group)),
            pl.BlockSpec((keys, HEAD_DIM), lambda h: (0, KV_HEADS + h // group)),
            pl.BlockSpec((rows, HEAD_DIM), lambda h: (0, h)),
        ],
        out_specs=[
            pl.BlockSpec((rows, HEAD_DIM), lambda h: (0, h)),
            pl.BlockSpec((keys, HEAD_DIM), lambda h: (0, h // group)),
            pl.BlockSpec((keys, HEAD_DIM), lambda h: (0, h // group)),
        ],
        out_shape=[
            jax.ShapeDtypeStruct((rows, HEADS * HEAD_DIM), low),
            jax.ShapeDtypeStruct((keys, width), full),
            jax.ShapeDtypeStruct((keys, width), full),
        ],
        cost_estimate=pl.CostEstimate(
            flops=10 * rows * keys * HEADS * HEAD_DIM * 3,
            bytes_accessed=8 * rows * HEADS * HEAD_DIM + 12 * keys * width,
            transcendentals=rows * keys * HEADS,
        ),
        name="attend_backward",
    )(kpos, cosine, sine, qkv, pairs, pairs, grad)


def body(
    tokens, lengths, attn_gain, w_query, b_query, w_key, b_key, w_value, b_value, w_out,
    ffn_gain, w_gate, w_up, w_down, cotangent,
):
    slot_count, rows, width = tokens.shape
    seq_count = lax.axis_size("seq")
    wt_count = lax.axis_size("wt")
    outer = wt_count // INNER
    seq_here = lax.axis_index("seq")
    inner_here = lax.axis_index("wt") % INNER
    line = [[o * INNER + i for o in range(outer)] for i in range(INNER)]
    hops_a, hops_b = plane_hops(seq_count)
    plane = INNER * seq_count
    share = w_query.shape[0]
    bias_q, bias_k = b_query.shape[0], b_key.shape[0]
    query_width = HEADS * HEAD_DIM
    pair_width = KV_HEADS * HEAD_DIM
    head_width = query_width + 2 * pair_width
    ff_own = w_down.shape[0] // seq_count
    ff_here = outer * ff_own
    ff_pad = -(-ff_here // 128) * 128

    flat = tokens.astype(full).reshape(rows, width)
    places = seq_here * rows + jnp.arange(rows, dtype=jnp.int32)
    keep = (places < lengths[0])[:, None]
    upstream_low = jnp.where(keep, cotangent.reshape(rows, width), jnp.zeros((), low))

    def line_gather(value):
        return lax.all_gather(value, "wt", axis=0, axis_index_groups=line, tiled=False)

    def line_reduce(value):
        return lax.psum_scatter(
            value, "wt", scatter_dimension=0, axis_index_groups=line, tiled=False
        )

    def reduce_weight(value):
        count, wide = value.shape[1:]
        half = wide // seq_count // 2
        split = value.reshape(outer, INNER, count, seq_count, 2, half)
        done = []
        for k, hops in enumerate((hops_a, hops_b)):
            piece = split[:, :, :, :, k].transpose(1, 3, 0, 2, 4)
            piece = piece.reshape(plane, outer, count, half)
            order = plane_order(hops, seq_count)
            back = [order.index(p) for p in range(plane)]
            table = jnp.asarray(back, dtype=jnp.int32)
            me = rank_of(hops)
            placed = [to_place(piece, table[me ^ p]) for p in range(plane)]
            done.append(reduce_hops(jnp.stack(placed), hops))
        lined = jnp.concatenate(done, axis=-1).astype(low)
        mine = line_reduce(lined)
        return seq_columns(mine)

    def seq_gather(value):
        stacked = gather_hops(value, bits_of("seq", seq_count))
        return jnp.stack([to_place(stacked, seq_here ^ p) for p in range(seq_count)])

    def seq_columns(value):
        got = seq_gather(value)
        return got.transpose(1, 0, 2).reshape(value.shape[0], -1)

    info = jnp.stack([seq_here, inner_here]).astype(jnp.int32)
    down_own = lax.dynamic_slice_in_dim(w_down, seq_here * ff_own, ff_own, axis=0).astype(low)

    def inner_swap(value, distance):
        count = lax.axis_size("wt")
        return lax.ppermute(value, "wt", [(i, i ^ distance) for i in range(count)])

    def inner_exchange(value):
        got = [value[0]] + [inner_swap(value[d], d) for d in range(1, INNER)]
        return jnp.stack(got)

    stacked = inner_exchange(split_units(info, w_gate, w_up, outer, seq_count, ff_own, ff_pad))
    block = jnp.stack([to_place(stacked, inner_here ^ p) for p in range(INNER)])
    block = block.reshape(INNER * share, 2 * ff_pad)
    half = HEAD_DIM // 2
    inverse = 10000.0 ** (-jnp.arange(half, dtype=full) / half)
    angle = places.astype(full)[:, None] * inverse[None, :]
    cosine = jnp.cos(angle)
    sine = jnp.sin(angle)
    cosine = jnp.concatenate([cosine, cosine], axis=1)
    sine = jnp.concatenate([-sine, sine], axis=1)

    def line_of(vector):
        return jnp.pad(vector, (0, HEAD_DIM - vector.shape[0]))

    small = jnp.stack([line_of(v) for v in (attn_gain, b_query, b_key, b_value, ffn_gain)])
    small = jnp.pad(small.astype(low), ((0, 11), (0, 0)))
    packed = jnp.concatenate([w_query, w_key, w_value], axis=1).astype(low)
    normed_low, qkv, vectors, head_all, out_all = gather_project(
        tokens.reshape(rows, width),
        packed, w_out.astype(low), small, cosine, sine,
    )
    head_w = head_all.reshape(width, head_width)
    out_w = out_all.reshape(query_width, width)
    gain_one = vectors[0, :width]
    gain_two = vectors[2, :width]
    units_w = line_gather(block).reshape(width, 2 * ff_pad)
    down_w = line_gather(down_own).reshape(ff_here, width)
    down_w = jnp.pad(down_w, ((0, ff_pad - ff_here), (0, 0)))

    seq_hops = bits_of("seq", seq_count)
    pairs = gather_hops(qkv[:, query_width:], seq_hops).reshape(SLOT, 2 * pair_width)
    distance = jnp.arange(SLOT, dtype=jnp.int32)
    key_place = (seq_here ^ (distance // rows)) * rows + distance % rows
    kpos = jnp.where(key_place < lengths[0], key_place - seq_here * rows, far_place)[None, :]
    mixed = attend_forward(kpos, qkv, pairs)
    resid = flat + product(mixed, out_w)
    normed_two, factor_two = norm_rows(resid, gain_two)
    normed_two_low = normed_two.astype(low)

    core = hops_a[-1]
    slow_a, slow_b = hops_a[:-1], hops_b[:-1]
    near_rows = plane * rows // 2

    def spread(block):
        part_a = gather_hops(block[: rows // 2], slow_a)
        part_b = gather_hops(block[rows // 2 :], slow_b)
        near = jnp.stack([part_a, part_b]).reshape(near_rows, width)
        return jnp.concatenate([near, swap(near, core)], axis=0)

    def hop_core(partial):
        other = swap(partial[near_rows:], core)
        near = (partial[:near_rows].astype(full) + other.astype(full)).astype(low)
        near = near.reshape(2, plane // 2, rows // 2, width)
        return (near[0], near[1])

    def hop_slow(parts, stage):
        return tuple(reduce_hop(part, hops[stage]) for part, hops in zip(parts, (slow_a, slow_b)))

    def hop_last(parts):
        got = [reduce_hops(part, hops[:1]) for part, hops in zip(parts, (slow_a, slow_b))]
        return jnp.concatenate(got, axis=0)

    stages = list(range(1, len(slow_a)))[::-1]
    grad_all = spread(upstream_low)
    rows_all = spread(normed_two_low)
    hidden_grad = product_right(grad_all, down_w)
    both = product(rows_all, units_w)
    gate, upper = both[:, :ff_pad], both[:, ff_pad:]
    sigma = jax.nn.sigmoid(gate)
    hidden = (gate * sigma * upper).astype(low)
    gate_grad = (hidden_grad * upper * sigma * (1.0 + gate * (1.0 - sigma))).astype(low)
    up_grad = (hidden_grad * gate * sigma).astype(low)
    units_grad = jnp.concatenate([gate_grad, up_grad], axis=1)
    partial = product_right(units_grad, units_w).astype(low)
    down_grad = product_left(after(hidden, partial), grad_all).astype(low)
    down_grad = down_grad[:ff_here]
    down_line = line_reduce(down_grad.reshape(outer, ff_own, width))
    back = hop_core(partial)
    rows_late, grad_late = lax.optimization_barrier((rows_all, units_grad, back, down_grad))[:2]
    units_w_grad = product_left(rows_late, grad_late).astype(low)
    units_line = line_reduce(units_w_grad.reshape(outer, INNER * share, 2 * ff_pad))
    for stage in stages:
        back = hop_slow(back, stage)
    hidden_late = after(hidden, back, units_w_grad)
    partial = product(hidden_late, down_w).astype(low)
    normed_two_grad = hop_last(back)

    upstream = upstream_low.astype(full)
    resid_norm_grad, gain_two_grad = norm_back(resid, factor_two, gain_two, normed_two_grad)
    resid_grad = upstream + resid_norm_grad
    attn_grad = resid_grad.astype(low)
    mixed_grad = product_right(attn_grad, out_w).astype(low)
    out_w_grad = product_left(mixed, attn_grad).astype(low)
    out_w_out = reduce_weight(out_w_grad.reshape(wt_count, -1, width)).astype(full)
    query_grad, key_part, value_part = attend_backward(
        kpos, cosine, sine, qkv, pairs, mixed_grad
    )
    forth = hop_core(after(partial, normed_two_grad))
    for stage in stages:
        forth = hop_slow(forth, stage)
    forth = hop_last(lax.optimization_barrier((*forth, query_grad))[:2])
    layer_out = jnp.where(keep, resid + forth, 0.0).astype(low)
    layer_out = layer_out.reshape(slot_count, rows, width)

    blocks = units_line.reshape(INNER, share, 2 * ff_pad)
    sent = jnp.stack([to_place(blocks, inner_here ^ d) for d in range(INNER)])
    gate_out, up_out = join_units(
        info, gather_hops(inner_exchange(sent), seq_hops), outer, ff_own
    )
    down_out = seq_gather(after(down_line, query_grad))
    down_out = down_out.reshape(seq_count * ff_own, width).astype(full)
    pair_part = jnp.concatenate([key_part, value_part], axis=1)
    pair_sum = reduce_hops(
        pair_part.reshape(seq_count, rows, 2 * pair_width).astype(low), seq_hops
    )
    key_rot_grad = pair_sum[:, :pair_width].reshape(rows, KV_HEADS, HEAD_DIM)
    turned = jnp.concatenate([key_rot_grad[..., half:], key_rot_grad[..., :half]], axis=-1)
    key_grad = key_rot_grad * cosine[:, None, :] - turned * sine[:, None, :]
    head_grad = jnp.concatenate(
        [query_grad, key_grad.reshape(rows, pair_width).astype(low),
         pair_sum[:, pair_width:].astype(low)],
        axis=1,
    )
    head_w_grad = product_left(normed_low, head_grad).astype(low)
    head_b_grad = jnp.sum(head_grad.astype(full), axis=0)
    normed_grad = product_right(head_grad, head_w)
    factor_one = lax.rsqrt(jnp.mean(flat * flat, axis=-1, keepdims=True) + epsilon)
    input_norm_grad, gain_one_grad = norm_back(flat, factor_one, gain_one, normed_grad)
    input_grad = (resid_grad + input_norm_grad).astype(low).reshape(slot_count, rows, width)

    edges = [0, share, share + bias_q]
    edges += [edges[-1] + bias_k, edges[-1] + 2 * bias_k]

    def parts(vector):
        return vector.reshape(wt_count, -1)

    small_grad = jnp.concatenate(
        [
            parts(gain_one_grad),
            parts(head_b_grad[:query_width]),
            parts(head_b_grad[query_width : query_width + pair_width]),
            parts(head_b_grad[query_width + pair_width :]),
            parts(gain_two_grad),
        ],
        axis=1,
    ).astype(low)
    extra = jnp.pad(
        small_grad[:, None, :],
        ((0, 0), (0, EXTRA - 1), (0, head_width - small_grad.shape[1])),
    )
    head_sum = reduce_weight(
        jnp.concatenate([head_w_grad.reshape(wt_count, share, head_width), extra], axis=1)
    ).astype(full)
    heads_out = head_sum[:share]
    small_out = head_sum[share]
    return (
        layer_out,
        input_grad,
        small_out[: edges[1]],
        heads_out[:, :query_width],
        small_out[edges[1] : edges[2]],
        heads_out[:, query_width : query_width + pair_width],
        small_out[edges[2] : edges[3]],
        heads_out[:, query_width + pair_width :],
        small_out[edges[3] : edges[4]],
        out_w_out,
        small_out[edges[4] : edges[4] + ffn_gain.shape[0]],
        gate_out,
        up_out,
        down_out,
    )


def solution(mesh):
    by_wt = P("wt")
    by_row = P("wt", None)
    by_token = P("wt", "seq", None)
    return jax.shard_map(
        body,
        mesh=mesh,
        in_specs=(
            by_token, by_wt, by_wt, by_row, by_wt, by_row, by_wt, by_row, by_wt, by_row,
            by_wt, by_row, by_row, by_row, by_token,
        ),
        out_specs=(
            by_token, by_token, by_wt, by_row, by_wt, by_row, by_wt, by_row, by_wt, by_row,
            by_wt, by_row, by_row, by_row,
        ),
        check_vma=False,
    )
```

```python
import functools
import math

import jax
import jax.numpy as jnp
from jax import lax
from jax.experimental import pallas as pl
from jax.experimental.pallas import tpu as pltpu
from jax.sharding import PartitionSpec as P


HEADS = 12
KV_HEADS = 2
HEAD_DIM = 128
SLOT = 1024
INNER = 4

epsilon = 1e-06
masked_score = -1e30
far_place = 1 << 30
scale = 1.0 / math.sqrt(HEAD_DIM)
low = jnp.bfloat16
full = jnp.float32


def product(left, right):
    return jnp.dot(left, right, preferred_element_type=full)


def product_left(left, right):
    return lax.dot_general(left, right, (((0,), (0,)), ((), ())), preferred_element_type=full)


def product_right(left, right):
    return lax.dot_general(left, right, (((1,), (1,)), ((), ())), preferred_element_type=full)


def norm_rows(values, gain):
    factor = lax.rsqrt(jnp.mean(values * values, axis=-1, keepdims=True) + epsilon)
    return (values * factor * gain, factor)


def norm_back(values, factor, gain, upstream):
    weighted = upstream * gain
    inner = jnp.mean(weighted * values, axis=-1, keepdims=True)
    grad_in = factor * weighted - values * (factor * factor * factor) * inner
    grad_gain = jnp.sum(upstream * values * factor, axis=0)
    return (grad_in, grad_gain)


def swap(value, hop):
    axis, bit = hop
    count = lax.axis_size(axis)
    return lax.ppermute(value, axis, [(i, i ^ bit) for i in range(count)])


def gather_hops(block, hops):
    held = block[None]
    for hop in hops:
        held = jnp.concatenate([held, swap(held, hop)], axis=0)
    return held


def reduce_hop(held, hop):
    half = held.shape[0] // 2
    other = swap(held[half:], hop)
    return (held[:half].astype(full) + other.astype(full)).astype(low)


def reduce_hops(held, hops):
    for k in range(len(hops) - 1, 0, -1):
        held = reduce_hop(held, hops[k])
    return held[0].astype(full) + swap(held[1], hops[0]).astype(full)


def bits_of(axis, count):
    found, bit = [], 1
    while bit < count:
        found.append((axis, bit))
        bit *= 2
    return found


def plane_hops(seq_count):
    inner = bits_of("wt", INNER)
    seq = bits_of("seq", seq_count)
    slow = inner[1:] + seq
    return (slow + inner[:1], slow[::-1] + inner[:1])


def to_place(stacked, place):
    return lax.dynamic_index_in_dim(stacked, place, 0, keepdims=False)


def flip(index, bit):
    return index + bit - 2 * bit * ((index // bit) % 2)


def flip_all(index, distance):
    bit = 1
    while bit <= distance:
        if distance & bit:
            index = flip(index, bit)
        bit *= 2
    return index


def inner_bits():
    return [bit for _, bit in bits_of("wt", INNER)]


def meet(peers):
    barrier = pltpu.get_barrier_semaphore()
    for peer in peers:
        pl.semaphore_signal(
            barrier, inc=1, device_id=peer, device_id_type=pl.DeviceIdType.MESH
        )
    pl.semaphore_wait(barrier, len(peers))


class Sender:
    def __init__(self, send_sems, recv_sems):
        self.sems = (send_sems, recv_sems)
        self.copies = []

    def start(self, source, target, peer):
        at = len(self.copies)
        copy = pltpu.make_async_remote_copy(
            src_ref=source,
            dst_ref=target,
            send_sem=self.sems[0].at[at],
            recv_sem=self.sems[1].at[at],
            device_id=peer,
            device_id_type=pl.DeviceIdType.MESH,
        )
        copy.start()
        self.copies.append(copy)
        return copy


def subsets(hops):
    found = [(0, 0)]
    for axis, bit in hops:
        more = [(a ^ bit, b) if axis == "wt" else (a, b ^ bit) for a, b in found]
        found = found + more
    return found


def plane_copies(seq_count):
    hops_a, _ = plane_hops(seq_count)
    slow = len(hops_a) - 1
    return (2 * (2**slow - 1), len(set(a for a, _ in subsets(hops_a[:-1]))))


def gather_kernel(
    outer, seq_count, x_ref, p_ref, wo_ref, s_ref, cos_ref, sin_ref,
    normed_ref, qkv_ref, vec_ref, head_ref, out_ref,
    w_scr, o_scr, s_scr, send_sems, recv_sems, local_sems,
):
    share, head_width = p_ref.shape
    width = x_ref.shape[1]
    wt, seq = lax.axis_index("wt"), lax.axis_index("seq")
    line, inner = wt // INNER, wt % INNER
    hops = plane_hops(seq_count)
    slow = len(hops[0]) - 1
    peers = [(flip_all(line, d) * INNER + inner, seq) for d in range(1, outer)]
    peers += [(wt - inner + flip(inner, bit), seq) for bit in inner_bits()]
    peers += [(wt, flip(seq, bit)) for _, bit in bits_of("seq", seq_count)]

    def own_columns(total):
        wide = total // seq_count
        return pl.ds(pl.multiple_of(seq * wide, 128), wide)

    fill = [
        pltpu.make_async_copy(
            ref.at[:, own_columns(ref.shape[1])],
            scratch.at[line, inner, :, own_columns(ref.shape[1])],
            local_sems.at[k],
        )
        for k, (ref, scratch) in enumerate(((p_ref, w_scr), (wo_ref, o_scr)))
    ] + [
        pltpu.make_async_copy(s_ref, s_scr.at[line, inner], local_sems.at[2]),
    ]
    for copy in fill:
        copy.start()
    meet(peers)
    out = Sender(send_sems, recv_sems)

    def hop_peer(hop):
        axis, bit = hop
        if axis == "wt":
            return (wt - inner + flip(inner, bit), seq)
        return (wt, flip(seq, bit))

    def columns(total, part, half):
        wide = total // seq_count
        first = -(-wide // 256) * 128
        start = part * wide + half * first
        return pl.ds(pl.multiple_of(start, 128), wide - first if half else first)

    def start_line(source, scratch, narrow):
        total = source.shape[1]
        copies = [None]
        for d in range(1, outer):
            if narrow:
                part = own_columns(total)
                pair = (source.at[:, part], scratch.at[line, inner, :, part])
            else:
                pair = (source, scratch.at[line, inner])
            copies.append(out.start(*pair, (flip_all(line, d) * INNER + inner, seq)))
        return copies

    small_line = start_line(s_ref, s_scr, False)
    head_line = start_line(p_ref, w_scr, True)
    out_line = start_line(wo_ref, o_scr, True)

    def start_stage(scratch, at, stage):
        total = scratch.shape[-1]
        copies = []
        if stage < slow:
            for half in range(2):
                hop = hops[half][stage]
                for a, b in subsets(hops[half][:stage]):
                    place = scratch.at[
                        at, flip_all(inner, a), :, columns(total, flip_all(seq, b), half)
                    ]
                    copies.append(out.start(place, place, hop_peer(hop)))
            return copies
        for a in sorted(set(a for a, _ in subsets(hops[0][:slow]))):
            place = scratch.at[at, flip_all(inner, a)]
            copies.append(out.start(place, place, hop_peer(hops[0][slow])))
        return copies

    def arrive(copies):
        for copy in copies:
            if copy is not None:
                copy.wait_recv()

    for copy in fill:
        copy.wait()
    waiting = [[copy] for copy in head_line]
    small_wait = small_line
    for step in range(outer + slow + 1):
        for stage in range(slow + 1):
            d = step - stage
            if 0 <= d < outer:
                arrive(waiting[d])
                waiting[d] = start_stage(w_scr, flip_all(line, d), stage)
        if step == 0:
            arrive(small_wait)
            small_wait = []
        if step < len(inner_bits()):
            arrive(small_wait)
            bit = inner_bits()[::-1][step]
            small_wait = []
            for a, _ in subsets([("wt", b) for b in inner_bits()[::-1][:step]]):
                place = s_scr.at[:, flip_all(inner, a)]
                small_wait.append(out.start(place, place, hop_peer(("wt", bit))))
    arrive(small_wait)
    arrive(out_line)
    out_wait = start_stage(o_scr, slice(None), 0)

    count = outer * INNER
    bias_k = share * KV_HEADS * HEAD_DIM // (HEADS * HEAD_DIM)
    query_width = HEADS * HEAD_DIM
    pair_width = KV_HEADS * HEAD_DIM
    vec_ref[...] = jnp.zeros_like(vec_ref)
    for k in range(count):
        small = s_scr[k // INNER, k % INNER].astype(full)
        at = k * share
        vec_ref[0:1, at : at + share] = small[0:1, :share]
        vec_ref[1:2, at : at + share] = small[1:2, :share]
        at = query_width + k * bias_k
        vec_ref[1:2, at : at + bias_k] = small[2:3, :bias_k]
        at = query_width + pair_width + k * bias_k
        vec_ref[1:2, at : at + bias_k] = small[3:4, :bias_k]
        at = k * share
        vec_ref[2:3, at : at + share] = small[4:5, :share]

    values = x_ref[...].astype(full)
    factor = lax.rsqrt(jnp.mean(values * values, axis=-1, keepdims=True) + epsilon)
    normed_ref[...] = (values * factor * vec_ref[0:1, :width]).astype(low)
    for d in range(outer):
        arrive(waiting[d])
    keep_head = pltpu.make_async_copy(w_scr, head_ref, local_sems.at[0])
    keep_head.start()
    wide = 2 * HEAD_DIM
    blocks = head_width // wide

    def project(at):
        weights = w_scr[:, :, :, pl.ds(at, wide)].reshape(width, wide)
        return (
            jnp.dot(normed_ref[...], weights, preferred_element_type=full)
            + vec_ref[1:2, pl.ds(at, wide)]
        )

    def turn_block(k):
        at = pl.multiple_of(k * wide, wide)
        got = project(at)
        for j in range(2):
            part = got[:, j * HEAD_DIM : (j + 1) * HEAD_DIM]
            turned = part * cos_ref[...] + pltpu.roll(part, HEAD_DIM // 2, 1) * sin_ref[...]
            where = pl.multiple_of(at + j * HEAD_DIM, HEAD_DIM)
            qkv_ref[:, pl.ds(where, HEAD_DIM)] = turned.astype(low)

    turned_blocks = blocks - pair_width // wide
    marks = [turned_blocks * (k + 1) // (slow + 1) for k in range(slow + 1)]
    begin = 0
    for stage in range(slow + 1):
        @pl.loop(begin, marks[stage])
        def _(k):
            turn_block(k)

        begin = marks[stage]
        arrive(out_wait)
        out_wait = start_stage(o_scr, slice(None), stage + 1) if stage < slow else []
    for k in range(turned_blocks, blocks):
        qkv_ref[:, k * wide : (k + 1) * wide] = project(k * wide).astype(low)
    keep_out = pltpu.make_async_copy(o_scr, out_ref, local_sems.at[1])
    keep_out.start()
    for copy in out.copies:
        copy.wait_send()
    keep_head.wait()
    keep_out.wait()


def gather_project(tokens, packed, w_out, small, cosine, sine):
    outer = lax.axis_size("wt") // INNER
    seq_count = lax.axis_size("seq")
    rows, width = tokens.shape
    share, head_width = packed.shape
    slow_copies, last_copies = plane_copies(seq_count)
    each = slow_copies + last_copies
    small_copies = 2 ** len(inner_bits()) - 1
    copies = 3 * (outer - 1) + (outer + 1) * each + small_copies
    vmem = pl.BlockSpec(memory_space=pltpu.VMEM)
    anywhere = pl.BlockSpec(memory_space=pl.ANY)
    sent = 2 * outer * INNER * share * (head_width + w_out.shape[1])
    return pl.pallas_call(
        functools.partial(gather_kernel, outer, seq_count),
        in_specs=[vmem] * 6,
        out_specs=[vmem, vmem, vmem, anywhere, anywhere],
        out_shape=[
            jax.ShapeDtypeStruct((rows, width), low),
            jax.ShapeDtypeStruct((rows, head_width), low),
            jax.ShapeDtypeStruct((8, head_width), full),
            jax.ShapeDtypeStruct((outer, INNER, share, head_width), low),
            jax.ShapeDtypeStruct((outer, INNER, share, w_out.shape[1]), low),
        ],
        scratch_shapes=[
            pltpu.VMEM((outer, INNER, share, head_width), low),
            pltpu.VMEM((outer, INNER, share, w_out.shape[1]), low),
            pltpu.VMEM((outer, INNER, small.shape[0], small.shape[1]), low),
            pltpu.SemaphoreType.DMA((copies,)),
            pltpu.SemaphoreType.DMA((copies,)),
            pltpu.SemaphoreType.DMA((3,)),
        ],
        compiler_params=pltpu.CompilerParams(
            collective_id=1, has_side_effects=True, vmem_limit_bytes=48 << 20
        ),
        cost_estimate=pl.CostEstimate(
            flops=2 * rows * width * head_width * 8, bytes_accessed=2 * sent, transcendentals=0
        ),
        name="gather_project",
    )(tokens, packed, w_out, small, cosine, sine)


def near_inner(seq_count):
    hops = plane_hops(seq_count)[0]
    return sorted(set(a for a, _ in subsets(hops[:-1])))


def reduce_kernel(outer, seq_count, count, *refs):
    given, results = refs[:count], refs[count : 2 * count]
    slow = len(plane_hops(seq_count)[0]) - 1
    held = refs[2 * count : 3 * count]
    lines = refs[3 * count : 4 * count]
    joined = refs[4 * count : 5 * count]
    landed = refs[5 * count : (6 + slow) * count]
    send_sems, recv_sems = refs[(6 + slow) * count :]
    wt, seq = lax.axis_index("wt"), lax.axis_index("seq")
    line, inner = wt // INNER, wt % INNER
    hops = plane_hops(seq_count)
    nears = near_inner(seq_count)
    peers = [(flip_all(line, d) * INNER + inner, seq) for d in range(1, outer)]
    peers += [(wt - inner + flip(inner, bit), seq) for bit in inner_bits()]
    peers += [(wt, flip_all(seq, d)) for d in range(1, seq_count)]
    meet(peers)
    out = Sender(send_sems, recv_sems)

    def hop_peer(hop):
        axis, bit = hop
        if axis == "wt":
            return (wt - inner + flip(inner, bit), seq)
        return (wt, flip(seq, bit))

    def columns(total, part, half):
        wide = total // seq_count
        first = -(-wide // 256) * 128
        start = part * wide + half * first
        return pl.ds(pl.multiple_of(start, 128), wide - first if half else first)

    def arrive(copies):
        for copy in copies:
            copy.wait_recv()

    def steps(k):
        source, total = given[k], given[k].shape[3]
        sums, wide = held[k], given[k].shape[3] // seq_count
        own = pl.ds(pl.multiple_of(seq * wide, 128), wide)
        core = hops[0][slow]
        copies = [
            out.start(
                source.at[:, flip_all(inner, a ^ core[1])],
                landed[k].at[:, at],
                hop_peer(core),
            )
            for at, a in enumerate(nears)
        ]
        yield
        arrive(copies)
        for at, a in enumerate(nears):
            place = flip_all(inner, a)

            @pl.loop(0, outer)
            def _(o):
                both = source[o, place].astype(full) + landed[k][o, at].astype(full)
                sums[o, at] = both.astype(low)

        for stage in range(slow - 1, -1, -1):
            target = landed[(1 + stage) * count + k]
            copies, blocks = [], []
            for half in range(2):
                axis, bit = hops[half][stage]
                for a, b in subsets(hops[half][:stage]):
                    from_a = a ^ bit if axis == "wt" else a
                    from_b = b ^ bit if axis == "seq" else b
                    sent = columns(total, flip_all(seq, from_b), half)
                    copies.append(
                        out.start(
                            sums.at[:, nears.index(from_a), :, sent],
                            target.at[:, nears.index(a), :, sent],
                            hop_peer((axis, bit)),
                        )
                    )
                    blocks.append((nears.index(a), columns(total, flip_all(seq, b), half)))
            yield
            arrive(copies)
            for at, part in blocks:

                @pl.loop(0, outer)
                def _(o):
                    both = sums[o, at, :, part].astype(full) + target[o, at, :, part].astype(full)
                    sums[o, at, :, part] = both.astype(low)

        copies = [
            out.start(
                sums.at[flip_all(line, d), 0, :, own],
                lines[k].at[d],
                (flip_all(line, d) * INNER + inner, seq),
            )
            for d in range(1, outer)
        ]
        yield
        arrive(copies)
        both = sums[line, 0, :, own].astype(full)
        for d in range(1, outer):
            both = both + lines[k][d].astype(full)
        joined[k][:, own] = both.astype(low)
        copies = [
            out.start(joined[k].at[:, own], joined[k].at[:, own], (wt, flip_all(seq, d)))
            for d in range(1, seq_count)
        ]
        yield
        arrive(copies)
        results[k][...] = joined[k][...].astype(full)

    running = [steps(k) for k in range(count)]
    while running:
        for one in list(running):
            if next(one, "done") == "done":
                running.remove(one)
    for copy in out.copies:
        copy.wait_send()


def reduce_shares(*partials):
    outer = lax.axis_size("wt") // INNER
    seq_count = lax.axis_size("seq")
    count = len(partials)
    slow = len(plane_hops(seq_count)[0]) - 1
    nears = len(near_inner(seq_count))
    vmem = pl.BlockSpec(memory_space=pltpu.VMEM)
    near = [
        pltpu.VMEM((outer, nears) + p.shape[2:], low) for p in partials
    ]
    shapes = [p.shape[2:] for p in partials]
    copies = count * (nears + 2 * (2**slow - 1) + outer - 1 + seq_count - 1)
    sent = sum(2 * p.size for p in partials)
    return pl.pallas_call(
        functools.partial(reduce_kernel, outer, seq_count, count),
        in_specs=[vmem] * count,
        out_specs=[vmem] * count,
        out_shape=[jax.ShapeDtypeStruct(shape, full) for shape in shapes],
        scratch_shapes=near
        + [pltpu.VMEM((outer, r, c // seq_count), low) for r, c in shapes]
        + [pltpu.VMEM(shape, low) for shape in shapes]
        + near * (1 + slow)
        + [pltpu.SemaphoreType.DMA((copies,)), pltpu.SemaphoreType.DMA((copies,))],
        compiler_params=pltpu.CompilerParams(
            collective_id=2, has_side_effects=True, vmem_limit_bytes=60 << 20
        ),
        cost_estimate=pl.CostEstimate(flops=0, bytes_accessed=8 * sent, transcendentals=0),
        name="reduce_shares",
    )(*partials)


def split_kernel(outer, seq_count, own, info_ref, gate_ref, up_ref, o_ref):
    inner = info_ref[1]
    width = outer * own
    padded = o_ref.shape[2] // 2
    for s in range(seq_count):
        @pl.when(info_ref[0] == s)
        def _():
            for q in range(INNER):
                place = jnp.bitwise_xor(inner, q)
                for k, ref in enumerate((gate_ref, up_ref)):
                    for o in range(outer):
                        at = ((o * INNER + q) * seq_count + s) * own
                        to = k * padded + o * own
                        o_ref[place, :, to : to + own] = ref[:, at : at + own].astype(low)
                    if padded > width:
                        blank = jnp.zeros((o_ref.shape[1], padded - width), low)
                        o_ref[place, :, k * padded + width : (k + 1) * padded] = blank


def split_units(info, gate, up, outer, seq_count, own, padded):
    vmem = pl.BlockSpec(memory_space=pltpu.VMEM)
    return pl.pallas_call(
        functools.partial(split_kernel, outer, seq_count, own),
        in_specs=[pl.BlockSpec(memory_space=pltpu.SMEM), vmem, vmem],
        out_specs=vmem,
        out_shape=jax.ShapeDtypeStruct((INNER, gate.shape[0], 2 * padded), low),
        name="split_units",
    )(info, gate, up)


def join_kernel(outer, seq_count, own, info_ref, u_ref, gate_ref, up_ref):
    seq, inner = info_ref[0], info_ref[1]
    padded = u_ref.shape[3] // 2
    for s in range(seq_count):
        for q in range(INNER):
            block = u_ref[jnp.bitwise_xor(seq, s), jnp.bitwise_xor(inner, q)].astype(full)
            for k, ref in enumerate((gate_ref, up_ref)):
                for o in range(outer):
                    at = ((o * INNER + q) * seq_count + s) * own
                    source = k * padded + o * own
                    ref[:, at : at + own] = block[:, source : source + own]


def join_units(info, units, outer, own):
    seq_count, _, rows, _ = units.shape
    vmem = pl.BlockSpec(memory_space=pltpu.VMEM)
    shape = jax.ShapeDtypeStruct((rows, outer * INNER * seq_count * own), full)
    return pl.pallas_call(
        functools.partial(join_kernel, outer, seq_count, own),
        in_specs=[pl.BlockSpec(memory_space=pltpu.SMEM), vmem],
        out_specs=[vmem, vmem],
        out_shape=[shape, shape],
        name="join_units",
    )(info, units)


def after(value, *others):
    return lax.optimization_barrier((value, *others))[0]


def shown(kpos_ref, rows, keys):
    places = lax.broadcasted_iota(jnp.int32, (rows, keys), 0)
    return kpos_ref[...] <= places


def fwd_kernel(kpos_ref, q_ref, k_ref, v_ref, o_ref):
    rows, keys = q_ref.shape[0], k_ref.shape[0]
    scores = (
        lax.dot_general(
            q_ref[...], k_ref[...], (((1,), (1,)), ((), ())), preferred_element_type=full
        )
        * scale
    )
    scores = jnp.where(shown(kpos_ref, rows, keys), scores, masked_score)
    top = jnp.max(scores, axis=-1, keepdims=True)
    weights = jnp.exp(scores - top)
    total = jnp.sum(weights, axis=-1, keepdims=True)
    probs = (weights * (1.0 / total)).astype(low)
    o_ref[...] = jnp.dot(probs, v_ref[...], preferred_element_type=full).astype(low)


def attend_forward(kpos, qkv, pairs):
    rows = qkv.shape[0]
    keys = pairs.shape[0]
    group = HEADS // KV_HEADS
    return pl.pallas_call(
        fwd_kernel,
        grid=(HEADS,),
        in_specs=[
            pl.BlockSpec((1, keys), lambda h: (0, 0)),
            pl.BlockSpec((rows, HEAD_DIM), lambda h: (0, h)),
            pl.BlockSpec((keys, HEAD_DIM), lambda h: (0, h // group)),
            pl.BlockSpec((keys, HEAD_DIM), lambda h: (0, KV_HEADS + h // group)),
        ],
        out_specs=pl.BlockSpec((rows, HEAD_DIM), lambda h: (0, h)),
        out_shape=jax.ShapeDtypeStruct((rows, HEADS * HEAD_DIM), low),
        cost_estimate=pl.CostEstimate(
            flops=4 * rows * keys * HEADS * HEAD_DIM * 3,
            bytes_accessed=4 * rows * HEADS * HEAD_DIM + 4 * keys * KV_HEADS * HEAD_DIM,
            transcendentals=rows * keys * HEADS,
        ),
        name="attend_forward",
    )(kpos, qkv, pairs, pairs)


def bwd_kernel(kpos_ref, cos_ref, sin_ref, q_ref, k_ref, v_ref, g_ref, dq_ref, dk_ref, dv_ref):
    rows, keys = q_ref.shape[0], k_ref.shape[0]
    group = HEADS // KV_HEADS
    head = pl.program_id(0)
    queries, key, value, grad = q_ref[...], k_ref[...], v_ref[...], g_ref[...]
    scores = (
        lax.dot_general(queries, key, (((1,), (1,)), ((), ())), preferred_element_type=full)
        * scale
    )
    scores = jnp.where(shown(kpos_ref, rows, keys), scores, masked_score)
    top = jnp.max(scores, axis=-1, keepdims=True)
    weights = jnp.exp(scores - top)
    total = jnp.sum(weights, axis=-1, keepdims=True)
    probs = weights * (1.0 / total)
    prob_grad = lax.dot_general(
        grad, value, (((1,), (1,)), ((), ())), preferred_element_type=full
    )
    inner = jnp.sum(probs * prob_grad, axis=-1, keepdims=True)
    score_grad = (probs * (prob_grad - inner)).astype(low)
    dv = lax.dot_general(
        probs.astype(low), grad, (((0,), (0,)), ((), ())), preferred_element_type=full
    )
    dk = (
        lax.dot_general(
            score_grad, queries, (((0,), (0,)), ((), ())), preferred_element_type=full
        )
        * scale
    )
    dq = jnp.dot(score_grad, key, preferred_element_type=full) * scale
    turned = dq * cos_ref[...] - pltpu.roll(dq, HEAD_DIM // 2, 1) * sin_ref[...]
    dq_ref[...] = turned.astype(low)

    @pl.when(head % group == 0)
    def _():
        dk_ref[...] = dk
        dv_ref[...] = dv

    @pl.when(head % group != 0)
    def _():
        dk_ref[...] += dk
        dv_ref[...] += dv


def attend_backward(kpos, cosine, sine, qkv, pairs, grad):
    rows = qkv.shape[0]
    keys = pairs.shape[0]
    group = HEADS // KV_HEADS
    width = KV_HEADS * HEAD_DIM
    return pl.pallas_call(
        bwd_kernel,
        grid=(HEADS,),
        in_specs=[
            pl.BlockSpec((1, keys), lambda h: (0, 0)),
            pl.BlockSpec((rows, HEAD_DIM), lambda h: (0, 0)),
            pl.BlockSpec((rows, HEAD_DIM), lambda h: (0, 0)),
            pl.BlockSpec((rows, HEAD_DIM), lambda h: (0, h)),
            pl.BlockSpec((keys, HEAD_DIM), lambda h: (0, h // group)),
            pl.BlockSpec((keys, HEAD_DIM), lambda h: (0, KV_HEADS + h // group)),
            pl.BlockSpec((rows, HEAD_DIM), lambda h: (0, h)),
        ],
        out_specs=[
            pl.BlockSpec((rows, HEAD_DIM), lambda h: (0, h)),
            pl.BlockSpec((keys, HEAD_DIM), lambda h: (0, h // group)),
            pl.BlockSpec((keys, HEAD_DIM), lambda h: (0, h // group)),
        ],
        out_shape=[
            jax.ShapeDtypeStruct((rows, HEADS * HEAD_DIM), low),
            jax.ShapeDtypeStruct((keys, width), full),
            jax.ShapeDtypeStruct((keys, width), full),
        ],
        cost_estimate=pl.CostEstimate(
            flops=10 * rows * keys * HEADS * HEAD_DIM * 3,
            bytes_accessed=8 * rows * HEADS * HEAD_DIM + 12 * keys * width,
            transcendentals=rows * keys * HEADS,
        ),
        name="attend_backward",
    )(kpos, cosine, sine, qkv, pairs, pairs, grad)


def body(
    tokens, lengths, attn_gain, w_query, b_query, w_key, b_key, w_value, b_value, w_out,
    ffn_gain, w_gate, w_up, w_down, cotangent,
):
    slot_count, rows, width = tokens.shape
    seq_count = lax.axis_size("seq")
    wt_count = lax.axis_size("wt")
    outer = wt_count // INNER
    seq_here = lax.axis_index("seq")
    inner_here = lax.axis_index("wt") % INNER
    line = [[o * INNER + i for o in range(outer)] for i in range(INNER)]
    hops_a, hops_b = plane_hops(seq_count)
    plane = INNER * seq_count
    share = w_query.shape[0]
    bias_q, bias_k = b_query.shape[0], b_key.shape[0]
    query_width = HEADS * HEAD_DIM
    pair_width = KV_HEADS * HEAD_DIM
    head_width = query_width + 2 * pair_width
    ff_own = w_down.shape[0] // seq_count
    ff_here = outer * ff_own
    ff_pad = -(-ff_here // 128) * 128

    flat = tokens.astype(full).reshape(rows, width)
    places = seq_here * rows + jnp.arange(rows, dtype=jnp.int32)
    keep = (places < lengths[0])[:, None]
    upstream_low = jnp.where(keep, cotangent.reshape(rows, width), jnp.zeros((), low))

    def line_gather(value):
        return lax.all_gather(value, "wt", axis=0, axis_index_groups=line, tiled=False)

    def line_reduce(value):
        return lax.psum_scatter(
            value, "wt", scatter_dimension=0, axis_index_groups=line, tiled=False
        )

    def seq_gather(value):
        stacked = gather_hops(value, bits_of("seq", seq_count))
        return jnp.stack([to_place(stacked, seq_here ^ p) for p in range(seq_count)])

    info = jnp.stack([seq_here, inner_here]).astype(jnp.int32)
    down_own = lax.dynamic_slice_in_dim(w_down, seq_here * ff_own, ff_own, axis=0).astype(low)

    def inner_swap(value, distance):
        count = lax.axis_size("wt")
        return lax.ppermute(value, "wt", [(i, i ^ distance) for i in range(count)])

    def inner_exchange(value):
        got = [value[0]] + [inner_swap(value[d], d) for d in range(1, INNER)]
        return jnp.stack(got)

    stacked = inner_exchange(split_units(info, w_gate, w_up, outer, seq_count, ff_own, ff_pad))
    block = jnp.stack([to_place(stacked, inner_here ^ p) for p in range(INNER)])
    block = block.reshape(INNER * share, 2 * ff_pad)
    half = HEAD_DIM // 2
    inverse = 10000.0 ** (-jnp.arange(half, dtype=full) / half)
    angle = places.astype(full)[:, None] * inverse[None, :]
    cosine = jnp.cos(angle)
    sine = jnp.sin(angle)
    cosine = jnp.concatenate([cosine, cosine], axis=1)
    sine = jnp.concatenate([-sine, sine], axis=1)

    def line_of(vector):
        return jnp.pad(vector, (0, HEAD_DIM - vector.shape[0]))

    small = jnp.stack([line_of(v) for v in (attn_gain, b_query, b_key, b_value, ffn_gain)])
    small = jnp.pad(small.astype(low), ((0, 11), (0, 0)))
    packed = jnp.concatenate([w_query, w_key, w_value], axis=1).astype(low)
    normed_low, qkv, vectors, head_all, out_all = gather_project(
        tokens.reshape(rows, width),
        packed, w_out.astype(low), small, cosine, sine,
    )
    head_w = head_all.reshape(width, head_width)
    out_w = out_all.reshape(query_width, width)
    gain_one = vectors[0, :width]
    gain_two = vectors[2, :width]
    units_w = line_gather(block).reshape(width, 2 * ff_pad)
    down_w = line_gather(down_own).reshape(ff_here, width)
    down_w = jnp.pad(down_w, ((0, ff_pad - ff_here), (0, 0)))

    seq_hops = bits_of("seq", seq_count)
    pairs = gather_hops(qkv[:, query_width:], seq_hops).reshape(SLOT, 2 * pair_width)
    distance = jnp.arange(SLOT, dtype=jnp.int32)
    key_place = (seq_here ^ (distance // rows)) * rows + distance % rows
    kpos = jnp.where(key_place < lengths[0], key_place - seq_here * rows, far_place)[None, :]
    mixed = attend_forward(kpos, qkv, pairs)
    resid = flat + product(mixed, out_w)
    normed_two, factor_two = norm_rows(resid, gain_two)
    normed_two_low = normed_two.astype(low)

    core = hops_a[-1]
    slow_a, slow_b = hops_a[:-1], hops_b[:-1]
    near_rows = plane * rows // 2

    def spread(block):
        part_a = gather_hops(block[: rows // 2], slow_a)
        part_b = gather_hops(block[rows // 2 :], slow_b)
        near = jnp.stack([part_a, part_b]).reshape(near_rows, width)
        return jnp.concatenate([near, swap(near, core)], axis=0)

    def hop_core(partial):
        other = swap(partial[near_rows:], core)
        near = (partial[:near_rows].astype(full) + other.astype(full)).astype(low)
        near = near.reshape(2, plane // 2, rows // 2, width)
        return (near[0], near[1])

    def hop_slow(parts, stage):
        return tuple(reduce_hop(part, hops[stage]) for part, hops in zip(parts, (slow_a, slow_b)))

    def hop_last(parts):
        got = [reduce_hops(part, hops[:1]) for part, hops in zip(parts, (slow_a, slow_b))]
        return jnp.concatenate(got, axis=0)

    stages = list(range(1, len(slow_a)))[::-1]
    grad_all = spread(after(upstream_low, pairs))
    rows_all = spread(normed_two_low)
    hidden_grad = product_right(grad_all, down_w)
    both = product(rows_all, units_w)
    gate, upper = both[:, :ff_pad], both[:, ff_pad:]
    sigma = jax.nn.sigmoid(gate)
    hidden = (gate * sigma * upper).astype(low)
    gate_grad = (hidden_grad * upper * sigma * (1.0 + gate * (1.0 - sigma))).astype(low)
    up_grad = (hidden_grad * gate * sigma).astype(low)
    units_grad = jnp.concatenate([gate_grad, up_grad], axis=1)
    partial = product_right(units_grad, units_w).astype(low)
    down_grad = product_left(after(hidden, partial), grad_all).astype(low)
    down_grad = down_grad[:ff_here]
    down_line = line_reduce(down_grad.reshape(outer, ff_own, width))
    back = hop_core(partial)
    rows_late, grad_late = lax.optimization_barrier((rows_all, units_grad, back, down_grad))[:2]
    units_w_grad = product_left(rows_late, grad_late).astype(low)
    units_line = line_reduce(units_w_grad.reshape(outer, INNER * share, 2 * ff_pad))
    for stage in stages:
        back = hop_slow(back, stage)
    hidden_late = after(hidden, back, units_w_grad)
    partial = product(hidden_late, down_w).astype(low)
    normed_two_grad = hop_last(back)

    upstream = upstream_low.astype(full)
    resid_norm_grad, gain_two_grad = norm_back(resid, factor_two, gain_two, normed_two_grad)
    resid_grad = upstream + resid_norm_grad
    attn_grad = resid_grad.astype(low)
    mixed_grad = product_right(attn_grad, out_w).astype(low)
    out_w_grad = product_left(mixed, attn_grad).astype(low)
    query_grad, key_part, value_part = attend_backward(
        kpos, cosine, sine, qkv, pairs, mixed_grad
    )
    forth = hop_core(after(partial, normed_two_grad))
    for stage in stages:
        forth = hop_slow(forth, stage)
    forth = hop_last(lax.optimization_barrier((*forth, query_grad))[:2])
    layer_out = jnp.where(keep, resid + forth, 0.0).astype(low)
    layer_out = layer_out.reshape(slot_count, rows, width)

    blocks = units_line.reshape(INNER, share, 2 * ff_pad)
    sent = jnp.stack([to_place(blocks, inner_here ^ d) for d in range(INNER)])
    gate_out, up_out = join_units(
        info, gather_hops(inner_exchange(sent), seq_hops), outer, ff_own
    )
    down_out = seq_gather(down_line)
    down_out = down_out.reshape(seq_count * ff_own, width).astype(full)
    pair_part = jnp.concatenate([key_part, value_part], axis=1)
    pair_sum = reduce_hops(
        pair_part.reshape(seq_count, rows, 2 * pair_width).astype(low), seq_hops
    )
    key_rot_grad = pair_sum[:, :pair_width].reshape(rows, KV_HEADS, HEAD_DIM)
    turned = jnp.concatenate([key_rot_grad[..., half:], key_rot_grad[..., :half]], axis=-1)
    key_grad = key_rot_grad * cosine[:, None, :] - turned * sine[:, None, :]
    head_grad = jnp.concatenate(
        [query_grad, key_grad.reshape(rows, pair_width).astype(low),
         pair_sum[:, pair_width:].astype(low)],
        axis=1,
    )
    head_w_grad = product_left(normed_low, head_grad).astype(low)
    head_b_grad = jnp.sum(head_grad.astype(full), axis=0)
    normed_grad = product_right(head_grad, head_w)
    factor_one = lax.rsqrt(jnp.mean(flat * flat, axis=-1, keepdims=True) + epsilon)
    input_norm_grad, gain_one_grad = norm_back(flat, factor_one, gain_one, normed_grad)
    input_grad = (resid_grad + input_norm_grad).astype(low).reshape(slot_count, rows, width)

    edges = [0, share, share + bias_q]
    edges += [edges[-1] + bias_k, edges[-1] + 2 * bias_k]

    def parts(vector):
        return vector.reshape(wt_count, -1)

    small_grad = jnp.concatenate(
        [
            parts(gain_one_grad),
            parts(head_b_grad[:query_width]),
            parts(head_b_grad[query_width : query_width + pair_width]),
            parts(head_b_grad[query_width + pair_width :]),
            parts(gain_two_grad),
        ],
        axis=1,
    ).astype(low)
    small_grad = jnp.pad(small_grad, ((0, 0), (0, 256 * seq_count - small_grad.shape[1])))
    small_grad = jnp.pad(small_grad[:, None, :], ((0, 0), (0, 15), (0, 0)))

    def by_owner(partial):
        return partial.reshape(outer, INNER, -1, partial.shape[-1])

    heads_out, out_w_out, small_out = reduce_shares(
        by_owner(head_w_grad), by_owner(out_w_grad), by_owner(small_grad)
    )
    small_out = small_out[0]
    return (
        layer_out,
        input_grad,
        small_out[: edges[1]],
        heads_out[:, :query_width],
        small_out[edges[1] : edges[2]],
        heads_out[:, query_width : query_width + pair_width],
        small_out[edges[2] : edges[3]],
        heads_out[:, query_width + pair_width :],
        small_out[edges[3] : edges[4]],
        out_w_out,
        small_out[edges[4] : edges[4] + ffn_gain.shape[0]],
        gate_out,
        up_out,
        down_out,
    )


def solution(mesh):
    by_wt = P("wt")
    by_row = P("wt", None)
    by_token = P("wt", "seq", None)
    return jax.shard_map(
        body,
        mesh=mesh,
        in_specs=(
            by_token, by_wt, by_wt, by_row, by_wt, by_row, by_wt, by_row, by_wt, by_row,
            by_wt, by_row, by_row, by_row, by_token,
        ),
        out_specs=(
            by_token, by_token, by_wt, by_row, by_wt, by_row, by_wt, by_row, by_wt, by_row,
            by_wt, by_row, by_row, by_row,
        ),
        check_vma=False,
    )
```

```python
import functools
import math

import jax
import jax.numpy as jnp
from jax import lax
from jax.experimental import pallas as pl
from jax.experimental.pallas import tpu as pltpu
from jax.sharding import PartitionSpec as P


HEADS = 12
KV_HEADS = 2
HEAD_DIM = 128
SLOT = 1024
INNER = 4

epsilon = 1e-06
masked_score = -1e30
far_place = 1 << 30
scale = 1.0 / math.sqrt(HEAD_DIM)
low = jnp.bfloat16
full = jnp.float32


def product(left, right):
    return jnp.dot(left, right, preferred_element_type=full)


def product_left(left, right):
    return lax.dot_general(left, right, (((0,), (0,)), ((), ())), preferred_element_type=full)


def product_right(left, right):
    return lax.dot_general(left, right, (((1,), (1,)), ((), ())), preferred_element_type=full)


def norm_rows(values, gain):
    factor = lax.rsqrt(jnp.mean(values * values, axis=-1, keepdims=True) + epsilon)
    return (values * factor * gain, factor)


def norm_back(values, factor, gain, upstream):
    weighted = upstream * gain
    inner = jnp.mean(weighted * values, axis=-1, keepdims=True)
    grad_in = factor * weighted - values * (factor * factor * factor) * inner
    grad_gain = jnp.sum(upstream * values * factor, axis=0)
    return (grad_in, grad_gain)


def swap(value, hop):
    axis, bit = hop
    count = lax.axis_size(axis)
    return lax.ppermute(value, axis, [(i, i ^ bit) for i in range(count)])


def gather_hops(block, hops):
    held = block[None]
    for hop in hops:
        held = jnp.concatenate([held, swap(held, hop)], axis=0)
    return held


def reduce_hop(held, hop):
    half = held.shape[0] // 2
    other = swap(held[half:], hop)
    return (held[:half].astype(full) + other.astype(full)).astype(low)


def reduce_hops(held, hops):
    for k in range(len(hops) - 1, 0, -1):
        held = reduce_hop(held, hops[k])
    return held[0].astype(full) + swap(held[1], hops[0]).astype(full)


def bits_of(axis, count):
    found, bit = [], 1
    while bit < count:
        found.append((axis, bit))
        bit *= 2
    return found


def plane_hops(seq_count):
    inner = bits_of("wt", INNER)
    seq = bits_of("seq", seq_count)
    slow = inner[1:] + seq
    return (slow + inner[:1], slow[::-1] + inner[:1])


def to_place(stacked, place):
    return lax.dynamic_index_in_dim(stacked, place, 0, keepdims=False)


def flip(index, bit):
    return index + bit - 2 * bit * ((index // bit) % 2)


def flip_all(index, distance):
    bit = 1
    while bit <= distance:
        if distance & bit:
            index = flip(index, bit)
        bit *= 2
    return index


def inner_bits():
    return [bit for _, bit in bits_of("wt", INNER)]


def meet(peers):
    barrier = pltpu.get_barrier_semaphore()
    for peer in peers:
        pl.semaphore_signal(
            barrier, inc=1, device_id=peer, device_id_type=pl.DeviceIdType.MESH
        )
    pl.semaphore_wait(barrier, len(peers))


class Sender:
    def __init__(self, send_sems, recv_sems):
        self.sems = (send_sems, recv_sems)
        self.copies = []

    def start(self, source, target, peer):
        at = len(self.copies)
        copy = pltpu.make_async_remote_copy(
            src_ref=source,
            dst_ref=target,
            send_sem=self.sems[0].at[at],
            recv_sem=self.sems[1].at[at],
            device_id=peer,
            device_id_type=pl.DeviceIdType.MESH,
        )
        copy.start()
        self.copies.append(copy)
        return copy


def subsets(hops):
    found = [(0, 0)]
    for axis, bit in hops:
        more = [(a ^ bit, b) if axis == "wt" else (a, b ^ bit) for a, b in found]
        found = found + more
    return found


def plane_copies(seq_count):
    hops_a, _ = plane_hops(seq_count)
    slow = len(hops_a) - 1
    return (2 * (2**slow - 1), len(set(a for a, _ in subsets(hops_a[:-1]))))


def line_kernel(outer, seq_count, p_ref, wo_ref, s_ref, head_ref, out_ref, small_ref, *sems):
    send_sems, recv_sems, local_sems = sems
    wt, seq = lax.axis_index("wt"), lax.axis_index("seq")
    line, inner = wt // INNER, wt % INNER

    def own_columns(total):
        wide = total // seq_count
        return pl.ds(pl.multiple_of(seq * wide, 128), wide)

    pairs = [
        (s_ref, small_ref),
        (p_ref.at[:, own_columns(p_ref.shape[1])], head_ref),
        (wo_ref.at[:, own_columns(wo_ref.shape[1])], out_ref),
    ]
    own = [
        pltpu.make_async_copy(source, target.at[0], local_sems.at[k])
        for k, (source, target) in enumerate(pairs)
    ]
    for copy in own:
        copy.start()
    peers = [(flip_all(line, d) * INNER + inner, seq) for d in range(1, outer)]
    meet(peers)
    out = Sender(send_sems, recv_sems)
    for source, target in pairs:
        for d in range(1, outer):
            out.start(source, target.at[d], peers[d - 1])
    for copy in own:
        copy.wait()
    for copy in out.copies:
        copy.wait()


def gather_line(packed, w_out, small):
    outer = lax.axis_size("wt") // INNER
    seq_count = lax.axis_size("seq")
    share, head_width = packed.shape
    vmem = pl.BlockSpec(memory_space=pltpu.VMEM)
    copies = 3 * (outer - 1)
    sent = 2 * outer * share * (head_width + w_out.shape[1])
    return pl.pallas_call(
        functools.partial(line_kernel, outer, seq_count),
        in_specs=[vmem] * 3,
        out_specs=[vmem] * 3,
        out_shape=[
            jax.ShapeDtypeStruct((outer, share, head_width // seq_count), low),
            jax.ShapeDtypeStruct((outer, share, w_out.shape[1] // seq_count), low),
            jax.ShapeDtypeStruct((outer,) + small.shape, low),
        ],
        scratch_shapes=[
            pltpu.SemaphoreType.DMA((copies,)),
            pltpu.SemaphoreType.DMA((copies,)),
            pltpu.SemaphoreType.DMA((3,)),
        ],
        compiler_params=pltpu.CompilerParams(collective_id=3, has_side_effects=True),
        cost_estimate=pl.CostEstimate(flops=0, bytes_accessed=8 * sent, transcendentals=0),
        name="gather_line",
    )(packed, w_out, small)


def gather_kernel(
    outer, seq_count, x_ref, p_ref, wo_ref, s_ref, cos_ref, sin_ref,
    normed_ref, qkv_ref, vec_ref, head_ref, out_ref,
    w_scr, o_scr, s_scr, send_sems, recv_sems, local_sems,
):
    share, head_width = p_ref.shape[1], w_scr.shape[3]
    width = x_ref.shape[1]
    wt, seq = lax.axis_index("wt"), lax.axis_index("seq")
    line, inner = wt // INNER, wt % INNER
    hops = plane_hops(seq_count)
    slow = len(hops[0]) - 1
    peers = [(wt - inner + flip(inner, bit), seq) for bit in inner_bits()]
    peers += [(wt, flip(seq, bit)) for _, bit in bits_of("seq", seq_count)]

    def own_columns(total):
        wide = total // seq_count
        return pl.ds(pl.multiple_of(seq * wide, 128), wide)

    fill = []
    for d in range(outer):
        at = flip_all(line, d)
        pairs = [
            (s_ref.at[d], s_scr.at[at, inner]),
            (p_ref.at[d], w_scr.at[at, inner, :, own_columns(head_width)]),
            (wo_ref.at[d], o_scr.at[at, inner, :, own_columns(o_scr.shape[3])]),
        ]
        fill += [
            pltpu.make_async_copy(source, target, local_sems.at[3 * d + k])
            for k, (source, target) in enumerate(pairs)
        ]
    for copy in fill:
        copy.start()
    meet(peers)
    out = Sender(send_sems, recv_sems)

    def hop_peer(hop):
        axis, bit = hop
        if axis == "wt":
            return (wt - inner + flip(inner, bit), seq)
        return (wt, flip(seq, bit))

    def columns(total, part, half):
        wide = total // seq_count
        first = -(-wide // 256) * 128
        start = part * wide + half * first
        return pl.ds(pl.multiple_of(start, 128), wide - first if half else first)

    def start_stage(scratch, at, stage):
        total = scratch.shape[-1]
        copies = []
        if stage < slow:
            for half in range(2):
                hop = hops[half][stage]
                for a, b in subsets(hops[half][:stage]):
                    place = scratch.at[
                        at, flip_all(inner, a), :, columns(total, flip_all(seq, b), half)
                    ]
                    copies.append(out.start(place, place, hop_peer(hop)))
            return copies
        for a in sorted(set(a for a, _ in subsets(hops[0][:slow]))):
            place = scratch.at[at, flip_all(inner, a)]
            copies.append(out.start(place, place, hop_peer(hops[0][slow])))
        return copies

    def arrive(copies):
        for copy in copies:
            if copy is not None:
                copy.wait_recv()

    for copy in fill:
        copy.wait()
    waiting = [[] for _ in range(outer)]
    small_wait = []
    for step in range(outer + slow + 1):
        for stage in range(slow + 1):
            d = step - stage
            if 0 <= d < outer:
                arrive(waiting[d])
                waiting[d] = start_stage(w_scr, flip_all(line, d), stage)
        if step < len(inner_bits()):
            arrive(small_wait)
            bit = inner_bits()[::-1][step]
            small_wait = []
            for a, _ in subsets([("wt", b) for b in inner_bits()[::-1][:step]]):
                place = s_scr.at[:, flip_all(inner, a)]
                small_wait.append(out.start(place, place, hop_peer(("wt", bit))))
    arrive(small_wait)
    out_wait = start_stage(o_scr, slice(None), 0)

    count = outer * INNER
    bias_k = share * KV_HEADS * HEAD_DIM // (HEADS * HEAD_DIM)
    query_width = HEADS * HEAD_DIM
    pair_width = KV_HEADS * HEAD_DIM
    vec_ref[...] = jnp.zeros_like(vec_ref)
    for k in range(count):
        small = s_scr[k // INNER, k % INNER].astype(full)
        at = k * share
        vec_ref[0:1, at : at + share] = small[0:1, :share]
        vec_ref[1:2, at : at + share] = small[1:2, :share]
        at = query_width + k * bias_k
        vec_ref[1:2, at : at + bias_k] = small[2:3, :bias_k]
        at = query_width + pair_width + k * bias_k
        vec_ref[1:2, at : at + bias_k] = small[3:4, :bias_k]
        at = k * share
        vec_ref[2:3, at : at + share] = small[4:5, :share]

    values = x_ref[...].astype(full)
    factor = lax.rsqrt(jnp.mean(values * values, axis=-1, keepdims=True) + epsilon)
    normed_ref[...] = (values * factor * vec_ref[0:1, :width]).astype(low)
    for d in range(outer):
        arrive(waiting[d])
    keep_head = pltpu.make_async_copy(w_scr, head_ref, local_sems.at[0])
    keep_head.start()
    wide = 2 * HEAD_DIM
    blocks = head_width // wide

    def project(at):
        weights = w_scr[:, :, :, pl.ds(at, wide)].reshape(width, wide)
        return (
            jnp.dot(normed_ref[...], weights, preferred_element_type=full)
            + vec_ref[1:2, pl.ds(at, wide)]
        )

    def turn_block(k):
        at = pl.multiple_of(k * wide, wide)
        got = project(at)
        for j in range(2):
            part = got[:, j * HEAD_DIM : (j + 1) * HEAD_DIM]
            turned = part * cos_ref[...] + pltpu.roll(part, HEAD_DIM // 2, 1) * sin_ref[...]
            where = pl.multiple_of(at + j * HEAD_DIM, HEAD_DIM)
            qkv_ref[:, pl.ds(where, HEAD_DIM)] = turned.astype(low)

    turned_blocks = blocks - pair_width // wide
    marks = [turned_blocks * (k + 1) // (slow + 1) for k in range(slow + 1)]
    begin = 0
    for stage in range(slow + 1):
        @pl.loop(begin, marks[stage])
        def _(k):
            turn_block(k)

        begin = marks[stage]
        arrive(out_wait)
        out_wait = start_stage(o_scr, slice(None), stage + 1) if stage < slow else []
    for k in range(turned_blocks, blocks):
        qkv_ref[:, k * wide : (k + 1) * wide] = project(k * wide).astype(low)
    keep_out = pltpu.make_async_copy(o_scr, out_ref, local_sems.at[1])
    keep_out.start()
    for copy in out.copies:
        copy.wait_send()
    keep_head.wait()
    keep_out.wait()


def gather_project(tokens, packed, w_out, small, cosine, sine):
    outer = lax.axis_size("wt") // INNER
    seq_count = lax.axis_size("seq")
    rows, width = tokens.shape
    share, head_width = packed.shape[1], packed.shape[2] * seq_count
    out_width = w_out.shape[2] * seq_count
    slow_copies, last_copies = plane_copies(seq_count)
    each = slow_copies + last_copies
    small_copies = 2 ** len(inner_bits()) - 1
    copies = (outer + 1) * each + small_copies
    vmem = pl.BlockSpec(memory_space=pltpu.VMEM)
    anywhere = pl.BlockSpec(memory_space=pl.ANY)
    sent = 2 * outer * INNER * share * (head_width + out_width)
    return pl.pallas_call(
        functools.partial(gather_kernel, outer, seq_count),
        in_specs=[vmem] * 6,
        out_specs=[vmem, vmem, vmem, anywhere, anywhere],
        out_shape=[
            jax.ShapeDtypeStruct((rows, width), low),
            jax.ShapeDtypeStruct((rows, head_width), low),
            jax.ShapeDtypeStruct((8, head_width), full),
            jax.ShapeDtypeStruct((outer, INNER, share, head_width), low),
            jax.ShapeDtypeStruct((outer, INNER, share, out_width), low),
        ],
        scratch_shapes=[
            pltpu.VMEM((outer, INNER, share, head_width), low),
            pltpu.VMEM((outer, INNER, share, out_width), low),
            pltpu.VMEM((outer, INNER) + small.shape[1:], low),
            pltpu.SemaphoreType.DMA((copies,)),
            pltpu.SemaphoreType.DMA((copies,)),
            pltpu.SemaphoreType.DMA((3 * outer,)),
        ],
        compiler_params=pltpu.CompilerParams(
            collective_id=1, has_side_effects=True, vmem_limit_bytes=48 << 20
        ),
        cost_estimate=pl.CostEstimate(
            flops=2 * rows * width * head_width * 8, bytes_accessed=2 * sent, transcendentals=0
        ),
        name="gather_project",
    )(tokens, packed, w_out, small, cosine, sine)


def near_inner(seq_count):
    hops = plane_hops(seq_count)[0]
    return sorted(set(a for a, _ in subsets(hops[:-1])))


def reduce_kernel(outer, seq_count, count, u_ref, *refs):
    refs = list(refs)
    units_ref = refs.pop(2 * count)
    own_sem = refs.pop()
    given, results = refs[:count], refs[count : 2 * count]
    slow = len(plane_hops(seq_count)[0]) - 1
    held = refs[2 * count : 3 * count]
    lines = refs[3 * count : 4 * count]
    joined = refs[4 * count : 5 * count]
    landed = refs[5 * count : (6 + slow) * count]
    send_sems, recv_sems = refs[(6 + slow) * count :]
    wt, seq = lax.axis_index("wt"), lax.axis_index("seq")
    line, inner = wt // INNER, wt % INNER
    hops = plane_hops(seq_count)
    nears = near_inner(seq_count)
    peers = [(flip_all(line, d) * INNER + inner, seq) for d in range(1, outer)]
    peers += [
        (wt - inner + flip_all(inner, a), flip_all(seq, b))
        for b in range(seq_count)
        for a in range(INNER)
        if a or b
    ]
    keep = pltpu.make_async_copy(u_ref.at[inner], units_ref.at[0, 0], own_sem.at[0])
    keep.start()
    meet(peers)
    out = Sender(send_sems, recv_sems)

    def hop_peer(hop):
        axis, bit = hop
        if axis == "wt":
            return (wt - inner + flip(inner, bit), seq)
        return (wt, flip(seq, bit))

    def columns(total, part, half):
        wide = total // seq_count
        first = -(-wide // 256) * 128
        start = part * wide + half * first
        return pl.ds(pl.multiple_of(start, 128), wide - first if half else first)

    def arrive(copies):
        for copy in copies:
            copy.wait_recv()

    def steps(k):
        source, total = given[k], given[k].shape[3]
        sums, wide = held[k], given[k].shape[3] // seq_count
        own = pl.ds(pl.multiple_of(seq * wide, 128), wide)
        core = hops[0][slow]
        copies = [
            out.start(
                source.at[:, flip_all(inner, a ^ core[1])],
                landed[k].at[:, at],
                hop_peer(core),
            )
            for at, a in enumerate(nears)
        ]
        yield
        arrive(copies)
        for at, a in enumerate(nears):
            place = flip_all(inner, a)

            @pl.loop(0, outer)
            def _(o):
                both = source[o, place].astype(full) + landed[k][o, at].astype(full)
                sums[o, at] = both.astype(low)

        for stage in range(slow - 1, -1, -1):
            target = landed[(1 + stage) * count + k]
            copies, blocks = [], []
            for half in range(2):
                axis, bit = hops[half][stage]
                for a, b in subsets(hops[half][:stage]):
                    from_a = a ^ bit if axis == "wt" else a
                    from_b = b ^ bit if axis == "seq" else b
                    sent = columns(total, flip_all(seq, from_b), half)
                    copies.append(
                        out.start(
                            sums.at[:, nears.index(from_a), :, sent],
                            target.at[:, nears.index(a), :, sent],
                            hop_peer((axis, bit)),
                        )
                    )
                    blocks.append((nears.index(a), columns(total, flip_all(seq, b), half)))
            yield
            arrive(copies)
            for at, part in blocks:

                @pl.loop(0, outer)
                def _(o):
                    both = sums[o, at, :, part].astype(full) + target[o, at, :, part].astype(full)
                    sums[o, at, :, part] = both.astype(low)

        copies = [
            out.start(
                sums.at[flip_all(line, d), 0, :, own],
                lines[k].at[d],
                (flip_all(line, d) * INNER + inner, seq),
            )
            for d in range(1, outer)
        ]
        yield
        arrive(copies)
        both = sums[line, 0, :, own].astype(full)
        for d in range(1, outer):
            both = both + lines[k][d].astype(full)
        joined[k][:, own] = both.astype(low)
        copies = [
            out.start(joined[k].at[:, own], joined[k].at[:, own], (wt, flip_all(seq, d)))
            for d in range(1, seq_count)
        ]
        yield
        arrive(copies)
        results[k][...] = joined[k][...].astype(full)

    def exchange():
        copies = []
        for b in range(seq_count):
            copies += [
                out.start(
                    u_ref.at[flip_all(inner, a)],
                    units_ref.at[b, a],
                    (wt - inner + flip_all(inner, a), flip_all(seq, b)),
                )
                for a in range(INNER)
                if a or b
            ]
            if b == 0:
                for _ in range(slow + 1):
                    yield
        yield
        arrive(copies)

    running = [steps(k) for k in range(count)] + [exchange()]
    while running:
        for one in list(running):
            if next(one, "done") == "done":
                running.remove(one)
    for copy in out.copies:
        copy.wait_send()
    keep.wait()


def reduce_shares(units, *partials):
    outer = lax.axis_size("wt") // INNER
    seq_count = lax.axis_size("seq")
    count = len(partials)
    slow = len(plane_hops(seq_count)[0]) - 1
    nears = len(near_inner(seq_count))
    vmem = pl.BlockSpec(memory_space=pltpu.VMEM)
    near = [
        pltpu.VMEM((outer, nears) + p.shape[2:], low) for p in partials
    ]
    shapes = [p.shape[2:] for p in partials]
    copies = count * (nears + 2 * (2**slow - 1) + outer - 1 + seq_count - 1)
    copies += INNER * seq_count - 1
    sent = sum(2 * p.size for p in partials)
    return pl.pallas_call(
        functools.partial(reduce_kernel, outer, seq_count, count),
        in_specs=[vmem] * (count + 1),
        out_specs=[vmem] * (count + 1),
        out_shape=[jax.ShapeDtypeStruct(shape, full) for shape in shapes]
        + [jax.ShapeDtypeStruct((seq_count,) + units.shape, low)],
        scratch_shapes=near
        + [pltpu.VMEM((outer, r, c // seq_count), low) for r, c in shapes]
        + [pltpu.VMEM(shape, low) for shape in shapes]
        + near * (1 + slow)
        + [pltpu.SemaphoreType.DMA((n,)) for n in (copies, copies, 1)],
        compiler_params=pltpu.CompilerParams(
            collective_id=2, has_side_effects=True, vmem_limit_bytes=60 << 20
        ),
        cost_estimate=pl.CostEstimate(flops=0, bytes_accessed=8 * sent, transcendentals=0),
        name="reduce_shares",
    )(units, *partials)


def split_kernel(outer, seq_count, own, info_ref, gate_ref, up_ref, o_ref):
    inner = info_ref[1]
    width = outer * own
    padded = o_ref.shape[2] // 2
    for s in range(seq_count):
        @pl.when(info_ref[0] == s)
        def _():
            for q in range(INNER):
                place = jnp.bitwise_xor(inner, q)
                for k, ref in enumerate((gate_ref, up_ref)):
                    for o in range(outer):
                        at = ((o * INNER + q) * seq_count + s) * own
                        to = k * padded + o * own
                        o_ref[place, :, to : to + own] = ref[:, at : at + own].astype(low)
                    if padded > width:
                        blank = jnp.zeros((o_ref.shape[1], padded - width), low)
                        o_ref[place, :, k * padded + width : (k + 1) * padded] = blank


def split_units(info, gate, up, outer, seq_count, own, padded):
    vmem = pl.BlockSpec(memory_space=pltpu.VMEM)
    return pl.pallas_call(
        functools.partial(split_kernel, outer, seq_count, own),
        in_specs=[pl.BlockSpec(memory_space=pltpu.SMEM), vmem, vmem],
        out_specs=vmem,
        out_shape=jax.ShapeDtypeStruct((INNER, gate.shape[0], 2 * padded), low),
        name="split_units",
    )(info, gate, up)


def join_kernel(outer, seq_count, own, info_ref, u_ref, gate_ref, up_ref):
    seq, inner = info_ref[0], info_ref[1]
    padded = u_ref.shape[3] // 2
    for s in range(seq_count):
        for q in range(INNER):
            block = u_ref[jnp.bitwise_xor(seq, s), jnp.bitwise_xor(inner, q)].astype(full)
            for k, ref in enumerate((gate_ref, up_ref)):
                for o in range(outer):
                    at = ((o * INNER + q) * seq_count + s) * own
                    source = k * padded + o * own
                    ref[:, at : at + own] = block[:, source : source + own]


def join_units(info, units, outer, own):
    seq_count, _, rows, _ = units.shape
    vmem = pl.BlockSpec(memory_space=pltpu.VMEM)
    shape = jax.ShapeDtypeStruct((rows, outer * INNER * seq_count * own), full)
    return pl.pallas_call(
        functools.partial(join_kernel, outer, seq_count, own),
        in_specs=[pl.BlockSpec(memory_space=pltpu.SMEM), vmem],
        out_specs=[vmem, vmem],
        out_shape=[shape, shape],
        name="join_units",
    )(info, units)


def hidden_kernel(both_ref, grad_ref, down_ref, hidden_ref, units_ref):
    wide = hidden_ref.shape[1]
    hidden_grad = lax.dot_general(
        grad_ref[...], down_ref[...], (((1,), (1,)), ((), ())), preferred_element_type=full
    )
    gate, upper = both_ref[:, :wide], both_ref[:, wide:]
    sigma = 1.0 / (1.0 + jnp.exp(-gate))
    taken = gate * sigma
    hidden_ref[...] = (taken * upper).astype(low)
    slope = sigma * (1.0 + gate * (1.0 - sigma))
    units_ref[:, :wide] = (hidden_grad * upper * slope).astype(low)
    units_ref[:, wide:] = (hidden_grad * taken).astype(low)


def hidden_units(both, grad, down_w):
    total, width = grad.shape
    wide = down_w.shape[0]
    block = min(512, total)
    return pl.pallas_call(
        hidden_kernel,
        grid=(total // block,),
        in_specs=[
            pl.BlockSpec((block, 2 * wide), lambda i: (i, 0)),
            pl.BlockSpec((block, width), lambda i: (i, 0)),
            pl.BlockSpec((wide, width), lambda i: (0, 0)),
        ],
        out_specs=[
            pl.BlockSpec((block, wide), lambda i: (i, 0)),
            pl.BlockSpec((block, 2 * wide), lambda i: (i, 0)),
        ],
        out_shape=[
            jax.ShapeDtypeStruct((total, wide), low),
            jax.ShapeDtypeStruct((total, 2 * wide), low),
        ],
        compiler_params=pltpu.CompilerParams(vmem_limit_bytes=56 << 20),
        cost_estimate=pl.CostEstimate(
            flops=2 * total * width * wide,
            bytes_accessed=2 * total * (width + 7 * wide) + 2 * wide * width,
            transcendentals=total * wide,
        ),
        name="hidden_units",
    )(both, grad, down_w)


def after(value, *others):
    return lax.optimization_barrier((value, *others))[0]


def shown(kpos_ref, rows, keys):
    places = lax.broadcasted_iota(jnp.int32, (rows, keys), 0)
    return kpos_ref[...] <= places


def fwd_kernel(kpos_ref, q_ref, k_ref, v_ref, o_ref):
    rows, keys = q_ref.shape[0], k_ref.shape[0]
    scores = (
        lax.dot_general(
            q_ref[...], k_ref[...], (((1,), (1,)), ((), ())), preferred_element_type=full
        )
        * scale
    )
    scores = jnp.where(shown(kpos_ref, rows, keys), scores, masked_score)
    top = jnp.max(scores, axis=-1, keepdims=True)
    weights = jnp.exp(scores - top)
    total = jnp.sum(weights, axis=-1, keepdims=True)
    probs = (weights * (1.0 / total)).astype(low)
    o_ref[...] = jnp.dot(probs, v_ref[...], preferred_element_type=full).astype(low)


def attend_forward(kpos, qkv, pairs):
    rows = qkv.shape[0]
    keys = pairs.shape[0]
    group = HEADS // KV_HEADS
    return pl.pallas_call(
        fwd_kernel,
        grid=(HEADS,),
        in_specs=[
            pl.BlockSpec((1, keys), lambda h: (0, 0)),
            pl.BlockSpec((rows, HEAD_DIM), lambda h: (0, h)),
            pl.BlockSpec((keys, HEAD_DIM), lambda h: (0, h // group)),
            pl.BlockSpec((keys, HEAD_DIM), lambda h: (0, KV_HEADS + h // group)),
        ],
        out_specs=pl.BlockSpec((rows, HEAD_DIM), lambda h: (0, h)),
        out_shape=jax.ShapeDtypeStruct((rows, HEADS * HEAD_DIM), low),
        cost_estimate=pl.CostEstimate(
            flops=4 * rows * keys * HEADS * HEAD_DIM * 3,
            bytes_accessed=4 * rows * HEADS * HEAD_DIM + 4 * keys * KV_HEADS * HEAD_DIM,
            transcendentals=rows * keys * HEADS,
        ),
        name="attend_forward",
    )(kpos, qkv, pairs, pairs)


def bwd_kernel(kpos_ref, cos_ref, sin_ref, q_ref, k_ref, v_ref, g_ref, dq_ref, dk_ref, dv_ref):
    rows, keys = q_ref.shape[0], k_ref.shape[0]
    group = HEADS // KV_HEADS
    head = pl.program_id(0)
    queries, key, value, grad = q_ref[...], k_ref[...], v_ref[...], g_ref[...]
    scores = (
        lax.dot_general(queries, key, (((1,), (1,)), ((), ())), preferred_element_type=full)
        * scale
    )
    scores = jnp.where(shown(kpos_ref, rows, keys), scores, masked_score)
    top = jnp.max(scores, axis=-1, keepdims=True)
    weights = jnp.exp(scores - top)
    total = jnp.sum(weights, axis=-1, keepdims=True)
    probs = weights * (1.0 / total)
    prob_grad = lax.dot_general(
        grad, value, (((1,), (1,)), ((), ())), preferred_element_type=full
    )
    inner = jnp.sum(probs * prob_grad, axis=-1, keepdims=True)
    score_grad = (probs * (prob_grad - inner)).astype(low)
    dv = lax.dot_general(
        probs.astype(low), grad, (((0,), (0,)), ((), ())), preferred_element_type=full
    )
    dk = (
        lax.dot_general(
            score_grad, queries, (((0,), (0,)), ((), ())), preferred_element_type=full
        )
        * scale
    )
    dq = jnp.dot(score_grad, key, preferred_element_type=full) * scale
    turned = dq * cos_ref[...] - pltpu.roll(dq, HEAD_DIM // 2, 1) * sin_ref[...]
    dq_ref[...] = turned.astype(low)

    @pl.when(head % group == 0)
    def _():
        dk_ref[...] = dk
        dv_ref[...] = dv

    @pl.when(head % group != 0)
    def _():
        dk_ref[...] += dk
        dv_ref[...] += dv


def attend_backward(kpos, cosine, sine, qkv, pairs, grad):
    rows = qkv.shape[0]
    keys = pairs.shape[0]
    group = HEADS // KV_HEADS
    width = KV_HEADS * HEAD_DIM
    return pl.pallas_call(
        bwd_kernel,
        grid=(HEADS,),
        in_specs=[
            pl.BlockSpec((1, keys), lambda h: (0, 0)),
            pl.BlockSpec((rows, HEAD_DIM), lambda h: (0, 0)),
            pl.BlockSpec((rows, HEAD_DIM), lambda h: (0, 0)),
            pl.BlockSpec((rows, HEAD_DIM), lambda h: (0, h)),
            pl.BlockSpec((keys, HEAD_DIM), lambda h: (0, h // group)),
            pl.BlockSpec((keys, HEAD_DIM), lambda h: (0, KV_HEADS + h // group)),
            pl.BlockSpec((rows, HEAD_DIM), lambda h: (0, h)),
        ],
        out_specs=[
            pl.BlockSpec((rows, HEAD_DIM), lambda h: (0, h)),
            pl.BlockSpec((keys, HEAD_DIM), lambda h: (0, h // group)),
            pl.BlockSpec((keys, HEAD_DIM), lambda h: (0, h // group)),
        ],
        out_shape=[
            jax.ShapeDtypeStruct((rows, HEADS * HEAD_DIM), low),
            jax.ShapeDtypeStruct((keys, width), full),
            jax.ShapeDtypeStruct((keys, width), full),
        ],
        cost_estimate=pl.CostEstimate(
            flops=10 * rows * keys * HEADS * HEAD_DIM * 3,
            bytes_accessed=8 * rows * HEADS * HEAD_DIM + 12 * keys * width,
            transcendentals=rows * keys * HEADS,
        ),
        name="attend_backward",
    )(kpos, cosine, sine, qkv, pairs, pairs, grad)


def body(
    tokens, lengths, attn_gain, w_query, b_query, w_key, b_key, w_value, b_value, w_out,
    ffn_gain, w_gate, w_up, w_down, cotangent,
):
    slot_count, rows, width = tokens.shape
    seq_count = lax.axis_size("seq")
    wt_count = lax.axis_size("wt")
    outer = wt_count // INNER
    seq_here = lax.axis_index("seq")
    inner_here = lax.axis_index("wt") % INNER
    line = [[o * INNER + i for o in range(outer)] for i in range(INNER)]
    hops_a, hops_b = plane_hops(seq_count)
    plane = INNER * seq_count
    share = w_query.shape[0]
    bias_q, bias_k = b_query.shape[0], b_key.shape[0]
    query_width = HEADS * HEAD_DIM
    pair_width = KV_HEADS * HEAD_DIM
    head_width = query_width + 2 * pair_width
    ff_own = w_down.shape[0] // seq_count
    ff_here = outer * ff_own
    ff_pad = -(-ff_here // 128) * 128

    flat = tokens.astype(full).reshape(rows, width)
    places = seq_here * rows + jnp.arange(rows, dtype=jnp.int32)
    keep = (places < lengths[0])[:, None]
    upstream_low = jnp.where(keep, cotangent.reshape(rows, width), jnp.zeros((), low))

    def line_gather(value):
        return lax.all_gather(value, "wt", axis=0, axis_index_groups=line, tiled=False)

    def line_reduce(value):
        return lax.psum_scatter(
            value, "wt", scatter_dimension=0, axis_index_groups=line, tiled=False
        )

    def seq_gather(value):
        stacked = gather_hops(value, bits_of("seq", seq_count))
        return jnp.stack([to_place(stacked, seq_here ^ p) for p in range(seq_count)])

    info = jnp.stack([seq_here, inner_here]).astype(jnp.int32)
    down_own = lax.dynamic_slice_in_dim(w_down, seq_here * ff_own, ff_own, axis=0).astype(low)

    def inner_swap(value, distance):
        count = lax.axis_size("wt")
        return lax.ppermute(value, "wt", [(i, i ^ distance) for i in range(count)])

    def inner_exchange(value):
        got = [value[0]] + [inner_swap(value[d], d) for d in range(1, INNER)]
        return jnp.stack(got)

    stacked = inner_exchange(split_units(info, w_gate, w_up, outer, seq_count, ff_own, ff_pad))
    block = jnp.stack([to_place(stacked, inner_here ^ p) for p in range(INNER)])
    block = block.reshape(INNER * share, 2 * ff_pad)
    half = HEAD_DIM // 2
    inverse = 10000.0 ** (-jnp.arange(half, dtype=full) / half)
    angle = places.astype(full)[:, None] * inverse[None, :]
    cosine = jnp.cos(angle)
    sine = jnp.sin(angle)
    cosine = jnp.concatenate([cosine, cosine], axis=1)
    sine = jnp.concatenate([-sine, sine], axis=1)

    def line_of(vector):
        return jnp.pad(vector, (0, HEAD_DIM - vector.shape[0]))

    small = jnp.stack([line_of(v) for v in (attn_gain, b_query, b_key, b_value, ffn_gain)])
    small = jnp.pad(small.astype(low), ((0, 11), (0, 0)))
    packed = jnp.concatenate([w_query, w_key, w_value], axis=1).astype(low)
    normed_low, qkv, vectors, head_all, out_all = gather_project(
        tokens.reshape(rows, width),
        *gather_line(packed, w_out.astype(low), small), cosine, sine,
    )
    head_w = head_all.reshape(width, head_width)
    out_w = out_all.reshape(query_width, width)
    gain_one = vectors[0, :width]
    gain_two = vectors[2, :width]
    units_w = line_gather(block).reshape(width, 2 * ff_pad)
    down_w = line_gather(down_own).reshape(ff_here, width)
    down_w = jnp.pad(down_w, ((0, ff_pad - ff_here), (0, 0)))

    seq_hops = bits_of("seq", seq_count)
    pairs = gather_hops(qkv[:, query_width:], seq_hops).reshape(SLOT, 2 * pair_width)
    distance = jnp.arange(SLOT, dtype=jnp.int32)
    key_place = (seq_here ^ (distance // rows)) * rows + distance % rows
    kpos = jnp.where(key_place < lengths[0], key_place - seq_here * rows, far_place)[None, :]
    mixed = attend_forward(kpos, qkv, pairs)
    resid = flat + product(mixed, out_w)
    normed_two, factor_two = norm_rows(resid, gain_two)
    normed_two_low = normed_two.astype(low)

    core = hops_a[-1]
    slow_a, slow_b = hops_a[:-1], hops_b[:-1]
    near_rows = plane * rows // 2

    def spread(block):
        part_a = gather_hops(block[: rows // 2], slow_a)
        part_b = gather_hops(block[rows // 2 :], slow_b)
        near = jnp.stack([part_a, part_b]).reshape(near_rows, width)
        return jnp.concatenate([near, swap(near, core)], axis=0)

    def hop_core(partial):
        other = swap(partial[near_rows:], core)
        near = (partial[:near_rows].astype(full) + other.astype(full)).astype(low)
        near = near.reshape(2, plane // 2, rows // 2, width)
        return (near[0], near[1])

    def hop_slow(parts, stage):
        return tuple(reduce_hop(part, hops[stage]) for part, hops in zip(parts, (slow_a, slow_b)))

    def hop_last(parts):
        got = [reduce_hops(part, hops[:1]) for part, hops in zip(parts, (slow_a, slow_b))]
        return jnp.concatenate(got, axis=0)

    stages = list(range(1, len(slow_a)))[::-1]
    grad_all = spread(after(upstream_low, pairs))
    rows_all = spread(normed_two_low)
    both = product(rows_all, units_w)
    hidden, units_grad = hidden_units(both, grad_all, down_w)
    partial = product_right(units_grad, units_w).astype(low)
    down_grad = product_left(after(hidden, partial), grad_all).astype(low)
    down_grad = down_grad[:ff_here]
    down_line = line_reduce(down_grad.reshape(outer, ff_own, width))
    back = hop_core(partial)
    rows_late, grad_late = lax.optimization_barrier((rows_all, units_grad, back, down_grad))[:2]
    units_w_grad = product_left(rows_late, grad_late).astype(low)
    units_line = line_reduce(units_w_grad.reshape(outer, INNER * share, 2 * ff_pad))
    for stage in stages:
        back = hop_slow(back, stage)
    hidden_late = after(hidden, back, units_w_grad)
    partial = product(hidden_late, down_w).astype(low)
    normed_two_grad = hop_last(back)

    upstream = upstream_low.astype(full)
    resid_norm_grad, gain_two_grad = norm_back(resid, factor_two, gain_two, normed_two_grad)
    resid_grad = upstream + resid_norm_grad
    attn_grad = resid_grad.astype(low)
    mixed_grad = product_right(attn_grad, out_w).astype(low)
    out_w_grad = product_left(mixed, attn_grad).astype(low)
    query_grad, key_part, value_part = attend_backward(
        kpos, cosine, sine, qkv, pairs, mixed_grad
    )
    forth = hop_core(after(partial, normed_two_grad))
    for stage in stages:
        forth = hop_slow(forth, stage)
    forth = hop_last(lax.optimization_barrier((*forth, query_grad))[:2])
    layer_out = jnp.where(keep, resid + forth, 0.0).astype(low)
    layer_out = layer_out.reshape(slot_count, rows, width)

    down_out = seq_gather(down_line)
    down_out = down_out.reshape(seq_count * ff_own, width).astype(full)
    pair_part = jnp.concatenate([key_part, value_part], axis=1)
    pair_sum = reduce_hops(
        pair_part.reshape(seq_count, rows, 2 * pair_width).astype(low), seq_hops
    )
    key_rot_grad = pair_sum[:, :pair_width].reshape(rows, KV_HEADS, HEAD_DIM)
    turned = jnp.concatenate([key_rot_grad[..., half:], key_rot_grad[..., :half]], axis=-1)
    key_grad = key_rot_grad * cosine[:, None, :] - turned * sine[:, None, :]
    head_grad = jnp.concatenate(
        [query_grad, key_grad.reshape(rows, pair_width).astype(low),
         pair_sum[:, pair_width:].astype(low)],
        axis=1,
    )
    head_w_grad = product_left(normed_low, head_grad).astype(low)
    head_b_grad = jnp.sum(head_grad.astype(full), axis=0)
    normed_grad = product_right(head_grad, head_w)
    factor_one = lax.rsqrt(jnp.mean(flat * flat, axis=-1, keepdims=True) + epsilon)
    input_norm_grad, gain_one_grad = norm_back(flat, factor_one, gain_one, normed_grad)
    input_grad = (resid_grad + input_norm_grad).astype(low).reshape(slot_count, rows, width)

    edges = [0, share, share + bias_q]
    edges += [edges[-1] + bias_k, edges[-1] + 2 * bias_k]

    def parts(vector):
        return vector.reshape(wt_count, -1)

    small_grad = jnp.concatenate(
        [
            parts(gain_one_grad),
            parts(head_b_grad[:query_width]),
            parts(head_b_grad[query_width : query_width + pair_width]),
            parts(head_b_grad[query_width + pair_width :]),
            parts(gain_two_grad),
        ],
        axis=1,
    ).astype(low)
    small_grad = jnp.pad(small_grad, ((0, 0), (0, 256 * seq_count - small_grad.shape[1])))
    small_grad = jnp.pad(small_grad[:, None, :], ((0, 0), (0, 15), (0, 0)))

    def by_owner(partial):
        return partial.reshape(outer, INNER, -1, partial.shape[-1])

    heads_out, out_w_out, small_out, units_got = reduce_shares(
        units_line.reshape(INNER, share, 2 * ff_pad), by_owner(head_w_grad), by_owner(out_w_grad), by_owner(small_grad)
    )
    small_out = small_out[0]
    gate_out, up_out = join_units(info, units_got, outer, ff_own)
    return (
        layer_out,
        input_grad,
        small_out[: edges[1]],
        heads_out[:, :query_width],
        small_out[edges[1] : edges[2]],
        heads_out[:, query_width : query_width + pair_width],
        small_out[edges[2] : edges[3]],
        heads_out[:, query_width + pair_width :],
        small_out[edges[3] : edges[4]],
        out_w_out,
        small_out[edges[4] : edges[4] + ffn_gain.shape[0]],
        gate_out,
        up_out,
        down_out,
    )


def solution(mesh):
    by_wt = P("wt")
    by_row = P("wt", None)
    by_token = P("wt", "seq", None)
    return jax.shard_map(
        body,
        mesh=mesh,
        in_specs=(
            by_token, by_wt, by_wt, by_row, by_wt, by_row, by_wt, by_row, by_wt, by_row,
            by_wt, by_row, by_row, by_row, by_token,
        ),
        out_specs=(
            by_token, by_token, by_wt, by_row, by_wt, by_row, by_wt, by_row, by_wt, by_row,
            by_wt, by_row, by_row, by_row,
        ),
        check_vma=False,
    )
```

```python
import functools
import math

import jax
import jax.numpy as jnp
from jax import lax
from jax.experimental import pallas as pl
from jax.experimental.pallas import tpu as pltpu
from jax.sharding import PartitionSpec as P


HEADS = 12
KV_HEADS = 2
HEAD_DIM = 128
SLOT = 1024
INNER = 4

epsilon = 1e-06
masked_score = -1e30
far_place = 1 << 30
scale = 1.0 / math.sqrt(HEAD_DIM)
low = jnp.bfloat16
full = jnp.float32


def product(left, right):
    return jnp.dot(left, right, preferred_element_type=full)


def product_left(left, right):
    return lax.dot_general(left, right, (((0,), (0,)), ((), ())), preferred_element_type=full)


def product_right(left, right):
    return lax.dot_general(left, right, (((1,), (1,)), ((), ())), preferred_element_type=full)


def norm_rows(values, gain):
    factor = lax.rsqrt(jnp.mean(values * values, axis=-1, keepdims=True) + epsilon)
    return (values * factor * gain, factor)


def norm_back(values, factor, gain, upstream):
    weighted = upstream * gain
    inner = jnp.mean(weighted * values, axis=-1, keepdims=True)
    grad_in = factor * weighted - values * (factor * factor * factor) * inner
    grad_gain = jnp.sum(upstream * values * factor, axis=0)
    return (grad_in, grad_gain)


def swap(value, hop):
    axis, bit = hop
    count = lax.axis_size(axis)
    return lax.ppermute(value, axis, [(i, i ^ bit) for i in range(count)])


def gather_hops(block, hops):
    held = block[None]
    for hop in hops:
        held = jnp.concatenate([held, swap(held, hop)], axis=0)
    return held


def reduce_hop(held, hop):
    half = held.shape[0] // 2
    other = swap(held[half:], hop)
    return (held[:half].astype(full) + other.astype(full)).astype(low)


def reduce_hops(held, hops):
    for k in range(len(hops) - 1, 0, -1):
        held = reduce_hop(held, hops[k])
    return held[0].astype(full) + swap(held[1], hops[0]).astype(full)


def bits_of(axis, count):
    found, bit = [], 1
    while bit < count:
        found.append((axis, bit))
        bit *= 2
    return found


def plane_hops(seq_count):
    inner = bits_of("wt", INNER)
    seq = bits_of("seq", seq_count)
    slow = inner[1:] + seq
    return (slow + inner[:1], slow[::-1] + inner[:1])


def to_place(stacked, place):
    return lax.dynamic_index_in_dim(stacked, place, 0, keepdims=False)


def flip(index, bit):
    return index + bit - 2 * bit * ((index // bit) % 2)


def flip_all(index, distance):
    bit = 1
    while bit <= distance:
        if distance & bit:
            index = flip(index, bit)
        bit *= 2
    return index


def inner_bits():
    return [bit for _, bit in bits_of("wt", INNER)]


def meet(peers):
    barrier = pltpu.get_barrier_semaphore()
    for peer in peers:
        pl.semaphore_signal(
            barrier, inc=1, device_id=peer, device_id_type=pl.DeviceIdType.MESH
        )
    pl.semaphore_wait(barrier, len(peers))


class Sender:
    def __init__(self, send_sems, recv_sems):
        self.sems = (send_sems, recv_sems)
        self.copies = []

    def start(self, source, target, peer):
        at = len(self.copies)
        copy = pltpu.make_async_remote_copy(
            src_ref=source,
            dst_ref=target,
            send_sem=self.sems[0].at[at],
            recv_sem=self.sems[1].at[at],
            device_id=peer,
            device_id_type=pl.DeviceIdType.MESH,
        )
        copy.start()
        self.copies.append(copy)
        return copy


def subsets(hops):
    found = [(0, 0)]
    for axis, bit in hops:
        more = [(a ^ bit, b) if axis == "wt" else (a, b ^ bit) for a, b in found]
        found = found + more
    return found


def plane_copies(seq_count):
    hops_a, _ = plane_hops(seq_count)
    slow = len(hops_a) - 1
    return (2 * (2**slow - 1), len(set(a for a, _ in subsets(hops_a[:-1]))))


def line_kernel(outer, seq_count, p_ref, wo_ref, s_ref, head_ref, out_ref, small_ref, *sems):
    send_sems, recv_sems, local_sems = sems
    wt, seq = lax.axis_index("wt"), lax.axis_index("seq")
    line, inner = wt // INNER, wt % INNER

    def own_columns(total):
        wide = total // seq_count
        return pl.ds(pl.multiple_of(seq * wide, 128), wide)

    pairs = [
        (s_ref, small_ref),
        (p_ref.at[:, own_columns(p_ref.shape[1])], head_ref),
        (wo_ref.at[:, own_columns(wo_ref.shape[1])], out_ref),
    ]
    own = [
        pltpu.make_async_copy(source, target.at[0], local_sems.at[k])
        for k, (source, target) in enumerate(pairs)
    ]
    for copy in own:
        copy.start()
    peers = [(flip_all(line, d) * INNER + inner, seq) for d in range(1, outer)]
    meet(peers)
    out = Sender(send_sems, recv_sems)
    for source, target in pairs:
        for d in range(1, outer):
            out.start(source, target.at[d], peers[d - 1])
    for copy in own:
        copy.wait()
    for copy in out.copies:
        copy.wait()


def gather_line(packed, w_out, small):
    outer = lax.axis_size("wt") // INNER
    seq_count = lax.axis_size("seq")
    share, head_width = packed.shape
    vmem = pl.BlockSpec(memory_space=pltpu.VMEM)
    copies = 3 * (outer - 1)
    sent = 2 * outer * share * (head_width + w_out.shape[1])
    return pl.pallas_call(
        functools.partial(line_kernel, outer, seq_count),
        in_specs=[vmem] * 3,
        out_specs=[vmem] * 3,
        out_shape=[
            jax.ShapeDtypeStruct((outer, share, head_width // seq_count), low),
            jax.ShapeDtypeStruct((outer, share, w_out.shape[1] // seq_count), low),
            jax.ShapeDtypeStruct((outer,) + small.shape, low),
        ],
        scratch_shapes=[
            pltpu.SemaphoreType.DMA((copies,)),
            pltpu.SemaphoreType.DMA((copies,)),
            pltpu.SemaphoreType.DMA((3,)),
        ],
        compiler_params=pltpu.CompilerParams(collective_id=3, has_side_effects=True),
        cost_estimate=pl.CostEstimate(flops=0, bytes_accessed=8 * sent, transcendentals=0),
        name="gather_line",
    )(packed, w_out, small)


def gather_kernel(
    outer, seq_count, x_ref, p_ref, wo_ref, s_ref, cos_ref, sin_ref,
    normed_ref, qkv_ref, vec_ref, head_ref, out_ref,
    w_scr, o_scr, s_scr, send_sems, recv_sems, local_sems,
):
    share, head_width = p_ref.shape[1], w_scr.shape[3]
    width = x_ref.shape[1]
    wt, seq = lax.axis_index("wt"), lax.axis_index("seq")
    line, inner = wt // INNER, wt % INNER
    hops = plane_hops(seq_count)
    slow = len(hops[0]) - 1
    peers = [(wt - inner + flip(inner, bit), seq) for bit in inner_bits()]
    peers += [(wt, flip(seq, bit)) for _, bit in bits_of("seq", seq_count)]

    def own_columns(total):
        wide = total // seq_count
        return pl.ds(pl.multiple_of(seq * wide, 128), wide)

    fill = []
    for d in range(outer):
        at = flip_all(line, d)
        pairs = [
            (s_ref.at[d], s_scr.at[at, inner]),
            (p_ref.at[d], w_scr.at[at, inner, :, own_columns(head_width)]),
            (wo_ref.at[d], o_scr.at[at, inner, :, own_columns(o_scr.shape[3])]),
        ]
        fill += [
            pltpu.make_async_copy(source, target, local_sems.at[3 * d + k])
            for k, (source, target) in enumerate(pairs)
        ]
    for copy in fill:
        copy.start()
    meet(peers)
    out = Sender(send_sems, recv_sems)

    def hop_peer(hop):
        axis, bit = hop
        if axis == "wt":
            return (wt - inner + flip(inner, bit), seq)
        return (wt, flip(seq, bit))

    def columns(total, part, half):
        wide = total // seq_count
        first = -(-wide // 256) * 128
        start = part * wide + half * first
        return pl.ds(pl.multiple_of(start, 128), wide - first if half else first)

    def start_stage(scratch, at, stage):
        total = scratch.shape[-1]
        copies = []
        if stage < slow:
            for half in range(2):
                hop = hops[half][stage]
                for a, b in subsets(hops[half][:stage]):
                    place = scratch.at[
                        at, flip_all(inner, a), :, columns(total, flip_all(seq, b), half)
                    ]
                    copies.append(out.start(place, place, hop_peer(hop)))
            return copies
        for a in sorted(set(a for a, _ in subsets(hops[0][:slow]))):
            place = scratch.at[at, flip_all(inner, a)]
            copies.append(out.start(place, place, hop_peer(hops[0][slow])))
        return copies

    def arrive(copies):
        for copy in copies:
            if copy is not None:
                copy.wait_recv()

    for copy in fill:
        copy.wait()
    waiting = [[] for _ in range(outer)]
    small_wait = []
    for step in range(outer + slow + 1):
        for stage in range(slow + 1):
            d = step - stage
            if 0 <= d < outer:
                arrive(waiting[d])
                waiting[d] = start_stage(w_scr, flip_all(line, d), stage)
        if step < len(inner_bits()):
            arrive(small_wait)
            bit = inner_bits()[::-1][step]
            small_wait = []
            for a, _ in subsets([("wt", b) for b in inner_bits()[::-1][:step]]):
                place = s_scr.at[:, flip_all(inner, a)]
                small_wait.append(out.start(place, place, hop_peer(("wt", bit))))
    arrive(small_wait)
    out_wait = start_stage(o_scr, slice(None), 0)

    count = outer * INNER
    bias_k = share * KV_HEADS * HEAD_DIM // (HEADS * HEAD_DIM)
    query_width = HEADS * HEAD_DIM
    pair_width = KV_HEADS * HEAD_DIM
    vec_ref[...] = jnp.zeros_like(vec_ref)
    for k in range(count):
        small = s_scr[k // INNER, k % INNER].astype(full)
        at = k * share
        vec_ref[0:1, at : at + share] = small[0:1, :share]
        vec_ref[1:2, at : at + share] = small[1:2, :share]
        at = query_width + k * bias_k
        vec_ref[1:2, at : at + bias_k] = small[2:3, :bias_k]
        at = query_width + pair_width + k * bias_k
        vec_ref[1:2, at : at + bias_k] = small[3:4, :bias_k]
        at = k * share
        vec_ref[2:3, at : at + share] = small[4:5, :share]

    values = x_ref[...].astype(full)
    factor = lax.rsqrt(jnp.mean(values * values, axis=-1, keepdims=True) + epsilon)
    normed_ref[...] = (values * factor * vec_ref[0:1, :width]).astype(low)
    for d in range(outer):
        arrive(waiting[d])
    keep_head = pltpu.make_async_copy(w_scr, head_ref, local_sems.at[0])
    keep_head.start()
    wide = 2 * HEAD_DIM
    blocks = head_width // wide

    def project(at):
        weights = w_scr[:, :, :, pl.ds(at, wide)].reshape(width, wide)
        return (
            jnp.dot(normed_ref[...], weights, preferred_element_type=full)
            + vec_ref[1:2, pl.ds(at, wide)]
        )

    def turn_block(k):
        at = pl.multiple_of(k * wide, wide)
        got = project(at)
        for j in range(2):
            part = got[:, j * HEAD_DIM : (j + 1) * HEAD_DIM]
            turned = part * cos_ref[...] + pltpu.roll(part, HEAD_DIM // 2, 1) * sin_ref[...]
            where = pl.multiple_of(at + j * HEAD_DIM, HEAD_DIM)
            qkv_ref[:, pl.ds(where, HEAD_DIM)] = turned.astype(low)

    turned_blocks = blocks - pair_width // wide
    marks = [turned_blocks * (k + 1) // (slow + 1) for k in range(slow + 1)]
    begin = 0
    for stage in range(slow + 1):
        @pl.loop(begin, marks[stage])
        def _(k):
            turn_block(k)

        begin = marks[stage]
        arrive(out_wait)
        out_wait = start_stage(o_scr, slice(None), stage + 1) if stage < slow else []
    for k in range(turned_blocks, blocks):
        qkv_ref[:, k * wide : (k + 1) * wide] = project(k * wide).astype(low)
    keep_out = pltpu.make_async_copy(o_scr, out_ref, local_sems.at[1])
    keep_out.start()
    for copy in out.copies:
        copy.wait_send()
    keep_head.wait()
    keep_out.wait()


def gather_project(tokens, packed, w_out, small, cosine, sine):
    outer = lax.axis_size("wt") // INNER
    seq_count = lax.axis_size("seq")
    rows, width = tokens.shape
    share, head_width = packed.shape[1], packed.shape[2] * seq_count
    out_width = w_out.shape[2] * seq_count
    slow_copies, last_copies = plane_copies(seq_count)
    each = slow_copies + last_copies
    small_copies = 2 ** len(inner_bits()) - 1
    copies = (outer + 1) * each + small_copies
    vmem = pl.BlockSpec(memory_space=pltpu.VMEM)
    anywhere = pl.BlockSpec(memory_space=pl.ANY)
    sent = 2 * outer * INNER * share * (head_width + out_width)
    return pl.pallas_call(
        functools.partial(gather_kernel, outer, seq_count),
        in_specs=[vmem] * 6,
        out_specs=[vmem, vmem, vmem, anywhere, anywhere],
        out_shape=[
            jax.ShapeDtypeStruct((rows, width), low),
            jax.ShapeDtypeStruct((rows, head_width), low),
            jax.ShapeDtypeStruct((8, head_width), full),
            jax.ShapeDtypeStruct((outer, INNER, share, head_width), low),
            jax.ShapeDtypeStruct((outer, INNER, share, out_width), low),
        ],
        scratch_shapes=[
            pltpu.VMEM((outer, INNER, share, head_width), low),
            pltpu.VMEM((outer, INNER, share, out_width), low),
            pltpu.VMEM((outer, INNER) + small.shape[1:], low),
            pltpu.SemaphoreType.DMA((copies,)),
            pltpu.SemaphoreType.DMA((copies,)),
            pltpu.SemaphoreType.DMA((3 * outer,)),
        ],
        compiler_params=pltpu.CompilerParams(
            collective_id=1, has_side_effects=True, vmem_limit_bytes=48 << 20
        ),
        cost_estimate=pl.CostEstimate(
            flops=2 * rows * width * head_width * 8, bytes_accessed=2 * sent, transcendentals=0
        ),
        name="gather_project",
    )(tokens, packed, w_out, small, cosine, sine)


def near_inner(seq_count):
    hops = plane_hops(seq_count)[0]
    return sorted(set(a for a, _ in subsets(hops[:-1])))


def reduce_kernel(outer, seq_count, count, u_ref, *refs):
    refs = list(refs)
    units_ref = refs.pop(2 * count)
    own_sem = refs.pop()
    given, results = refs[:count], refs[count : 2 * count]
    slow = len(plane_hops(seq_count)[0]) - 1
    held = refs[2 * count : 3 * count]
    lines = refs[3 * count : 4 * count]
    joined = refs[4 * count : 5 * count]
    landed = refs[5 * count : (6 + slow) * count]
    send_sems, recv_sems = refs[(6 + slow) * count :]
    wt, seq = lax.axis_index("wt"), lax.axis_index("seq")
    line, inner = wt // INNER, wt % INNER
    hops = plane_hops(seq_count)
    nears = near_inner(seq_count)
    peers = [(flip_all(line, d) * INNER + inner, seq) for d in range(1, outer)]
    peers += [
        (wt - inner + flip_all(inner, a), flip_all(seq, b))
        for b in range(seq_count)
        for a in range(INNER)
        if a or b
    ]
    keep = pltpu.make_async_copy(u_ref.at[inner], units_ref.at[0, 0], own_sem.at[0])
    keep.start()
    meet(peers)
    out = Sender(send_sems, recv_sems)

    def hop_peer(hop):
        axis, bit = hop
        if axis == "wt":
            return (wt - inner + flip(inner, bit), seq)
        return (wt, flip(seq, bit))

    def columns(total, part, half):
        wide = total // seq_count
        first = -(-wide // 256) * 128
        start = part * wide + half * first
        return pl.ds(pl.multiple_of(start, 128), wide - first if half else first)

    def arrive(copies):
        for copy in copies:
            copy.wait_recv()

    def steps(k):
        source, total = given[k], given[k].shape[3]
        sums, wide = held[k], given[k].shape[3] // seq_count
        own = pl.ds(pl.multiple_of(seq * wide, 128), wide)
        core = hops[0][slow]
        copies = [
            out.start(
                source.at[:, flip_all(inner, a ^ core[1])],
                landed[k].at[:, at],
                hop_peer(core),
            )
            for at, a in enumerate(nears)
        ]
        yield
        arrive(copies)
        for at, a in enumerate(nears):
            place = flip_all(inner, a)

            @pl.loop(0, outer)
            def _(o):
                both = source[o, place].astype(full) + landed[k][o, at].astype(full)
                sums[o, at] = both.astype(low)

        for stage in range(slow - 1, -1, -1):
            target = landed[(1 + stage) * count + k]
            copies, blocks = [], []
            for half in range(2):
                axis, bit = hops[half][stage]
                for a, b in subsets(hops[half][:stage]):
                    from_a = a ^ bit if axis == "wt" else a
                    from_b = b ^ bit if axis == "seq" else b
                    sent = columns(total, flip_all(seq, from_b), half)
                    copies.append(
                        out.start(
                            sums.at[:, nears.index(from_a), :, sent],
                            target.at[:, nears.index(a), :, sent],
                            hop_peer((axis, bit)),
                        )
                    )
                    blocks.append((nears.index(a), columns(total, flip_all(seq, b), half)))
            yield
            arrive(copies)
            for at, part in blocks:

                @pl.loop(0, outer)
                def _(o):
                    both = sums[o, at, :, part].astype(full) + target[o, at, :, part].astype(full)
                    sums[o, at, :, part] = both.astype(low)

        copies = [
            out.start(
                sums.at[flip_all(line, d), 0, :, own],
                lines[k].at[d],
                (flip_all(line, d) * INNER + inner, seq),
            )
            for d in range(1, outer)
        ]
        yield
        arrive(copies)
        both = sums[line, 0, :, own].astype(full)
        for d in range(1, outer):
            both = both + lines[k][d].astype(full)
        joined[k][:, own] = both.astype(low)
        copies = [
            out.start(joined[k].at[:, own], joined[k].at[:, own], (wt, flip_all(seq, d)))
            for d in range(1, seq_count)
        ]
        yield
        arrive(copies)
        results[k][...] = joined[k][...].astype(full)

    def exchange():
        copies = []
        for b in range(seq_count):
            copies += [
                out.start(
                    u_ref.at[flip_all(inner, a)],
                    units_ref.at[b, a],
                    (wt - inner + flip_all(inner, a), flip_all(seq, b)),
                )
                for a in range(INNER)
                if a or b
            ]
            if b == 0:
                for _ in range(slow + 1):
                    yield
        yield
        arrive(copies)

    running = [steps(k) for k in range(count)] + [exchange()]
    for _ in range(2):
        next(running[0])
    while running:
        for one in list(running):
            if next(one, "done") == "done":
                running.remove(one)
    for copy in out.copies:
        copy.wait_send()
    keep.wait()


def reduce_shares(units, *partials):
    outer = lax.axis_size("wt") // INNER
    seq_count = lax.axis_size("seq")
    count = len(partials)
    slow = len(plane_hops(seq_count)[0]) - 1
    nears = len(near_inner(seq_count))
    vmem = pl.BlockSpec(memory_space=pltpu.VMEM)
    near = [
        pltpu.VMEM((outer, nears) + p.shape[2:], low) for p in partials
    ]
    shapes = [p.shape[2:] for p in partials]
    copies = count * (nears + 2 * (2**slow - 1) + outer - 1 + seq_count - 1)
    copies += INNER * seq_count - 1
    sent = sum(2 * p.size for p in partials)
    return pl.pallas_call(
        functools.partial(reduce_kernel, outer, seq_count, count),
        in_specs=[vmem] * (count + 1),
        out_specs=[vmem] * (count + 1),
        out_shape=[jax.ShapeDtypeStruct(shape, full) for shape in shapes]
        + [jax.ShapeDtypeStruct((seq_count,) + units.shape, low)],
        scratch_shapes=near
        + [pltpu.VMEM((outer, r, c // seq_count), low) for r, c in shapes]
        + [pltpu.VMEM(shape, low) for shape in shapes]
        + near * (1 + slow)
        + [pltpu.SemaphoreType.DMA((n,)) for n in (copies, copies, 1)],
        compiler_params=pltpu.CompilerParams(
            collective_id=2, has_side_effects=True, vmem_limit_bytes=60 << 20
        ),
        cost_estimate=pl.CostEstimate(flops=0, bytes_accessed=8 * sent, transcendentals=0),
        name="reduce_shares",
    )(units, *partials)


def split_kernel(outer, seq_count, own, info_ref, gate_ref, up_ref, o_ref):
    inner = info_ref[1]
    width = outer * own
    padded = o_ref.shape[2] // 2
    for s in range(seq_count):
        @pl.when(info_ref[0] == s)
        def _():
            for q in range(INNER):
                place = jnp.bitwise_xor(inner, q)
                for k, ref in enumerate((gate_ref, up_ref)):
                    for o in range(outer):
                        at = ((o * INNER + q) * seq_count + s) * own
                        to = k * padded + o * own
                        o_ref[place, :, to : to + own] = ref[:, at : at + own].astype(low)
                    if padded > width:
                        blank = jnp.zeros((o_ref.shape[1], padded - width), low)
                        o_ref[place, :, k * padded + width : (k + 1) * padded] = blank


def split_units(info, gate, up, outer, seq_count, own, padded):
    vmem = pl.BlockSpec(memory_space=pltpu.VMEM)
    return pl.pallas_call(
        functools.partial(split_kernel, outer, seq_count, own),
        in_specs=[pl.BlockSpec(memory_space=pltpu.SMEM), vmem, vmem],
        out_specs=vmem,
        out_shape=jax.ShapeDtypeStruct((INNER, gate.shape[0], 2 * padded), low),
        name="split_units",
    )(info, gate, up)


def join_kernel(outer, seq_count, own, info_ref, u_ref, gate_ref, up_ref):
    seq, inner = info_ref[0], info_ref[1]
    padded = u_ref.shape[3] // 2
    for s in range(seq_count):
        for q in range(INNER):
            block = u_ref[jnp.bitwise_xor(seq, s), jnp.bitwise_xor(inner, q)].astype(full)
            for k, ref in enumerate((gate_ref, up_ref)):
                for o in range(outer):
                    at = ((o * INNER + q) * seq_count + s) * own
                    source = k * padded + o * own
                    ref[:, at : at + own] = block[:, source : source + own]


def join_units(info, units, outer, own):
    seq_count, _, rows, _ = units.shape
    vmem = pl.BlockSpec(memory_space=pltpu.VMEM)
    shape = jax.ShapeDtypeStruct((rows, outer * INNER * seq_count * own), full)
    return pl.pallas_call(
        functools.partial(join_kernel, outer, seq_count, own),
        in_specs=[pl.BlockSpec(memory_space=pltpu.SMEM), vmem],
        out_specs=[vmem, vmem],
        out_shape=[shape, shape],
        name="join_units",
    )(info, units)


def hidden_kernel(both_ref, grad_ref, down_ref, hidden_ref, units_ref):
    wide = hidden_ref.shape[1]
    hidden_grad = lax.dot_general(
        grad_ref[...], down_ref[...], (((1,), (1,)), ((), ())), preferred_element_type=full
    )
    gate, upper = both_ref[:, :wide], both_ref[:, wide:]
    sigma = 1.0 / (1.0 + jnp.exp(-gate))
    taken = gate * sigma
    hidden_ref[...] = (taken * upper).astype(low)
    slope = sigma * (1.0 + gate * (1.0 - sigma))
    units_ref[:, :wide] = (hidden_grad * upper * slope).astype(low)
    units_ref[:, wide:] = (hidden_grad * taken).astype(low)


def hidden_units(both, grad, down_w):
    total, width = grad.shape
    wide = down_w.shape[0]
    block = min(512, total)
    return pl.pallas_call(
        hidden_kernel,
        grid=(total // block,),
        in_specs=[
            pl.BlockSpec((block, 2 * wide), lambda i: (i, 0)),
            pl.BlockSpec((block, width), lambda i: (i, 0)),
            pl.BlockSpec((wide, width), lambda i: (0, 0)),
        ],
        out_specs=[
            pl.BlockSpec((block, wide), lambda i: (i, 0)),
            pl.BlockSpec((block, 2 * wide), lambda i: (i, 0)),
        ],
        out_shape=[
            jax.ShapeDtypeStruct((total, wide), low),
            jax.ShapeDtypeStruct((total, 2 * wide), low),
        ],
        compiler_params=pltpu.CompilerParams(vmem_limit_bytes=56 << 20),
        cost_estimate=pl.CostEstimate(
            flops=2 * total * width * wide,
            bytes_accessed=2 * total * (width + 7 * wide) + 2 * wide * width,
            transcendentals=total * wide,
        ),
        name="hidden_units",
    )(both, grad, down_w)


def after(value, *others):
    return lax.optimization_barrier((value, *others))[0]


def shown(kpos_ref, rows, keys):
    places = lax.broadcasted_iota(jnp.int32, (rows, keys), 0)
    return kpos_ref[...] <= places


def fwd_kernel(kpos_ref, q_ref, k_ref, v_ref, o_ref):
    rows, keys = q_ref.shape[0], k_ref.shape[0]
    scores = (
        lax.dot_general(
            q_ref[...], k_ref[...], (((1,), (1,)), ((), ())), preferred_element_type=full
        )
        * scale
    )
    scores = jnp.where(shown(kpos_ref, rows, keys), scores, masked_score)
    top = jnp.max(scores, axis=-1, keepdims=True)
    weights = jnp.exp(scores - top)
    total = jnp.sum(weights, axis=-1, keepdims=True)
    probs = (weights * (1.0 / total)).astype(low)
    o_ref[...] = jnp.dot(probs, v_ref[...], preferred_element_type=full).astype(low)


def attend_forward(kpos, qkv, pairs):
    rows = qkv.shape[0]
    keys = pairs.shape[0]
    group = HEADS // KV_HEADS
    return pl.pallas_call(
        fwd_kernel,
        grid=(HEADS,),
        in_specs=[
            pl.BlockSpec((1, keys), lambda h: (0, 0)),
            pl.BlockSpec((rows, HEAD_DIM), lambda h: (0, h)),
            pl.BlockSpec((keys, HEAD_DIM), lambda h: (0, h // group)),
            pl.BlockSpec((keys, HEAD_DIM), lambda h: (0, KV_HEADS + h // group)),
        ],
        out_specs=pl.BlockSpec((rows, HEAD_DIM), lambda h: (0, h)),
        out_shape=jax.ShapeDtypeStruct((rows, HEADS * HEAD_DIM), low),
        cost_estimate=pl.CostEstimate(
            flops=4 * rows * keys * HEADS * HEAD_DIM * 3,
            bytes_accessed=4 * rows * HEADS * HEAD_DIM + 4 * keys * KV_HEADS * HEAD_DIM,
            transcendentals=rows * keys * HEADS,
        ),
        name="attend_forward",
    )(kpos, qkv, pairs, pairs)


def bwd_kernel(kpos_ref, cos_ref, sin_ref, q_ref, k_ref, v_ref, g_ref, dq_ref, dk_ref, dv_ref):
    rows, keys = q_ref.shape[0], k_ref.shape[0]
    group = HEADS // KV_HEADS
    head = pl.program_id(0)
    queries, key, value, grad = q_ref[...], k_ref[...], v_ref[...], g_ref[...]
    scores = (
        lax.dot_general(queries, key, (((1,), (1,)), ((), ())), preferred_element_type=full)
        * scale
    )
    scores = jnp.where(shown(kpos_ref, rows, keys), scores, masked_score)
    top = jnp.max(scores, axis=-1, keepdims=True)
    weights = jnp.exp(scores - top)
    total = jnp.sum(weights, axis=-1, keepdims=True)
    probs = weights * (1.0 / total)
    prob_grad = lax.dot_general(
        grad, value, (((1,), (1,)), ((), ())), preferred_element_type=full
    )
    inner = jnp.sum(probs * prob_grad, axis=-1, keepdims=True)
    score_grad = (probs * (prob_grad - inner)).astype(low)
    dv = lax.dot_general(
        probs.astype(low), grad, (((0,), (0,)), ((), ())), preferred_element_type=full
    )
    dk = (
        lax.dot_general(
            score_grad, queries, (((0,), (0,)), ((), ())), preferred_element_type=full
        )
        * scale
    )
    dq = jnp.dot(score_grad, key, preferred_element_type=full) * scale
    turned = dq * cos_ref[...] - pltpu.roll(dq, HEAD_DIM // 2, 1) * sin_ref[...]
    dq_ref[...] = turned.astype(low)

    @pl.when(head % group == 0)
    def _():
        dk_ref[...] = dk
        dv_ref[...] = dv

    @pl.when(head % group != 0)
    def _():
        dk_ref[...] += dk
        dv_ref[...] += dv


def attend_backward(kpos, cosine, sine, qkv, pairs, grad):
    rows = qkv.shape[0]
    keys = pairs.shape[0]
    group = HEADS // KV_HEADS
    width = KV_HEADS * HEAD_DIM
    return pl.pallas_call(
        bwd_kernel,
        grid=(HEADS,),
        in_specs=[
            pl.BlockSpec((1, keys), lambda h: (0, 0)),
            pl.BlockSpec((rows, HEAD_DIM), lambda h: (0, 0)),
            pl.BlockSpec((rows, HEAD_DIM), lambda h: (0, 0)),
            pl.BlockSpec((rows, HEAD_DIM), lambda h: (0, h)),
            pl.BlockSpec((keys, HEAD_DIM), lambda h: (0, h // group)),
            pl.BlockSpec((keys, HEAD_DIM), lambda h: (0, KV_HEADS + h // group)),
            pl.BlockSpec((rows, HEAD_DIM), lambda h: (0, h)),
        ],
        out_specs=[
            pl.BlockSpec((rows, HEAD_DIM), lambda h: (0, h)),
            pl.BlockSpec((keys, HEAD_DIM), lambda h: (0, h // group)),
            pl.BlockSpec((keys, HEAD_DIM), lambda h: (0, h // group)),
        ],
        out_shape=[
            jax.ShapeDtypeStruct((rows, HEADS * HEAD_DIM), low),
            jax.ShapeDtypeStruct((keys, width), full),
            jax.ShapeDtypeStruct((keys, width), full),
        ],
        cost_estimate=pl.CostEstimate(
            flops=10 * rows * keys * HEADS * HEAD_DIM * 3,
            bytes_accessed=8 * rows * HEADS * HEAD_DIM + 12 * keys * width,
            transcendentals=rows * keys * HEADS,
        ),
        name="attend_backward",
    )(kpos, cosine, sine, qkv, pairs, pairs, grad)


def body(
    tokens, lengths, attn_gain, w_query, b_query, w_key, b_key, w_value, b_value, w_out,
    ffn_gain, w_gate, w_up, w_down, cotangent,
):
    slot_count, rows, width = tokens.shape
    seq_count = lax.axis_size("seq")
    wt_count = lax.axis_size("wt")
    outer = wt_count // INNER
    seq_here = lax.axis_index("seq")
    inner_here = lax.axis_index("wt") % INNER
    line = [[o * INNER + i for o in range(outer)] for i in range(INNER)]
    hops_a, hops_b = plane_hops(seq_count)
    plane = INNER * seq_count
    share = w_query.shape[0]
    bias_q, bias_k = b_query.shape[0], b_key.shape[0]
    query_width = HEADS * HEAD_DIM
    pair_width = KV_HEADS * HEAD_DIM
    head_width = query_width + 2 * pair_width
    ff_own = w_down.shape[0] // seq_count
    ff_here = outer * ff_own
    ff_pad = -(-ff_here // 128) * 128

    flat = tokens.astype(full).reshape(rows, width)
    places = seq_here * rows + jnp.arange(rows, dtype=jnp.int32)
    keep = (places < lengths[0])[:, None]
    upstream_low = jnp.where(keep, cotangent.reshape(rows, width), jnp.zeros((), low))

    def line_gather(value):
        return lax.all_gather(value, "wt", axis=0, axis_index_groups=line, tiled=False)

    def line_reduce(value):
        return lax.psum_scatter(
            value, "wt", scatter_dimension=0, axis_index_groups=line, tiled=False
        )

    def seq_gather(value):
        stacked = gather_hops(value, bits_of("seq", seq_count))
        return jnp.stack([to_place(stacked, seq_here ^ p) for p in range(seq_count)])

    info = jnp.stack([seq_here, inner_here]).astype(jnp.int32)
    down_own = lax.dynamic_slice_in_dim(w_down, seq_here * ff_own, ff_own, axis=0).astype(low)

    def inner_swap(value, distance):
        count = lax.axis_size("wt")
        return lax.ppermute(value, "wt", [(i, i ^ distance) for i in range(count)])

    def inner_exchange(value):
        got = [value[0]] + [inner_swap(value[d], d) for d in range(1, INNER)]
        return jnp.stack(got)

    stacked = inner_exchange(split_units(info, w_gate, w_up, outer, seq_count, ff_own, ff_pad))
    block = jnp.stack([to_place(stacked, inner_here ^ p) for p in range(INNER)])
    block = block.reshape(INNER * share, 2 * ff_pad)
    half = HEAD_DIM // 2
    inverse = 10000.0 ** (-jnp.arange(half, dtype=full) / half)
    angle = places.astype(full)[:, None] * inverse[None, :]
    cosine = jnp.cos(angle)
    sine = jnp.sin(angle)
    cosine = jnp.concatenate([cosine, cosine], axis=1)
    sine = jnp.concatenate([-sine, sine], axis=1)

    def line_of(vector):
        return jnp.pad(vector, (0, HEAD_DIM - vector.shape[0]))

    small = jnp.stack([line_of(v) for v in (attn_gain, b_query, b_key, b_value, ffn_gain)])
    small = jnp.pad(small.astype(low), ((0, 11), (0, 0)))
    packed = jnp.concatenate([w_query, w_key, w_value], axis=1).astype(low)
    normed_low, qkv, vectors, head_all, out_all = gather_project(
        tokens.reshape(rows, width),
        *gather_line(packed, w_out.astype(low), small), cosine, sine,
    )
    head_w = head_all.reshape(width, head_width)
    out_w = out_all.reshape(query_width, width)
    gain_one = vectors[0, :width]
    gain_two = vectors[2, :width]
    units_w = line_gather(block).reshape(width, 2 * ff_pad)
    down_w = line_gather(down_own).reshape(ff_here, width)
    down_w = jnp.pad(down_w, ((0, ff_pad - ff_here), (0, 0)))

    seq_hops = bits_of("seq", seq_count)
    pairs = gather_hops(qkv[:, query_width:], seq_hops).reshape(SLOT, 2 * pair_width)
    distance = jnp.arange(SLOT, dtype=jnp.int32)
    key_place = (seq_here ^ (distance // rows)) * rows + distance % rows
    kpos = jnp.where(key_place < lengths[0], key_place - seq_here * rows, far_place)[None, :]
    mixed = attend_forward(kpos, qkv, pairs)
    resid = flat + product(mixed, out_w)
    normed_two, factor_two = norm_rows(resid, gain_two)
    normed_two_low = normed_two.astype(low)

    core = hops_a[-1]
    slow_a, slow_b = hops_a[:-1], hops_b[:-1]
    near_rows = plane * rows // 2

    def spread(block):
        part_a = gather_hops(block[: rows // 2], slow_a)
        part_b = gather_hops(block[rows // 2 :], slow_b)
        near = jnp.stack([part_a, part_b]).reshape(near_rows, width)
        return jnp.concatenate([near, swap(near, core)], axis=0)

    def hop_core(partial):
        other = swap(partial[near_rows:], core)
        near = (partial[:near_rows].astype(full) + other.astype(full)).astype(low)
        near = near.reshape(2, plane // 2, rows // 2, width)
        return (near[0], near[1])

    def hop_slow(parts, stage):
        return tuple(reduce_hop(part, hops[stage]) for part, hops in zip(parts, (slow_a, slow_b)))

    def hop_last(parts):
        got = [reduce_hops(part, hops[:1]) for part, hops in zip(parts, (slow_a, slow_b))]
        return jnp.concatenate(got, axis=0)

    stages = list(range(1, len(slow_a)))[::-1]
    grad_all = spread(upstream_low)
    rows_all = spread(normed_two_low)
    both = product(rows_all, units_w)
    hidden, units_grad = hidden_units(both, grad_all, down_w)
    down_grad = product_left(hidden, grad_all).astype(low)
    units_grad, down_grad = lax.optimization_barrier((units_grad, down_grad))
    down_grad = down_grad[:ff_here]
    partial = product_right(units_grad, units_w).astype(low)
    down_line = line_reduce(down_grad.reshape(outer, ff_own, width))
    back = hop_core(partial)
    rows_late, grad_late = lax.optimization_barrier((rows_all, units_grad, back, down_grad))[:2]
    units_w_grad = product_left(rows_late, grad_late).astype(low)
    units_line = line_reduce(units_w_grad.reshape(outer, INNER * share, 2 * ff_pad))
    for stage in stages:
        back = hop_slow(back, stage)
    hidden_late = after(hidden, back, units_w_grad)
    partial = product(hidden_late, down_w).astype(low)
    normed_two_grad = hop_last(back)

    upstream = upstream_low.astype(full)
    resid_norm_grad, gain_two_grad = norm_back(resid, factor_two, gain_two, normed_two_grad)
    resid_grad = upstream + resid_norm_grad
    attn_grad = resid_grad.astype(low)
    mixed_grad = product_right(attn_grad, out_w).astype(low)
    out_w_grad = product_left(mixed, attn_grad).astype(low)
    query_grad, key_part, value_part = attend_backward(
        kpos, cosine, sine, qkv, pairs, mixed_grad
    )
    forth = hop_core(after(partial, normed_two_grad))
    for stage in stages:
        forth = hop_slow(forth, stage)
    forth = hop_last(lax.optimization_barrier((*forth, query_grad))[:2])
    layer_out = jnp.where(keep, resid + forth, 0.0).astype(low)
    layer_out = layer_out.reshape(slot_count, rows, width)

    down_out = seq_gather(down_line)
    down_out = down_out.reshape(seq_count * ff_own, width).astype(full)
    pair_part = jnp.concatenate([key_part, value_part], axis=1)
    pair_sum = reduce_hops(
        pair_part.reshape(seq_count, rows, 2 * pair_width).astype(low), seq_hops
    )
    key_rot_grad = pair_sum[:, :pair_width].reshape(rows, KV_HEADS, HEAD_DIM)
    turned = jnp.concatenate([key_rot_grad[..., half:], key_rot_grad[..., :half]], axis=-1)
    key_grad = key_rot_grad * cosine[:, None, :] - turned * sine[:, None, :]
    head_grad = jnp.concatenate(
        [query_grad, key_grad.reshape(rows, pair_width).astype(low),
         pair_sum[:, pair_width:].astype(low)],
        axis=1,
    )
    head_w_grad = product_left(normed_low, head_grad).astype(low)
    head_b_grad = jnp.sum(head_grad.astype(full), axis=0)
    normed_grad = product_right(head_grad, head_w)
    factor_one = lax.rsqrt(jnp.mean(flat * flat, axis=-1, keepdims=True) + epsilon)
    input_norm_grad, gain_one_grad = norm_back(flat, factor_one, gain_one, normed_grad)
    input_grad = (resid_grad + input_norm_grad).astype(low).reshape(slot_count, rows, width)

    edges = [0, share, share + bias_q]
    edges += [edges[-1] + bias_k, edges[-1] + 2 * bias_k]

    def parts(vector):
        return vector.reshape(wt_count, -1)

    small_grad = jnp.concatenate(
        [
            parts(gain_one_grad),
            parts(head_b_grad[:query_width]),
            parts(head_b_grad[query_width : query_width + pair_width]),
            parts(head_b_grad[query_width + pair_width :]),
            parts(gain_two_grad),
        ],
        axis=1,
    ).astype(low)
    small_grad = jnp.pad(small_grad, ((0, 0), (0, 256 * seq_count - small_grad.shape[1])))
    small_grad = jnp.pad(small_grad[:, None, :], ((0, 0), (0, 15), (0, 0)))

    def by_owner(partial):
        return partial.reshape(outer, INNER, -1, partial.shape[-1])

    out_w_out, heads_out, small_out, units_got = reduce_shares(
        units_line.reshape(INNER, share, 2 * ff_pad),
        by_owner(out_w_grad),
        by_owner(head_w_grad),
        by_owner(small_grad),
    )
    small_out = small_out[0]
    gate_out, up_out = join_units(info, units_got, outer, ff_own)
    return (
        layer_out,
        input_grad,
        small_out[: edges[1]],
        heads_out[:, :query_width],
        small_out[edges[1] : edges[2]],
        heads_out[:, query_width : query_width + pair_width],
        small_out[edges[2] : edges[3]],
        heads_out[:, query_width + pair_width :],
        small_out[edges[3] : edges[4]],
        out_w_out,
        small_out[edges[4] : edges[4] + ffn_gain.shape[0]],
        gate_out,
        up_out,
        down_out,
    )


def solution(mesh):
    by_wt = P("wt")
    by_row = P("wt", None)
    by_token = P("wt", "seq", None)
    return jax.shard_map(
        body,
        mesh=mesh,
        in_specs=(
            by_token, by_wt, by_wt, by_row, by_wt, by_row, by_wt, by_row, by_wt, by_row,
            by_wt, by_row, by_row, by_row, by_token,
        ),
        out_specs=(
            by_token, by_token, by_wt, by_row, by_wt, by_row, by_wt, by_row, by_wt, by_row,
            by_wt, by_row, by_row, by_row,
        ),
        check_vma=False,
    )
```

```python
import functools
import math

import jax
import jax.numpy as jnp
from jax import lax
from jax.experimental import pallas as pl
from jax.experimental.pallas import tpu as pltpu
from jax.sharding import PartitionSpec as P


HEADS = 12
KV_HEADS = 2
HEAD_DIM = 128
SLOT = 1024
INNER = 4

epsilon = 1e-06
masked_score = -1e30
far_place = 1 << 30
scale = 1.0 / math.sqrt(HEAD_DIM)
low = jnp.bfloat16
full = jnp.float32


def product(left, right):
    return jnp.dot(left, right, preferred_element_type=full)


def product_left(left, right):
    return lax.dot_general(left, right, (((0,), (0,)), ((), ())), preferred_element_type=full)


def product_right(left, right):
    return lax.dot_general(left, right, (((1,), (1,)), ((), ())), preferred_element_type=full)


def norm_rows(values, gain):
    factor = lax.rsqrt(jnp.mean(values * values, axis=-1, keepdims=True) + epsilon)
    return (values * factor * gain, factor)


def norm_back(values, factor, gain, upstream):
    weighted = upstream * gain
    inner = jnp.mean(weighted * values, axis=-1, keepdims=True)
    grad_in = factor * weighted - values * (factor * factor * factor) * inner
    grad_gain = jnp.sum(upstream * values * factor, axis=0)
    return (grad_in, grad_gain)


def swap(value, hop):
    axis, bit = hop
    count = lax.axis_size(axis)
    return lax.ppermute(value, axis, [(i, i ^ bit) for i in range(count)])


def gather_hops(block, hops):
    held = block[None]
    for hop in hops:
        held = jnp.concatenate([held, swap(held, hop)], axis=0)
    return held


def reduce_hop(held, hop):
    half = held.shape[0] // 2
    other = swap(held[half:], hop)
    return (held[:half].astype(full) + other.astype(full)).astype(low)


def reduce_hops(held, hops):
    for k in range(len(hops) - 1, 0, -1):
        held = reduce_hop(held, hops[k])
    return held[0].astype(full) + swap(held[1], hops[0]).astype(full)


def bits_of(axis, count):
    found, bit = [], 1
    while bit < count:
        found.append((axis, bit))
        bit *= 2
    return found


def plane_hops(seq_count):
    inner = bits_of("wt", INNER)
    seq = bits_of("seq", seq_count)
    slow = inner[1:] + seq
    return (slow + inner[:1], slow[::-1] + inner[:1])


def to_place(stacked, place):
    return lax.dynamic_index_in_dim(stacked, place, 0, keepdims=False)


def flip(index, bit):
    return index + bit - 2 * bit * ((index // bit) % 2)


def flip_all(index, distance):
    bit = 1
    while bit <= distance:
        if distance & bit:
            index = flip(index, bit)
        bit *= 2
    return index


def inner_bits():
    return [bit for _, bit in bits_of("wt", INNER)]


def meet(peers):
    barrier = pltpu.get_barrier_semaphore()
    for peer in peers:
        pl.semaphore_signal(
            barrier, inc=1, device_id=peer, device_id_type=pl.DeviceIdType.MESH
        )
    pl.semaphore_wait(barrier, len(peers))


class Sender:
    def __init__(self, send_sems, recv_sems):
        self.sems = (send_sems, recv_sems)
        self.copies = []

    def start(self, source, target, peer):
        at = len(self.copies)
        copy = pltpu.make_async_remote_copy(
            src_ref=source,
            dst_ref=target,
            send_sem=self.sems[0].at[at],
            recv_sem=self.sems[1].at[at],
            device_id=peer,
            device_id_type=pl.DeviceIdType.MESH,
        )
        copy.start()
        self.copies.append(copy)
        return copy


def subsets(hops):
    found = [(0, 0)]
    for axis, bit in hops:
        more = [(a ^ bit, b) if axis == "wt" else (a, b ^ bit) for a, b in found]
        found = found + more
    return found


def plane_copies(seq_count):
    hops_a, _ = plane_hops(seq_count)
    slow = len(hops_a) - 1
    return (2 * (2**slow - 1), len(set(a for a, _ in subsets(hops_a[:-1]))))


def line_kernel(outer, seq_count, p_ref, wo_ref, s_ref, head_ref, out_ref, small_ref, *sems):
    send_sems, recv_sems, local_sems = sems
    wt, seq = lax.axis_index("wt"), lax.axis_index("seq")
    line, inner = wt // INNER, wt % INNER

    def own_columns(total):
        wide = total // seq_count
        return pl.ds(pl.multiple_of(seq * wide, 128), wide)

    pairs = [
        (s_ref, small_ref),
        (p_ref.at[:, own_columns(p_ref.shape[1])], head_ref),
        (wo_ref.at[:, own_columns(wo_ref.shape[1])], out_ref),
    ]
    own = [
        pltpu.make_async_copy(source, target.at[0], local_sems.at[k])
        for k, (source, target) in enumerate(pairs)
    ]
    for copy in own:
        copy.start()
    peers = [(flip_all(line, d) * INNER + inner, seq) for d in range(1, outer)]
    meet(peers)
    out = Sender(send_sems, recv_sems)
    for source, target in pairs:
        for d in range(1, outer):
            out.start(source, target.at[d], peers[d - 1])
    for copy in own:
        copy.wait()
    for copy in out.copies:
        copy.wait()


def gather_line(packed, w_out, small):
    outer = lax.axis_size("wt") // INNER
    seq_count = lax.axis_size("seq")
    share, head_width = packed.shape
    vmem = pl.BlockSpec(memory_space=pltpu.VMEM)
    copies = 3 * (outer - 1)
    sent = 2 * outer * share * (head_width + w_out.shape[1])
    return pl.pallas_call(
        functools.partial(line_kernel, outer, seq_count),
        in_specs=[vmem] * 3,
        out_specs=[vmem] * 3,
        out_shape=[
            jax.ShapeDtypeStruct((outer, share, head_width // seq_count), low),
            jax.ShapeDtypeStruct((outer, share, w_out.shape[1] // seq_count), low),
            jax.ShapeDtypeStruct((outer,) + small.shape, low),
        ],
        scratch_shapes=[
            pltpu.SemaphoreType.DMA((copies,)),
            pltpu.SemaphoreType.DMA((copies,)),
            pltpu.SemaphoreType.DMA((3,)),
        ],
        compiler_params=pltpu.CompilerParams(collective_id=3, has_side_effects=True),
        cost_estimate=pl.CostEstimate(flops=0, bytes_accessed=8 * sent, transcendentals=0),
        name="gather_line",
    )(packed, w_out, small)


def gather_kernel(
    outer, seq_count, x_ref, p_ref, wo_ref, s_ref, cos_ref, sin_ref,
    normed_ref, qkv_ref, vec_ref, head_ref, out_ref,
    w_scr, o_scr, s_scr, send_sems, recv_sems, local_sems,
):
    share, head_width = p_ref.shape[1], w_scr.shape[3]
    width = x_ref.shape[1]
    wt, seq = lax.axis_index("wt"), lax.axis_index("seq")
    line, inner = wt // INNER, wt % INNER
    hops = plane_hops(seq_count)
    slow = len(hops[0]) - 1
    peers = [(wt - inner + flip(inner, bit), seq) for bit in inner_bits()]
    peers += [(wt, flip(seq, bit)) for _, bit in bits_of("seq", seq_count)]

    def own_columns(total):
        wide = total // seq_count
        return pl.ds(pl.multiple_of(seq * wide, 128), wide)

    fill = []
    for d in range(outer):
        at = flip_all(line, d)
        pairs = [
            (s_ref.at[d], s_scr.at[at, inner]),
            (p_ref.at[d], w_scr.at[at, inner, :, own_columns(head_width)]),
            (wo_ref.at[d], o_scr.at[at, inner, :, own_columns(o_scr.shape[3])]),
        ]
        fill += [
            pltpu.make_async_copy(source, target, local_sems.at[3 * d + k])
            for k, (source, target) in enumerate(pairs)
        ]
    for copy in fill:
        copy.start()
    meet(peers)
    out = Sender(send_sems, recv_sems)

    def hop_peer(hop):
        axis, bit = hop
        if axis == "wt":
            return (wt - inner + flip(inner, bit), seq)
        return (wt, flip(seq, bit))

    def columns(total, part, half):
        wide = total // seq_count
        first = -(-wide // 256) * 128
        start = part * wide + half * first
        return pl.ds(pl.multiple_of(start, 128), wide - first if half else first)

    def start_stage(scratch, at, stage):
        total = scratch.shape[-1]
        copies = []
        if stage < slow:
            for half in range(2):
                hop = hops[half][stage]
                for a, b in subsets(hops[half][:stage]):
                    place = scratch.at[
                        at, flip_all(inner, a), :, columns(total, flip_all(seq, b), half)
                    ]
                    copies.append(out.start(place, place, hop_peer(hop)))
            return copies
        for a in sorted(set(a for a, _ in subsets(hops[0][:slow]))):
            place = scratch.at[at, flip_all(inner, a)]
            copies.append(out.start(place, place, hop_peer(hops[0][slow])))
        return copies

    def arrive(copies):
        for copy in copies:
            if copy is not None:
                copy.wait_recv()

    for copy in fill:
        copy.wait()
    waiting = [[] for _ in range(outer)]
    small_wait = []
    for step in range(outer + slow + 1):
        for stage in range(slow + 1):
            d = step - stage
            if 0 <= d < outer:
                arrive(waiting[d])
                waiting[d] = start_stage(w_scr, flip_all(line, d), stage)
        if step < len(inner_bits()):
            arrive(small_wait)
            bit = inner_bits()[::-1][step]
            small_wait = []
            for a, _ in subsets([("wt", b) for b in inner_bits()[::-1][:step]]):
                place = s_scr.at[:, flip_all(inner, a)]
                small_wait.append(out.start(place, place, hop_peer(("wt", bit))))
    arrive(small_wait)
    out_wait = start_stage(o_scr, slice(None), 0)

    count = outer * INNER
    bias_k = share * KV_HEADS * HEAD_DIM // (HEADS * HEAD_DIM)
    query_width = HEADS * HEAD_DIM
    pair_width = KV_HEADS * HEAD_DIM
    vec_ref[...] = jnp.zeros_like(vec_ref)
    for k in range(count):
        small = s_scr[k // INNER, k % INNER].astype(full)
        at = k * share
        vec_ref[0:1, at : at + share] = small[0:1, :share]
        vec_ref[1:2, at : at + share] = small[1:2, :share]
        at = query_width + k * bias_k
        vec_ref[1:2, at : at + bias_k] = small[2:3, :bias_k]
        at = query_width + pair_width + k * bias_k
        vec_ref[1:2, at : at + bias_k] = small[3:4, :bias_k]
        at = k * share
        vec_ref[2:3, at : at + share] = small[4:5, :share]

    values = x_ref[...].astype(full)
    factor = lax.rsqrt(jnp.mean(values * values, axis=-1, keepdims=True) + epsilon)
    normed_ref[...] = (values * factor * vec_ref[0:1, :width]).astype(low)
    for d in range(outer):
        arrive(waiting[d])
    keep_head = pltpu.make_async_copy(w_scr, head_ref, local_sems.at[0])
    keep_head.start()
    wide = 2 * HEAD_DIM
    blocks = head_width // wide

    def project(at):
        weights = w_scr[:, :, :, pl.ds(at, wide)].reshape(width, wide)
        return (
            jnp.dot(normed_ref[...], weights, preferred_element_type=full)
            + vec_ref[1:2, pl.ds(at, wide)]
        )

    def turn_block(k):
        at = pl.multiple_of(k * wide, wide)
        got = project(at)
        for j in range(2):
            part = got[:, j * HEAD_DIM : (j + 1) * HEAD_DIM]
            turned = part * cos_ref[...] + pltpu.roll(part, HEAD_DIM // 2, 1) * sin_ref[...]
            where = pl.multiple_of(at + j * HEAD_DIM, HEAD_DIM)
            qkv_ref[:, pl.ds(where, HEAD_DIM)] = turned.astype(low)

    turned_blocks = blocks - pair_width // wide
    marks = [turned_blocks * (k + 1) // (slow + 1) for k in range(slow + 1)]
    begin = 0
    for stage in range(slow + 1):
        @pl.loop(begin, marks[stage])
        def _(k):
            turn_block(k)

        begin = marks[stage]
        arrive(out_wait)
        out_wait = start_stage(o_scr, slice(None), stage + 1) if stage < slow else []
    for k in range(turned_blocks, blocks):
        qkv_ref[:, k * wide : (k + 1) * wide] = project(k * wide).astype(low)
    keep_out = pltpu.make_async_copy(o_scr, out_ref, local_sems.at[1])
    keep_out.start()
    for copy in out.copies:
        copy.wait_send()
    keep_head.wait()
    keep_out.wait()


def gather_project(tokens, packed, w_out, small, cosine, sine):
    outer = lax.axis_size("wt") // INNER
    seq_count = lax.axis_size("seq")
    rows, width = tokens.shape
    share, head_width = packed.shape[1], packed.shape[2] * seq_count
    out_width = w_out.shape[2] * seq_count
    slow_copies, last_copies = plane_copies(seq_count)
    each = slow_copies + last_copies
    small_copies = 2 ** len(inner_bits()) - 1
    copies = (outer + 1) * each + small_copies
    vmem = pl.BlockSpec(memory_space=pltpu.VMEM)
    anywhere = pl.BlockSpec(memory_space=pl.ANY)
    sent = 2 * outer * INNER * share * (head_width + out_width)
    return pl.pallas_call(
        functools.partial(gather_kernel, outer, seq_count),
        in_specs=[vmem] * 6,
        out_specs=[vmem, vmem, vmem, anywhere, anywhere],
        out_shape=[
            jax.ShapeDtypeStruct((rows, width), low),
            jax.ShapeDtypeStruct((rows, head_width), low),
            jax.ShapeDtypeStruct((8, head_width), full),
            jax.ShapeDtypeStruct((outer, INNER, share, head_width), low),
            jax.ShapeDtypeStruct((outer, INNER, share, out_width), low),
        ],
        scratch_shapes=[
            pltpu.VMEM((outer, INNER, share, head_width), low),
            pltpu.VMEM((outer, INNER, share, out_width), low),
            pltpu.VMEM((outer, INNER) + small.shape[1:], low),
            pltpu.SemaphoreType.DMA((copies,)),
            pltpu.SemaphoreType.DMA((copies,)),
            pltpu.SemaphoreType.DMA((3 * outer,)),
        ],
        compiler_params=pltpu.CompilerParams(
            collective_id=1, has_side_effects=True, vmem_limit_bytes=48 << 20
        ),
        cost_estimate=pl.CostEstimate(
            flops=2 * rows * width * head_width * 8, bytes_accessed=2 * sent, transcendentals=0
        ),
        name="gather_project",
    )(tokens, packed, w_out, small, cosine, sine)


def near_inner(seq_count):
    hops = plane_hops(seq_count)[0]
    return sorted(set(a for a, _ in subsets(hops[:-1])))


def reduce_kernel(outer, seq_count, count, *refs):
    given, results = refs[:count], refs[count : 2 * count]
    slow = len(plane_hops(seq_count)[0]) - 1
    held = refs[2 * count : 3 * count]
    lines = refs[3 * count : 4 * count]
    joined = refs[4 * count : 5 * count]
    landed = refs[5 * count : (6 + slow) * count]
    send_sems, recv_sems = refs[(6 + slow) * count :]
    wt, seq = lax.axis_index("wt"), lax.axis_index("seq")
    line, inner = wt // INNER, wt % INNER
    hops = plane_hops(seq_count)
    nears = near_inner(seq_count)
    peers = [(flip_all(line, d) * INNER + inner, seq) for d in range(1, outer)]
    peers += [(wt - inner + flip(inner, bit), seq) for bit in inner_bits()]
    peers += [(wt, flip_all(seq, d)) for d in range(1, seq_count)]
    meet(peers)
    out = Sender(send_sems, recv_sems)

    def hop_peer(hop):
        axis, bit = hop
        if axis == "wt":
            return (wt - inner + flip(inner, bit), seq)
        return (wt, flip(seq, bit))

    def columns(total, part, half):
        wide = total // seq_count
        first = -(-wide // 256) * 128
        start = part * wide + half * first
        return pl.ds(pl.multiple_of(start, 128), wide - first if half else first)

    def arrive(copies):
        for copy in copies:
            copy.wait_recv()

    def steps(k):
        source, total = given[k], given[k].shape[3]
        sums, wide = held[k], given[k].shape[3] // seq_count
        own = pl.ds(pl.multiple_of(seq * wide, 128), wide)
        core = hops[0][slow]
        copies = [
            out.start(
                source.at[:, flip_all(inner, a ^ core[1])],
                landed[k].at[:, at],
                hop_peer(core),
            )
            for at, a in enumerate(nears)
        ]
        yield
        arrive(copies)
        for at, a in enumerate(nears):
            place = flip_all(inner, a)

            @pl.loop(0, outer)
            def _(o):
                both = source[o, place].astype(full) + landed[k][o, at].astype(full)
                sums[o, at] = both.astype(low)

        for stage in range(slow - 1, -1, -1):
            target = landed[(1 + stage) * count + k]
            copies, blocks = [], []
            for half in range(2):
                axis, bit = hops[half][stage]
                for a, b in subsets(hops[half][:stage]):
                    from_a = a ^ bit if axis == "wt" else a
                    from_b = b ^ bit if axis == "seq" else b
                    sent = columns(total, flip_all(seq, from_b), half)
                    copies.append(
                        out.start(
                            sums.at[:, nears.index(from_a), :, sent],
                            target.at[:, nears.index(a), :, sent],
                            hop_peer((axis, bit)),
                        )
                    )
                    blocks.append((nears.index(a), columns(total, flip_all(seq, b), half)))
            yield
            arrive(copies)
            for at, part in blocks:

                @pl.loop(0, outer)
                def _(o):
                    both = sums[o, at, :, part].astype(full) + target[o, at, :, part].astype(full)
                    sums[o, at, :, part] = both.astype(low)

        copies = [
            out.start(
                sums.at[flip_all(line, d), 0, :, own],
                lines[k].at[d],
                (flip_all(line, d) * INNER + inner, seq),
            )
            for d in range(1, outer)
        ]
        yield
        arrive(copies)
        both = sums[line, 0, :, own].astype(full)
        for d in range(1, outer):
            both = both + lines[k][d].astype(full)
        joined[k][:, own] = both.astype(low)
        copies = [
            out.start(joined[k].at[:, own], joined[k].at[:, own], (wt, flip_all(seq, d)))
            for d in range(1, seq_count)
        ]
        yield
        arrive(copies)
        results[k][...] = joined[k][...].astype(full)

    running = [steps(k) for k in range(count)]
    for _ in range(2):
        next(running[0])
    while running:
        for one in list(running):
            if next(one, "done") == "done":
                running.remove(one)
    for copy in out.copies:
        copy.wait_send()


def reduce_shares(*partials):
    outer = lax.axis_size("wt") // INNER
    seq_count = lax.axis_size("seq")
    count = len(partials)
    slow = len(plane_hops(seq_count)[0]) - 1
    nears = len(near_inner(seq_count))
    vmem = pl.BlockSpec(memory_space=pltpu.VMEM)
    near = [
        pltpu.VMEM((outer, nears) + p.shape[2:], low) for p in partials
    ]
    shapes = [p.shape[2:] for p in partials]
    copies = count * (nears + 2 * (2**slow - 1) + outer - 1 + seq_count - 1)
    sent = sum(2 * p.size for p in partials)
    return pl.pallas_call(
        functools.partial(reduce_kernel, outer, seq_count, count),
        in_specs=[vmem] * count,
        out_specs=[vmem] * count,
        out_shape=[jax.ShapeDtypeStruct(shape, full) for shape in shapes],
        scratch_shapes=near
        + [pltpu.VMEM((outer, r, c // seq_count), low) for r, c in shapes]
        + [pltpu.VMEM(shape, low) for shape in shapes]
        + near * (1 + slow)
        + [pltpu.SemaphoreType.DMA((n,)) for n in (copies, copies)],
        compiler_params=pltpu.CompilerParams(
            collective_id=2, has_side_effects=True, vmem_limit_bytes=60 << 20
        ),
        cost_estimate=pl.CostEstimate(flops=0, bytes_accessed=8 * sent, transcendentals=0),
        name="reduce_shares",
    )(*partials)


def split_kernel(outer, seq_count, own, info_ref, gate_ref, up_ref, o_ref):
    inner = info_ref[1]
    width = outer * own
    padded = o_ref.shape[2] // 2
    for s in range(seq_count):
        @pl.when(info_ref[0] == s)
        def _():
            for q in range(INNER):
                place = jnp.bitwise_xor(inner, q)
                for k, ref in enumerate((gate_ref, up_ref)):
                    for o in range(outer):
                        at = ((o * INNER + q) * seq_count + s) * own
                        to = k * padded + o * own
                        o_ref[place, :, to : to + own] = ref[:, at : at + own].astype(low)
                    if padded > width:
                        blank = jnp.zeros((o_ref.shape[1], padded - width), low)
                        o_ref[place, :, k * padded + width : (k + 1) * padded] = blank


def split_units(info, gate, up, outer, seq_count, own, padded):
    vmem = pl.BlockSpec(memory_space=pltpu.VMEM)
    return pl.pallas_call(
        functools.partial(split_kernel, outer, seq_count, own),
        in_specs=[pl.BlockSpec(memory_space=pltpu.SMEM), vmem, vmem],
        out_specs=vmem,
        out_shape=jax.ShapeDtypeStruct((INNER, gate.shape[0], 2 * padded), low),
        name="split_units",
    )(info, gate, up)


def join_kernel(outer, seq_count, own, info_ref, u_ref, gate_ref, up_ref):
    seq, inner = info_ref[0], info_ref[1]
    padded = u_ref.shape[3] // 2
    for s in range(seq_count):
        for q in range(INNER):
            block = u_ref[jnp.bitwise_xor(seq, s), jnp.bitwise_xor(inner, q)].astype(full)
            for k, ref in enumerate((gate_ref, up_ref)):
                for o in range(outer):
                    at = ((o * INNER + q) * seq_count + s) * own
                    source = k * padded + o * own
                    ref[:, at : at + own] = block[:, source : source + own]


def join_units(info, units, outer, own):
    seq_count, _, rows, _ = units.shape
    vmem = pl.BlockSpec(memory_space=pltpu.VMEM)
    shape = jax.ShapeDtypeStruct((rows, outer * INNER * seq_count * own), full)
    return pl.pallas_call(
        functools.partial(join_kernel, outer, seq_count, own),
        in_specs=[pl.BlockSpec(memory_space=pltpu.SMEM), vmem],
        out_specs=[vmem, vmem],
        out_shape=[shape, shape],
        name="join_units",
    )(info, units)


def hidden_kernel(both_ref, grad_ref, down_ref, hidden_ref, units_ref):
    wide = hidden_ref.shape[1]
    hidden_grad = lax.dot_general(
        grad_ref[...], down_ref[...], (((1,), (1,)), ((), ())), preferred_element_type=full
    )
    gate, upper = both_ref[:, :wide], both_ref[:, wide:]
    sigma = 1.0 / (1.0 + jnp.exp(-gate))
    taken = gate * sigma
    hidden_ref[...] = (taken * upper).astype(low)
    slope = sigma * (1.0 + gate * (1.0 - sigma))
    units_ref[:, :wide] = (hidden_grad * upper * slope).astype(low)
    units_ref[:, wide:] = (hidden_grad * taken).astype(low)


def hidden_units(both, grad, down_w):
    total, width = grad.shape
    wide = down_w.shape[0]
    block = min(512, total)
    return pl.pallas_call(
        hidden_kernel,
        grid=(total // block,),
        in_specs=[
            pl.BlockSpec((block, 2 * wide), lambda i: (i, 0)),
            pl.BlockSpec((block, width), lambda i: (i, 0)),
            pl.BlockSpec((wide, width), lambda i: (0, 0)),
        ],
        out_specs=[
            pl.BlockSpec((block, wide), lambda i: (i, 0)),
            pl.BlockSpec((block, 2 * wide), lambda i: (i, 0)),
        ],
        out_shape=[
            jax.ShapeDtypeStruct((total, wide), low),
            jax.ShapeDtypeStruct((total, 2 * wide), low),
        ],
        compiler_params=pltpu.CompilerParams(vmem_limit_bytes=56 << 20),
        cost_estimate=pl.CostEstimate(
            flops=2 * total * width * wide,
            bytes_accessed=2 * total * (width + 7 * wide) + 2 * wide * width,
            transcendentals=total * wide,
        ),
        name="hidden_units",
    )(both, grad, down_w)


def after(value, *others):
    return lax.optimization_barrier((value, *others))[0]


def shown(kpos_ref, rows, keys):
    places = lax.broadcasted_iota(jnp.int32, (rows, keys), 0)
    return kpos_ref[...] <= places


def fwd_kernel(kpos_ref, q_ref, k_ref, v_ref, o_ref):
    rows, keys = q_ref.shape[0], k_ref.shape[0]
    scores = (
        lax.dot_general(
            q_ref[...], k_ref[...], (((1,), (1,)), ((), ())), preferred_element_type=full
        )
        * scale
    )
    scores = jnp.where(shown(kpos_ref, rows, keys), scores, masked_score)
    top = jnp.max(scores, axis=-1, keepdims=True)
    weights = jnp.exp(scores - top)
    total = jnp.sum(weights, axis=-1, keepdims=True)
    probs = (weights * (1.0 / total)).astype(low)
    o_ref[...] = jnp.dot(probs, v_ref[...], preferred_element_type=full).astype(low)


def attend_forward(kpos, qkv, pairs):
    rows = qkv.shape[0]
    keys = pairs.shape[0]
    group = HEADS // KV_HEADS
    return pl.pallas_call(
        fwd_kernel,
        grid=(HEADS,),
        in_specs=[
            pl.BlockSpec((1, keys), lambda h: (0, 0)),
            pl.BlockSpec((rows, HEAD_DIM), lambda h: (0, h)),
            pl.BlockSpec((keys, HEAD_DIM), lambda h: (0, h // group)),
            pl.BlockSpec((keys, HEAD_DIM), lambda h: (0, KV_HEADS + h // group)),
        ],
        out_specs=pl.BlockSpec((rows, HEAD_DIM), lambda h: (0, h)),
        out_shape=jax.ShapeDtypeStruct((rows, HEADS * HEAD_DIM), low),
        cost_estimate=pl.CostEstimate(
            flops=4 * rows * keys * HEADS * HEAD_DIM * 3,
            bytes_accessed=4 * rows * HEADS * HEAD_DIM + 4 * keys * KV_HEADS * HEAD_DIM,
            transcendentals=rows * keys * HEADS,
        ),
        name="attend_forward",
    )(kpos, qkv, pairs, pairs)


def bwd_kernel(kpos_ref, cos_ref, sin_ref, q_ref, k_ref, v_ref, g_ref, dq_ref, dk_ref, dv_ref):
    rows, keys = q_ref.shape[0], k_ref.shape[0]
    group = HEADS // KV_HEADS
    head = pl.program_id(0)
    queries, key, value, grad = q_ref[...], k_ref[...], v_ref[...], g_ref[...]
    scores = (
        lax.dot_general(queries, key, (((1,), (1,)), ((), ())), preferred_element_type=full)
        * scale
    )
    scores = jnp.where(shown(kpos_ref, rows, keys), scores, masked_score)
    top = jnp.max(scores, axis=-1, keepdims=True)
    weights = jnp.exp(scores - top)
    total = jnp.sum(weights, axis=-1, keepdims=True)
    probs = weights * (1.0 / total)
    prob_grad = lax.dot_general(
        grad, value, (((1,), (1,)), ((), ())), preferred_element_type=full
    )
    inner = jnp.sum(probs * prob_grad, axis=-1, keepdims=True)
    score_grad = (probs * (prob_grad - inner)).astype(low)
    dv = lax.dot_general(
        probs.astype(low), grad, (((0,), (0,)), ((), ())), preferred_element_type=full
    )
    dk = (
        lax.dot_general(
            score_grad, queries, (((0,), (0,)), ((), ())), preferred_element_type=full
        )
        * scale
    )
    dq = jnp.dot(score_grad, key, preferred_element_type=full) * scale
    turned = dq * cos_ref[...] - pltpu.roll(dq, HEAD_DIM // 2, 1) * sin_ref[...]
    dq_ref[...] = turned.astype(low)

    @pl.when(head % group == 0)
    def _():
        dk_ref[...] = dk
        dv_ref[...] = dv

    @pl.when(head % group != 0)
    def _():
        dk_ref[...] += dk
        dv_ref[...] += dv


def attend_backward(kpos, cosine, sine, qkv, pairs, grad):
    rows = qkv.shape[0]
    keys = pairs.shape[0]
    group = HEADS // KV_HEADS
    width = KV_HEADS * HEAD_DIM
    return pl.pallas_call(
        bwd_kernel,
        grid=(HEADS,),
        in_specs=[
            pl.BlockSpec((1, keys), lambda h: (0, 0)),
            pl.BlockSpec((rows, HEAD_DIM), lambda h: (0, 0)),
            pl.BlockSpec((rows, HEAD_DIM), lambda h: (0, 0)),
            pl.BlockSpec((rows, HEAD_DIM), lambda h: (0, h)),
            pl.BlockSpec((keys, HEAD_DIM), lambda h: (0, h // group)),
            pl.BlockSpec((keys, HEAD_DIM), lambda h: (0, KV_HEADS + h // group)),
            pl.BlockSpec((rows, HEAD_DIM), lambda h: (0, h)),
        ],
        out_specs=[
            pl.BlockSpec((rows, HEAD_DIM), lambda h: (0, h)),
            pl.BlockSpec((keys, HEAD_DIM), lambda h: (0, h // group)),
            pl.BlockSpec((keys, HEAD_DIM), lambda h: (0, h // group)),
        ],
        out_shape=[
            jax.ShapeDtypeStruct((rows, HEADS * HEAD_DIM), low),
            jax.ShapeDtypeStruct((keys, width), full),
            jax.ShapeDtypeStruct((keys, width), full),
        ],
        cost_estimate=pl.CostEstimate(
            flops=10 * rows * keys * HEADS * HEAD_DIM * 3,
            bytes_accessed=8 * rows * HEADS * HEAD_DIM + 12 * keys * width,
            transcendentals=rows * keys * HEADS,
        ),
        name="attend_backward",
    )(kpos, cosine, sine, qkv, pairs, pairs, grad)


def body(
    tokens, lengths, attn_gain, w_query, b_query, w_key, b_key, w_value, b_value, w_out,
    ffn_gain, w_gate, w_up, w_down, cotangent,
):
    slot_count, rows, width = tokens.shape
    seq_count = lax.axis_size("seq")
    wt_count = lax.axis_size("wt")
    outer = wt_count // INNER
    seq_here = lax.axis_index("seq")
    inner_here = lax.axis_index("wt") % INNER
    line = [[o * INNER + i for o in range(outer)] for i in range(INNER)]
    hops_a, hops_b = plane_hops(seq_count)
    plane = INNER * seq_count
    share = w_query.shape[0]
    bias_q, bias_k = b_query.shape[0], b_key.shape[0]
    query_width = HEADS * HEAD_DIM
    pair_width = KV_HEADS * HEAD_DIM
    head_width = query_width + 2 * pair_width
    ff_own = w_down.shape[0] // seq_count
    ff_here = outer * ff_own
    ff_pad = -(-ff_here // 128) * 128

    flat = tokens.astype(full).reshape(rows, width)
    places = seq_here * rows + jnp.arange(rows, dtype=jnp.int32)
    keep = (places < lengths[0])[:, None]
    upstream_low = jnp.where(keep, cotangent.reshape(rows, width), jnp.zeros((), low))

    def line_gather(value):
        return lax.all_gather(value, "wt", axis=0, axis_index_groups=line, tiled=False)

    def line_reduce(value):
        return lax.psum_scatter(
            value, "wt", scatter_dimension=0, axis_index_groups=line, tiled=False
        )

    def seq_gather(value):
        stacked = gather_hops(value, bits_of("seq", seq_count))
        return jnp.stack([to_place(stacked, seq_here ^ p) for p in range(seq_count)])

    info = jnp.stack([seq_here, inner_here]).astype(jnp.int32)
    down_own = lax.dynamic_slice_in_dim(w_down, seq_here * ff_own, ff_own, axis=0).astype(low)

    def inner_swap(value, distance):
        count = lax.axis_size("wt")
        return lax.ppermute(value, "wt", [(i, i ^ distance) for i in range(count)])

    def inner_exchange(value):
        got = [value[0]] + [inner_swap(value[d], d) for d in range(1, INNER)]
        return jnp.stack(got)

    stacked = inner_exchange(split_units(info, w_gate, w_up, outer, seq_count, ff_own, ff_pad))
    block = jnp.stack([to_place(stacked, inner_here ^ p) for p in range(INNER)])
    block = block.reshape(INNER * share, 2 * ff_pad)
    half = HEAD_DIM // 2
    inverse = 10000.0 ** (-jnp.arange(half, dtype=full) / half)
    angle = places.astype(full)[:, None] * inverse[None, :]
    cosine = jnp.cos(angle)
    sine = jnp.sin(angle)
    cosine = jnp.concatenate([cosine, cosine], axis=1)
    sine = jnp.concatenate([-sine, sine], axis=1)

    def line_of(vector):
        return jnp.pad(vector, (0, HEAD_DIM - vector.shape[0]))

    small = jnp.stack([line_of(v) for v in (attn_gain, b_query, b_key, b_value, ffn_gain)])
    small = jnp.pad(small.astype(low), ((0, 11), (0, 0)))
    packed = jnp.concatenate([w_query, w_key, w_value], axis=1).astype(low)
    normed_low, qkv, vectors, head_all, out_all = gather_project(
        tokens.reshape(rows, width),
        *gather_line(packed, w_out.astype(low), small), cosine, sine,
    )
    head_w = head_all.reshape(width, head_width)
    out_w = out_all.reshape(query_width, width)
    gain_one = vectors[0, :width]
    gain_two = vectors[2, :width]
    units_w = line_gather(block).reshape(width, 2 * ff_pad)
    down_w = line_gather(down_own).reshape(ff_here, width)
    down_w = jnp.pad(down_w, ((0, ff_pad - ff_here), (0, 0)))

    seq_hops = bits_of("seq", seq_count)
    pairs = gather_hops(qkv[:, query_width:], seq_hops).reshape(SLOT, 2 * pair_width)
    distance = jnp.arange(SLOT, dtype=jnp.int32)
    key_place = (seq_here ^ (distance // rows)) * rows + distance % rows
    kpos = jnp.where(key_place < lengths[0], key_place - seq_here * rows, far_place)[None, :]
    mixed = attend_forward(kpos, qkv, pairs)
    resid = flat + product(mixed, out_w)
    normed_two, factor_two = norm_rows(resid, gain_two)
    normed_two_low = normed_two.astype(low)

    core = hops_a[-1]
    slow_a, slow_b = hops_a[:-1], hops_b[:-1]
    near_rows = plane * rows // 2

    def spread(block):
        part_a = gather_hops(block[: rows // 2], slow_a)
        part_b = gather_hops(block[rows // 2 :], slow_b)
        near = jnp.stack([part_a, part_b]).reshape(near_rows, width)
        far = swap(near, core)
        return jnp.concatenate([near, far], axis=0)

    def hop_core(partial):
        other = swap(partial[near_rows:], core)
        near = (partial[:near_rows].astype(full) + other.astype(full)).astype(low)
        near = near.reshape(2, plane // 2, rows // 2, width)
        return (near[0], near[1])

    def hop_slow(parts, stage):
        return tuple(reduce_hop(part, hops[stage]) for part, hops in zip(parts, (slow_a, slow_b)))

    def hop_last(parts):
        got = [reduce_hops(part, hops[:1]) for part, hops in zip(parts, (slow_a, slow_b))]
        return jnp.concatenate(got, axis=0)

    stages = list(range(1, len(slow_a)))[::-1]
    grad_all = spread(upstream_low)
    rows_all = spread(normed_two_low)
    both = product(rows_all, units_w)
    hidden, units_grad = hidden_units(both, grad_all, down_w)
    down_grad = product_left(hidden, grad_all).astype(low)
    units_grad, down_grad = lax.optimization_barrier((units_grad, down_grad))
    down_grad = down_grad[:ff_here]
    partial = product_right(units_grad, units_w).astype(low)
    down_line = line_reduce(down_grad.reshape(outer, ff_own, width))
    back = hop_core(partial)
    rows_late, grad_late = lax.optimization_barrier((rows_all, units_grad, back, down_grad))[:2]
    units_w_grad = product_left(rows_late, grad_late).astype(low)
    units_line = line_reduce(units_w_grad.reshape(outer, INNER * share, 2 * ff_pad))
    for stage in stages:
        back = hop_slow(back, stage)
    hidden_late = after(hidden, back, units_w_grad)
    partial = product(hidden_late, down_w).astype(low)
    normed_two_grad = hop_last(back)

    upstream = upstream_low.astype(full)
    resid_norm_grad, gain_two_grad = norm_back(resid, factor_two, gain_two, normed_two_grad)
    resid_grad = upstream + resid_norm_grad
    attn_grad = resid_grad.astype(low)
    mixed_grad = product_right(attn_grad, out_w).astype(low)
    out_w_grad = product_left(mixed, attn_grad).astype(low)
    query_grad, key_part, value_part = attend_backward(
        kpos, cosine, sine, qkv, pairs, mixed_grad
    )
    forth = hop_core(after(partial, normed_two_grad))
    for stage in stages:
        forth = hop_slow(forth, stage)
    forth = hop_last(lax.optimization_barrier((*forth, query_grad))[:2])
    layer_out = jnp.where(keep, resid + forth, 0.0).astype(low)
    layer_out = layer_out.reshape(slot_count, rows, width)

    blocks = units_line.reshape(INNER, share, 2 * ff_pad)

    def plane_swap(distance, seq_distance):
        block = to_place(blocks, inner_here ^ distance)
        if not distance and not seq_distance:
            return block
        pairs = [
            (w * seq_count + q, (w ^ distance) * seq_count + (q ^ seq_distance))
            for w in range(wt_count)
            for q in range(seq_count)
        ]
        return lax.ppermute(block, ("wt", "seq"), pairs)

    units_got = [
        jnp.stack([plane_swap(a, b) for a in range(INNER)]) for b in range(seq_count)
    ]
    down_out = seq_gather(down_line)
    down_out = down_out.reshape(seq_count * ff_own, width).astype(full)
    pair_part = jnp.concatenate([key_part, value_part], axis=1)
    pair_sum = reduce_hops(
        pair_part.reshape(seq_count, rows, 2 * pair_width).astype(low), seq_hops
    )
    key_rot_grad = pair_sum[:, :pair_width].reshape(rows, KV_HEADS, HEAD_DIM)
    turned = jnp.concatenate([key_rot_grad[..., half:], key_rot_grad[..., :half]], axis=-1)
    key_grad = key_rot_grad * cosine[:, None, :] - turned * sine[:, None, :]
    head_grad = jnp.concatenate(
        [query_grad, key_grad.reshape(rows, pair_width).astype(low),
         pair_sum[:, pair_width:].astype(low)],
        axis=1,
    )
    head_w_grad = product_left(normed_low, head_grad).astype(low)
    head_b_grad = jnp.sum(head_grad.astype(full), axis=0)
    normed_grad = product_right(head_grad, head_w)
    factor_one = lax.rsqrt(jnp.mean(flat * flat, axis=-1, keepdims=True) + epsilon)
    input_norm_grad, gain_one_grad = norm_back(flat, factor_one, gain_one, normed_grad)
    input_grad = (resid_grad + input_norm_grad).astype(low).reshape(slot_count, rows, width)

    edges = [0, share, share + bias_q]
    edges += [edges[-1] + bias_k, edges[-1] + 2 * bias_k]

    def parts(vector):
        return vector.reshape(wt_count, -1)

    small_grad = jnp.concatenate(
        [
            parts(gain_one_grad),
            parts(head_b_grad[:query_width]),
            parts(head_b_grad[query_width : query_width + pair_width]),
            parts(head_b_grad[query_width + pair_width :]),
            parts(gain_two_grad),
        ],
        axis=1,
    ).astype(low)
    small_grad = jnp.pad(small_grad, ((0, 0), (0, 256 * seq_count - small_grad.shape[1])))
    small_grad = jnp.pad(small_grad[:, None, :], ((0, 0), (0, 15), (0, 0)))

    def by_owner(partial):
        return partial.reshape(outer, INNER, -1, partial.shape[-1])

    out_w_out, heads_out, small_out = reduce_shares(
        by_owner(out_w_grad),
        by_owner(head_w_grad),
        by_owner(small_grad),
    )
    small_out = small_out[0]
    gate_out, up_out = join_units(info, jnp.stack(units_got), outer, ff_own)
    return (
        layer_out,
        input_grad,
        small_out[: edges[1]],
        heads_out[:, :query_width],
        small_out[edges[1] : edges[2]],
        heads_out[:, query_width : query_width + pair_width],
        small_out[edges[2] : edges[3]],
        heads_out[:, query_width + pair_width :],
        small_out[edges[3] : edges[4]],
        out_w_out,
        small_out[edges[4] : edges[4] + ffn_gain.shape[0]],
        gate_out,
        up_out,
        down_out,
    )


def solution(mesh):
    by_wt = P("wt")
    by_row = P("wt", None)
    by_token = P("wt", "seq", None)
    return jax.shard_map(
        body,
        mesh=mesh,
        in_specs=(
            by_token, by_wt, by_wt, by_row, by_wt, by_row, by_wt, by_row, by_wt, by_row,
            by_wt, by_row, by_row, by_row, by_token,
        ),
        out_specs=(
            by_token, by_token, by_wt, by_row, by_wt, by_row, by_wt, by_row, by_wt, by_row,
            by_wt, by_row, by_row, by_row,
        ),
        check_vma=False,
    )
```

```python
import functools
import math

import jax
import jax.numpy as jnp
from jax import lax
from jax.experimental import pallas as pl
from jax.experimental.pallas import tpu as pltpu
from jax.sharding import PartitionSpec as P


HEADS = 12
KV_HEADS = 2
HEAD_DIM = 128
SLOT = 1024
INNER = 4

epsilon = 1e-06
masked_score = -1e30
far_place = 1 << 30
scale = 1.0 / math.sqrt(HEAD_DIM)
low = jnp.bfloat16
full = jnp.float32


def product(left, right):
    return jnp.dot(left, right, preferred_element_type=full)


def product_left(left, right):
    return lax.dot_general(left, right, (((0,), (0,)), ((), ())), preferred_element_type=full)


def product_right(left, right):
    return lax.dot_general(left, right, (((1,), (1,)), ((), ())), preferred_element_type=full)


def norm_rows(values, gain):
    factor = lax.rsqrt(jnp.mean(values * values, axis=-1, keepdims=True) + epsilon)
    return (values * factor * gain, factor)


def norm_back(values, factor, gain, upstream):
    weighted = upstream * gain
    inner = jnp.mean(weighted * values, axis=-1, keepdims=True)
    grad_in = factor * weighted - values * (factor * factor * factor) * inner
    grad_gain = jnp.sum(upstream * values * factor, axis=0)
    return (grad_in, grad_gain)


def swap(value, hop):
    axis, bit = hop
    count = lax.axis_size(axis)
    return lax.ppermute(value, axis, [(i, i ^ bit) for i in range(count)])


def gather_hops(block, hops):
    held = block[None]
    for hop in hops:
        held = jnp.concatenate([held, swap(held, hop)], axis=0)
    return held


def reduce_hop(held, hop):
    half = held.shape[0] // 2
    other = swap(held[half:], hop)
    return (held[:half].astype(full) + other.astype(full)).astype(low)


def reduce_hops(held, hops):
    for k in range(len(hops) - 1, 0, -1):
        held = reduce_hop(held, hops[k])
    return held[0].astype(full) + swap(held[1], hops[0]).astype(full)


def bits_of(axis, count):
    found, bit = [], 1
    while bit < count:
        found.append((axis, bit))
        bit *= 2
    return found


def plane_hops(seq_count):
    inner = bits_of("wt", INNER)
    seq = bits_of("seq", seq_count)
    slow = inner[1:] + seq
    return (slow + inner[:1], slow[::-1] + inner[:1])


def to_place(stacked, place):
    return lax.dynamic_index_in_dim(stacked, place, 0, keepdims=False)


def flip(index, bit):
    return index + bit - 2 * bit * ((index // bit) % 2)


def flip_all(index, distance):
    bit = 1
    while bit <= distance:
        if distance & bit:
            index = flip(index, bit)
        bit *= 2
    return index


def inner_bits():
    return [bit for _, bit in bits_of("wt", INNER)]


def meet(peers):
    barrier = pltpu.get_barrier_semaphore()
    for peer in peers:
        pl.semaphore_signal(
            barrier, inc=1, device_id=peer, device_id_type=pl.DeviceIdType.MESH
        )
    pl.semaphore_wait(barrier, len(peers))


class Sender:
    def __init__(self, send_sems, recv_sems):
        self.sems = (send_sems, recv_sems)
        self.copies = []

    def start(self, source, target, peer):
        at = len(self.copies)
        copy = pltpu.make_async_remote_copy(
            src_ref=source,
            dst_ref=target,
            send_sem=self.sems[0].at[at],
            recv_sem=self.sems[1].at[at],
            device_id=peer,
            device_id_type=pl.DeviceIdType.MESH,
        )
        copy.start()
        self.copies.append(copy)
        return copy


def subsets(hops):
    found = [(0, 0)]
    for axis, bit in hops:
        more = [(a ^ bit, b) if axis == "wt" else (a, b ^ bit) for a, b in found]
        found = found + more
    return found


def plane_copies(seq_count):
    hops_a, _ = plane_hops(seq_count)
    slow = len(hops_a) - 1
    return (2 * (2**slow - 1), len(set(a for a, _ in subsets(hops_a[:-1]))))


def line_kernel(outer, seq_count, p_ref, s_ref, head_ref, small_ref, *sems):
    send_sems, recv_sems, local_sems = sems
    wt, seq = lax.axis_index("wt"), lax.axis_index("seq")
    line, inner = wt // INNER, wt % INNER

    def own_columns(total):
        wide = total // seq_count
        return pl.ds(pl.multiple_of(seq * wide, 128), wide)

    pairs = [
        (s_ref, small_ref),
        (p_ref.at[:, own_columns(p_ref.shape[1])], head_ref),
    ]
    own = [
        pltpu.make_async_copy(source, target.at[0], local_sems.at[k])
        for k, (source, target) in enumerate(pairs)
    ]
    for copy in own:
        copy.start()
    peers = [(flip_all(line, d) * INNER + inner, seq) for d in range(1, outer)]
    meet(peers)
    out = Sender(send_sems, recv_sems)
    for source, target in pairs:
        for d in range(1, outer):
            out.start(source, target.at[d], peers[d - 1])
    for copy in own:
        copy.wait()
    for copy in out.copies:
        copy.wait()


def gather_line(packed, small):
    outer = lax.axis_size("wt") // INNER
    seq_count = lax.axis_size("seq")
    share, head_width = packed.shape
    vmem = pl.BlockSpec(memory_space=pltpu.VMEM)
    copies = 2 * (outer - 1)
    sent = 2 * outer * share * head_width
    return pl.pallas_call(
        functools.partial(line_kernel, outer, seq_count),
        in_specs=[vmem] * 2,
        out_specs=[vmem] * 2,
        out_shape=[
            jax.ShapeDtypeStruct((outer, share, head_width // seq_count), low),
            jax.ShapeDtypeStruct((outer,) + small.shape, low),
        ],
        scratch_shapes=[
            pltpu.SemaphoreType.DMA((copies,)),
            pltpu.SemaphoreType.DMA((copies,)),
            pltpu.SemaphoreType.DMA((2,)),
        ],
        compiler_params=pltpu.CompilerParams(collective_id=3, has_side_effects=True),
        cost_estimate=pl.CostEstimate(flops=0, bytes_accessed=8 * sent, transcendentals=0),
        name="gather_line",
    )(packed, small)


def gather_kernel(
    outer, seq_count, x_ref, p_ref, wo_ref, s_ref, cos_ref, sin_ref,
    normed_ref, qkv_ref, vec_ref, head_ref, out_ref,
    w_scr, o_scr, s_scr, send_sems, recv_sems, local_sems,
):
    share, head_width = p_ref.shape[1], w_scr.shape[3]
    width = x_ref.shape[1]
    wt, seq = lax.axis_index("wt"), lax.axis_index("seq")
    line, inner = wt // INNER, wt % INNER
    hops = plane_hops(seq_count)
    slow = len(hops[0]) - 1
    line_peers = [(flip_all(line, d) * INNER + inner, seq) for d in range(1, outer)]
    peers = [(wt - inner + flip(inner, bit), seq) for bit in inner_bits()]
    peers += [(wt, flip(seq, bit)) for _, bit in bits_of("seq", seq_count)] + line_peers

    def own_columns(total):
        wide = total // seq_count
        return pl.ds(pl.multiple_of(seq * wide, 128), wide)

    mine = own_columns(o_scr.shape[3])
    fill = [
        pltpu.make_async_copy(
            wo_ref.at[:, mine], o_scr.at[line, inner, :, mine], local_sems.at[2 * outer]
        )
    ]
    for d in range(outer):
        at = flip_all(line, d)
        pairs = [
            (s_ref.at[d], s_scr.at[at, inner]),
            (p_ref.at[d], w_scr.at[at, inner, :, own_columns(head_width)]),
        ]
        fill += [
            pltpu.make_async_copy(source, target, local_sems.at[2 * d + k])
            for k, (source, target) in enumerate(pairs)
        ]
    for copy in fill:
        copy.start()
    meet(peers)
    out = Sender(send_sems, recv_sems)

    def hop_peer(hop):
        axis, bit = hop
        if axis == "wt":
            return (wt - inner + flip(inner, bit), seq)
        return (wt, flip(seq, bit))

    def columns(total, part, half):
        wide = total // seq_count
        first = -(-wide // 256) * 128
        start = part * wide + half * first
        return pl.ds(pl.multiple_of(start, 128), wide - first if half else first)

    def start_stage(scratch, at, stage):
        total = scratch.shape[-1]
        copies = []
        if stage < slow:
            for half in range(2):
                hop = hops[half][stage]
                for a, b in subsets(hops[half][:stage]):
                    place = scratch.at[
                        at, flip_all(inner, a), :, columns(total, flip_all(seq, b), half)
                    ]
                    copies.append(out.start(place, place, hop_peer(hop)))
            return copies
        for a in sorted(set(a for a, _ in subsets(hops[0][:slow]))):
            place = scratch.at[at, flip_all(inner, a)]
            copies.append(out.start(place, place, hop_peer(hops[0][slow])))
        return copies

    def arrive(copies):
        for copy in copies:
            if copy is not None:
                copy.wait_recv()

    out_line = [
        out.start(wo_ref.at[:, mine], o_scr.at[line, inner, :, mine], peer)
        for peer in line_peers
    ]
    for copy in fill:
        copy.wait()
    waiting = [[] for _ in range(outer)]
    small_wait = []
    for step in range(outer + slow + 1):
        for stage in range(slow + 1):
            d = step - stage
            if 0 <= d < outer:
                arrive(waiting[d])
                waiting[d] = start_stage(w_scr, flip_all(line, d), stage)
        if step < len(inner_bits()):
            arrive(small_wait)
            bit = inner_bits()[::-1][step]
            small_wait = []
            for a, _ in subsets([("wt", b) for b in inner_bits()[::-1][:step]]):
                place = s_scr.at[:, flip_all(inner, a)]
                small_wait.append(out.start(place, place, hop_peer(("wt", bit))))
    arrive(small_wait)
    arrive(out_line)
    out_wait = start_stage(o_scr, slice(None), 0)

    count = outer * INNER
    bias_k = share * KV_HEADS * HEAD_DIM // (HEADS * HEAD_DIM)
    query_width = HEADS * HEAD_DIM
    pair_width = KV_HEADS * HEAD_DIM
    vec_ref[...] = jnp.zeros_like(vec_ref)
    for k in range(count):
        small = s_scr[k // INNER, k % INNER].astype(full)
        at = k * share
        vec_ref[0:1, at : at + share] = small[0:1, :share]
        vec_ref[1:2, at : at + share] = small[1:2, :share]
        at = query_width + k * bias_k
        vec_ref[1:2, at : at + bias_k] = small[2:3, :bias_k]
        at = query_width + pair_width + k * bias_k
        vec_ref[1:2, at : at + bias_k] = small[3:4, :bias_k]
        at = k * share
        vec_ref[2:3, at : at + share] = small[4:5, :share]

    values = x_ref[...].astype(full)
    factor = lax.rsqrt(jnp.mean(values * values, axis=-1, keepdims=True) + epsilon)
    normed_ref[...] = (values * factor * vec_ref[0:1, :width]).astype(low)
    for d in range(outer):
        arrive(waiting[d])
    keep_head = pltpu.make_async_copy(w_scr, head_ref, local_sems.at[0])
    keep_head.start()
    wide = 2 * HEAD_DIM
    blocks = head_width // wide

    def project(at):
        weights = w_scr[:, :, :, pl.ds(at, wide)].reshape(width, wide)
        return (
            jnp.dot(normed_ref[...], weights, preferred_element_type=full)
            + vec_ref[1:2, pl.ds(at, wide)]
        )

    def turn_block(k):
        at = pl.multiple_of(k * wide, wide)
        got = project(at)
        for j in range(2):
            part = got[:, j * HEAD_DIM : (j + 1) * HEAD_DIM]
            turned = part * cos_ref[...] + pltpu.roll(part, HEAD_DIM // 2, 1) * sin_ref[...]
            where = pl.multiple_of(at + j * HEAD_DIM, HEAD_DIM)
            qkv_ref[:, pl.ds(where, HEAD_DIM)] = turned.astype(low)

    turned_blocks = blocks - pair_width // wide
    marks = [turned_blocks * (k + 1) // (slow + 1) for k in range(slow + 1)]
    begin = 0
    for stage in range(slow + 1):
        @pl.loop(begin, marks[stage])
        def _(k):
            turn_block(k)

        begin = marks[stage]
        arrive(out_wait)
        out_wait = start_stage(o_scr, slice(None), stage + 1) if stage < slow else []
    for k in range(turned_blocks, blocks):
        qkv_ref[:, k * wide : (k + 1) * wide] = project(k * wide).astype(low)
    keep_out = pltpu.make_async_copy(o_scr, out_ref, local_sems.at[1])
    keep_out.start()
    for copy in out.copies:
        copy.wait_send()
    keep_head.wait()
    keep_out.wait()


def gather_project(tokens, packed, w_out, small, cosine, sine):
    outer = lax.axis_size("wt") // INNER
    seq_count = lax.axis_size("seq")
    rows, width = tokens.shape
    share, head_width = packed.shape[1], packed.shape[2] * seq_count
    out_width = w_out.shape[1]
    slow_copies, last_copies = plane_copies(seq_count)
    each = slow_copies + last_copies
    small_copies = 2 ** len(inner_bits()) - 1
    copies = (outer + 1) * each + small_copies + outer - 1
    vmem = pl.BlockSpec(memory_space=pltpu.VMEM)
    anywhere = pl.BlockSpec(memory_space=pl.ANY)
    sent = 2 * outer * INNER * share * (head_width + out_width)
    return pl.pallas_call(
        functools.partial(gather_kernel, outer, seq_count),
        in_specs=[vmem] * 6,
        out_specs=[vmem, vmem, vmem, anywhere, anywhere],
        out_shape=[
            jax.ShapeDtypeStruct((rows, width), low),
            jax.ShapeDtypeStruct((rows, head_width), low),
            jax.ShapeDtypeStruct((8, head_width), full),
            jax.ShapeDtypeStruct((outer, INNER, share, head_width), low),
            jax.ShapeDtypeStruct((outer, INNER, share, out_width), low),
        ],
        scratch_shapes=[
            pltpu.VMEM((outer, INNER, share, head_width), low),
            pltpu.VMEM((outer, INNER, share, out_width), low),
            pltpu.VMEM((outer, INNER) + small.shape[1:], low),
            pltpu.SemaphoreType.DMA((copies,)),
            pltpu.SemaphoreType.DMA((copies,)),
            pltpu.SemaphoreType.DMA((2 * outer + 1,)),
        ],
        compiler_params=pltpu.CompilerParams(
            collective_id=1, has_side_effects=True, vmem_limit_bytes=48 << 20
        ),
        cost_estimate=pl.CostEstimate(
            flops=2 * rows * width * head_width * 8, bytes_accessed=2 * sent, transcendentals=0
        ),
        name="gather_project",
    )(tokens, packed, w_out, small, cosine, sine)


def near_inner(seq_count):
    hops = plane_hops(seq_count)[0]
    return sorted(set(a for a, _ in subsets(hops[:-1])))


def reduce_kernel(outer, seq_count, count, *refs):
    given, results = refs[:count], refs[count : 2 * count]
    slow = len(plane_hops(seq_count)[0]) - 1
    held = refs[2 * count : 3 * count]
    lines = refs[3 * count : 4 * count]
    joined = refs[4 * count : 5 * count]
    landed = refs[5 * count : (6 + slow) * count]
    send_sems, recv_sems = refs[(6 + slow) * count :]
    wt, seq = lax.axis_index("wt"), lax.axis_index("seq")
    line, inner = wt // INNER, wt % INNER
    hops = plane_hops(seq_count)
    nears = near_inner(seq_count)
    peers = [(flip_all(line, d) * INNER + inner, seq) for d in range(1, outer)]
    peers += [(wt - inner + flip(inner, bit), seq) for bit in inner_bits()]
    peers += [(wt, flip_all(seq, d)) for d in range(1, seq_count)]
    meet(peers)
    out = Sender(send_sems, recv_sems)

    def hop_peer(hop):
        axis, bit = hop
        if axis == "wt":
            return (wt - inner + flip(inner, bit), seq)
        return (wt, flip(seq, bit))

    def columns(total, part, half):
        wide = total // seq_count
        first = -(-wide // 256) * 128
        start = part * wide + half * first
        return pl.ds(pl.multiple_of(start, 128), wide - first if half else first)

    def arrive(copies):
        for copy in copies:
            copy.wait_recv()

    def steps(k):
        source, total = given[k], given[k].shape[3]
        sums, wide = held[k], given[k].shape[3] // seq_count
        own = pl.ds(pl.multiple_of(seq * wide, 128), wide)
        core = hops[0][slow]
        copies = [
            out.start(
                source.at[:, flip_all(inner, a ^ core[1])],
                landed[k].at[:, at],
                hop_peer(core),
            )
            for at, a in enumerate(nears)
        ]
        yield
        arrive(copies)
        for at, a in enumerate(nears):
            place = flip_all(inner, a)

            @pl.loop(0, outer)
            def _(o):
                both = source[o, place].astype(full) + landed[k][o, at].astype(full)
                sums[o, at] = both.astype(low)

        for stage in range(slow - 1, -1, -1):
            target = landed[(1 + stage) * count + k]
            copies, blocks = [], []
            for half in range(2):
                axis, bit = hops[half][stage]
                for a, b in subsets(hops[half][:stage]):
                    from_a = a ^ bit if axis == "wt" else a
                    from_b = b ^ bit if axis == "seq" else b
                    sent = columns(total, flip_all(seq, from_b), half)
                    copies.append(
                        out.start(
                            sums.at[:, nears.index(from_a), :, sent],
                            target.at[:, nears.index(a), :, sent],
                            hop_peer((axis, bit)),
                        )
                    )
                    blocks.append((nears.index(a), columns(total, flip_all(seq, b), half)))
            yield
            arrive(copies)
            for at, part in blocks:

                @pl.loop(0, outer)
                def _(o):
                    both = sums[o, at, :, part].astype(full) + target[o, at, :, part].astype(full)
                    sums[o, at, :, part] = both.astype(low)

        copies = [
            out.start(
                sums.at[flip_all(line, d), 0, :, own],
                lines[k].at[d],
                (flip_all(line, d) * INNER + inner, seq),
            )
            for d in range(1, outer)
        ]
        yield
        arrive(copies)
        both = sums[line, 0, :, own].astype(full)
        for d in range(1, outer):
            both = both + lines[k][d].astype(full)
        joined[k][:, own] = both.astype(low)
        copies = [
            out.start(joined[k].at[:, own], joined[k].at[:, own], (wt, flip_all(seq, d)))
            for d in range(1, seq_count)
        ]
        yield
        arrive(copies)
        results[k][...] = joined[k][...].astype(full)

    running = [steps(k) for k in range(count)]
    for _ in range(2):
        next(running[0])
    while running:
        for one in list(running):
            if next(one, "done") == "done":
                running.remove(one)
    for copy in out.copies:
        copy.wait_send()


def reduce_shares(*partials):
    outer = lax.axis_size("wt") // INNER
    seq_count = lax.axis_size("seq")
    count = len(partials)
    slow = len(plane_hops(seq_count)[0]) - 1
    nears = len(near_inner(seq_count))
    vmem = pl.BlockSpec(memory_space=pltpu.VMEM)
    near = [
        pltpu.VMEM((outer, nears) + p.shape[2:], low) for p in partials
    ]
    shapes = [p.shape[2:] for p in partials]
    copies = count * (nears + 2 * (2**slow - 1) + outer - 1 + seq_count - 1)
    sent = sum(2 * p.size for p in partials)
    return pl.pallas_call(
        functools.partial(reduce_kernel, outer, seq_count, count),
        in_specs=[vmem] * count,
        out_specs=[vmem] * count,
        out_shape=[jax.ShapeDtypeStruct(shape, full) for shape in shapes],
        scratch_shapes=near
        + [pltpu.VMEM((outer, r, c // seq_count), low) for r, c in shapes]
        + [pltpu.VMEM(shape, low) for shape in shapes]
        + near * (1 + slow)
        + [pltpu.SemaphoreType.DMA((n,)) for n in (copies, copies)],
        compiler_params=pltpu.CompilerParams(
            collective_id=2, has_side_effects=True, vmem_limit_bytes=60 << 20
        ),
        cost_estimate=pl.CostEstimate(flops=0, bytes_accessed=8 * sent, transcendentals=0),
        name="reduce_shares",
    )(*partials)


def split_kernel(outer, seq_count, own, info_ref, gate_ref, up_ref, o_ref):
    inner = info_ref[1]
    width = outer * own
    padded = o_ref.shape[2] // 2
    for s in range(seq_count):
        @pl.when(info_ref[0] == s)
        def _():
            for q in range(INNER):
                place = jnp.bitwise_xor(inner, q)
                for k, ref in enumerate((gate_ref, up_ref)):
                    for o in range(outer):
                        at = ((o * INNER + q) * seq_count + s) * own
                        to = k * padded + o * own
                        o_ref[place, :, to : to + own] = ref[:, at : at + own].astype(low)
                    if padded > width:
                        blank = jnp.zeros((o_ref.shape[1], padded - width), low)
                        o_ref[place, :, k * padded + width : (k + 1) * padded] = blank


def split_units(info, gate, up, outer, seq_count, own, padded):
    vmem = pl.BlockSpec(memory_space=pltpu.VMEM)
    return pl.pallas_call(
        functools.partial(split_kernel, outer, seq_count, own),
        in_specs=[pl.BlockSpec(memory_space=pltpu.SMEM), vmem, vmem],
        out_specs=vmem,
        out_shape=jax.ShapeDtypeStruct((INNER, gate.shape[0], 2 * padded), low),
        name="split_units",
    )(info, gate, up)


def join_kernel(outer, seq_count, own, info_ref, u_ref, gate_ref, up_ref):
    seq, inner = info_ref[0], info_ref[1]
    padded = u_ref.shape[3] // 2
    for s in range(seq_count):
        for q in range(INNER):
            block = u_ref[jnp.bitwise_xor(seq, s), jnp.bitwise_xor(inner, q)].astype(full)
            for k, ref in enumerate((gate_ref, up_ref)):
                for o in range(outer):
                    at = ((o * INNER + q) * seq_count + s) * own
                    source = k * padded + o * own
                    ref[:, at : at + own] = block[:, source : source + own]


def join_units(info, units, outer, own):
    seq_count, _, rows, _ = units.shape
    vmem = pl.BlockSpec(memory_space=pltpu.VMEM)
    shape = jax.ShapeDtypeStruct((rows, outer * INNER * seq_count * own), full)
    return pl.pallas_call(
        functools.partial(join_kernel, outer, seq_count, own),
        in_specs=[pl.BlockSpec(memory_space=pltpu.SMEM), vmem],
        out_specs=[vmem, vmem],
        out_shape=[shape, shape],
        name="join_units",
    )(info, units)


def hidden_kernel(near_ref, far_ref, grad_ref, down_ref, hidden_ref, units_ref):
    wide = hidden_ref.shape[1]
    hidden_grad = lax.dot_general(
        grad_ref[...], down_ref[...], (((1,), (1,)), ((), ())), preferred_element_type=full
    )
    step, half = pl.program_id(0), pl.num_programs(0) // 2

    def finish(both_ref):
        gate, upper = both_ref[:, :wide], both_ref[:, wide:]
        sigma = 1.0 / (1.0 + jnp.exp(-gate))
        taken = gate * sigma
        hidden_ref[...] = (taken * upper).astype(low)
        slope = sigma * (1.0 + gate * (1.0 - sigma))
        units_ref[:, :wide] = (hidden_grad * upper * slope).astype(low)
        units_ref[:, wide:] = (hidden_grad * taken).astype(low)

    @pl.when(step < half)
    def _():
        finish(near_ref)

    @pl.when(step >= half)
    def _():
        finish(far_ref)


def hidden_units(near, far, grad, down_w):
    total, width = grad.shape
    wide = down_w.shape[0]
    block = min(512, total // 2)
    half = total // block // 2
    return pl.pallas_call(
        hidden_kernel,
        grid=(total // block,),
        in_specs=[
            pl.BlockSpec((block, 2 * wide), lambda i: (jnp.minimum(i, half - 1), 0)),
            pl.BlockSpec((block, 2 * wide), lambda i: (jnp.maximum(i - half, 0), 0)),
            pl.BlockSpec((block, width), lambda i: (i, 0)),
            pl.BlockSpec((wide, width), lambda i: (0, 0), pipeline_mode=pl.Buffered(1)),
        ],
        out_specs=[
            pl.BlockSpec((block, wide), lambda i: (i, 0)),
            pl.BlockSpec((block, 2 * wide), lambda i: (i, 0)),
        ],
        out_shape=[
            jax.ShapeDtypeStruct((total, wide), low),
            jax.ShapeDtypeStruct((total, 2 * wide), low),
        ],
        compiler_params=pltpu.CompilerParams(vmem_limit_bytes=60 << 20),
        cost_estimate=pl.CostEstimate(
            flops=2 * total * width * wide,
            bytes_accessed=2 * total * (width + 7 * wide) + 2 * wide * width,
            transcendentals=total * wide,
        ),
        name="hidden_units",
    )(near, far, grad, down_w)


def after(value, *others):
    return lax.optimization_barrier((value, *others))[0]


def shown(kpos_ref, rows, keys):
    places = lax.broadcasted_iota(jnp.int32, (rows, keys), 0)
    return kpos_ref[...] <= places


def fwd_kernel(kpos_ref, q_ref, k_ref, v_ref, o_ref):
    rows, keys = q_ref.shape[0], k_ref.shape[0]
    scores = (
        lax.dot_general(
            q_ref[...], k_ref[...], (((1,), (1,)), ((), ())), preferred_element_type=full
        )
        * scale
    )
    scores = jnp.where(shown(kpos_ref, rows, keys), scores, masked_score)
    top = jnp.max(scores, axis=-1, keepdims=True)
    weights = jnp.exp(scores - top)
    total = jnp.sum(weights, axis=-1, keepdims=True)
    probs = (weights * (1.0 / total)).astype(low)
    o_ref[...] = jnp.dot(probs, v_ref[...], preferred_element_type=full).astype(low)


def attend_forward(kpos, qkv, pairs):
    rows = qkv.shape[0]
    keys = pairs.shape[0]
    group = HEADS // KV_HEADS
    return pl.pallas_call(
        fwd_kernel,
        grid=(HEADS,),
        in_specs=[
            pl.BlockSpec((1, keys), lambda h: (0, 0)),
            pl.BlockSpec((rows, HEAD_DIM), lambda h: (0, h)),
            pl.BlockSpec((keys, HEAD_DIM), lambda h: (0, h // group)),
            pl.BlockSpec((keys, HEAD_DIM), lambda h: (0, KV_HEADS + h // group)),
        ],
        out_specs=pl.BlockSpec((rows, HEAD_DIM), lambda h: (0, h)),
        out_shape=jax.ShapeDtypeStruct((rows, HEADS * HEAD_DIM), low),
        cost_estimate=pl.CostEstimate(
            flops=4 * rows * keys * HEADS * HEAD_DIM * 3,
            bytes_accessed=4 * rows * HEADS * HEAD_DIM + 4 * keys * KV_HEADS * HEAD_DIM,
            transcendentals=rows * keys * HEADS,
        ),
        name="attend_forward",
    )(kpos, qkv, pairs, pairs)


def bwd_kernel(kpos_ref, cos_ref, sin_ref, q_ref, k_ref, v_ref, g_ref, dq_ref, dk_ref, dv_ref):
    rows, keys = q_ref.shape[0], k_ref.shape[0]
    group = HEADS // KV_HEADS
    head = pl.program_id(0)
    queries, key, value, grad = q_ref[...], k_ref[...], v_ref[...], g_ref[...]
    scores = (
        lax.dot_general(queries, key, (((1,), (1,)), ((), ())), preferred_element_type=full)
        * scale
    )
    scores = jnp.where(shown(kpos_ref, rows, keys), scores, masked_score)
    top = jnp.max(scores, axis=-1, keepdims=True)
    weights = jnp.exp(scores - top)
    total = jnp.sum(weights, axis=-1, keepdims=True)
    probs = weights * (1.0 / total)
    prob_grad = lax.dot_general(
        grad, value, (((1,), (1,)), ((), ())), preferred_element_type=full
    )
    inner = jnp.sum(probs * prob_grad, axis=-1, keepdims=True)
    score_grad = (probs * (prob_grad - inner)).astype(low)
    dv = lax.dot_general(
        probs.astype(low), grad, (((0,), (0,)), ((), ())), preferred_element_type=full
    )
    dk = (
        lax.dot_general(
            score_grad, queries, (((0,), (0,)), ((), ())), preferred_element_type=full
        )
        * scale
    )
    dq = jnp.dot(score_grad, key, preferred_element_type=full) * scale
    turned = dq * cos_ref[...] - pltpu.roll(dq, HEAD_DIM // 2, 1) * sin_ref[...]
    dq_ref[...] = turned.astype(low)

    @pl.when(head % group == 0)
    def _():
        dk_ref[...] = dk
        dv_ref[...] = dv

    @pl.when(head % group != 0)
    def _():
        dk_ref[...] += dk
        dv_ref[...] += dv


def attend_backward(kpos, cosine, sine, qkv, pairs, grad):
    rows = qkv.shape[0]
    keys = pairs.shape[0]
    group = HEADS // KV_HEADS
    width = KV_HEADS * HEAD_DIM
    return pl.pallas_call(
        bwd_kernel,
        grid=(HEADS,),
        in_specs=[
            pl.BlockSpec((1, keys), lambda h: (0, 0)),
            pl.BlockSpec((rows, HEAD_DIM), lambda h: (0, 0)),
            pl.BlockSpec((rows, HEAD_DIM), lambda h: (0, 0)),
            pl.BlockSpec((rows, HEAD_DIM), lambda h: (0, h)),
            pl.BlockSpec((keys, HEAD_DIM), lambda h: (0, h // group)),
            pl.BlockSpec((keys, HEAD_DIM), lambda h: (0, KV_HEADS + h // group)),
            pl.BlockSpec((rows, HEAD_DIM), lambda h: (0, h)),
        ],
        out_specs=[
            pl.BlockSpec((rows, HEAD_DIM), lambda h: (0, h)),
            pl.BlockSpec((keys, HEAD_DIM), lambda h: (0, h // group)),
            pl.BlockSpec((keys, HEAD_DIM), lambda h: (0, h // group)),
        ],
        out_shape=[
            jax.ShapeDtypeStruct((rows, HEADS * HEAD_DIM), low),
            jax.ShapeDtypeStruct((keys, width), full),
            jax.ShapeDtypeStruct((keys, width), full),
        ],
        cost_estimate=pl.CostEstimate(
            flops=10 * rows * keys * HEADS * HEAD_DIM * 3,
            bytes_accessed=8 * rows * HEADS * HEAD_DIM + 12 * keys * width,
            transcendentals=rows * keys * HEADS,
        ),
        name="attend_backward",
    )(kpos, cosine, sine, qkv, pairs, pairs, grad)


def body(
    tokens, lengths, attn_gain, w_query, b_query, w_key, b_key, w_value, b_value, w_out,
    ffn_gain, w_gate, w_up, w_down, cotangent,
):
    slot_count, rows, width = tokens.shape
    seq_count = lax.axis_size("seq")
    wt_count = lax.axis_size("wt")
    outer = wt_count // INNER
    seq_here = lax.axis_index("seq")
    inner_here = lax.axis_index("wt") % INNER
    line = [[o * INNER + i for o in range(outer)] for i in range(INNER)]
    hops_a, hops_b = plane_hops(seq_count)
    plane = INNER * seq_count
    share = w_query.shape[0]
    bias_q, bias_k = b_query.shape[0], b_key.shape[0]
    query_width = HEADS * HEAD_DIM
    pair_width = KV_HEADS * HEAD_DIM
    head_width = query_width + 2 * pair_width
    ff_own = w_down.shape[0] // seq_count
    ff_here = outer * ff_own
    ff_pad = -(-ff_here // 128) * 128

    flat = tokens.astype(full).reshape(rows, width)
    places = seq_here * rows + jnp.arange(rows, dtype=jnp.int32)
    keep = (places < lengths[0])[:, None]
    upstream_low = jnp.where(keep, cotangent.reshape(rows, width), jnp.zeros((), low))

    def line_gather(value):
        return lax.all_gather(value, "wt", axis=0, axis_index_groups=line, tiled=False)

    def line_reduce(value):
        return lax.psum_scatter(
            value, "wt", scatter_dimension=0, axis_index_groups=line, tiled=False
        )

    def seq_gather(value):
        stacked = gather_hops(value, bits_of("seq", seq_count))
        return jnp.stack([to_place(stacked, seq_here ^ p) for p in range(seq_count)])

    info = jnp.stack([seq_here, inner_here]).astype(jnp.int32)
    down_own = lax.dynamic_slice_in_dim(w_down, seq_here * ff_own, ff_own, axis=0).astype(low)

    def inner_swap(value, distance):
        count = lax.axis_size("wt")
        return lax.ppermute(value, "wt", [(i, i ^ distance) for i in range(count)])

    def inner_exchange(value):
        got = [value[0]] + [inner_swap(value[d], d) for d in range(1, INNER)]
        return jnp.stack(got)

    stacked = inner_exchange(split_units(info, w_gate, w_up, outer, seq_count, ff_own, ff_pad))
    block = jnp.stack([to_place(stacked, inner_here ^ p) for p in range(INNER)])
    block = block.reshape(INNER * share, 2 * ff_pad)
    half = HEAD_DIM // 2
    inverse = 10000.0 ** (-jnp.arange(half, dtype=full) / half)
    angle = places.astype(full)[:, None] * inverse[None, :]
    cosine = jnp.cos(angle)
    sine = jnp.sin(angle)
    cosine = jnp.concatenate([cosine, cosine], axis=1)
    sine = jnp.concatenate([-sine, sine], axis=1)

    def line_of(vector):
        return jnp.pad(vector, (0, HEAD_DIM - vector.shape[0]))

    small = jnp.stack([line_of(v) for v in (attn_gain, b_query, b_key, b_value, ffn_gain)])
    small = jnp.pad(small.astype(low), ((0, 11), (0, 0)))
    packed = jnp.concatenate([w_query, w_key, w_value], axis=1).astype(low)
    head_line, small_line = gather_line(packed, small)
    project_inputs = (head_line, w_out.astype(low), small_line)
    normed_low, qkv, vectors, head_all, out_all = gather_project(
        tokens.reshape(rows, width),
        *project_inputs, cosine, sine,
    )
    head_w = head_all.reshape(width, head_width)
    out_w = out_all.reshape(query_width, width)
    gain_one = vectors[0, :width]
    gain_two = vectors[2, :width]
    units_w = line_gather(block).reshape(width, 2 * ff_pad)
    down_w = line_gather(down_own).reshape(ff_here, width)
    down_w = jnp.pad(down_w, ((0, ff_pad - ff_here), (0, 0)))

    seq_hops = bits_of("seq", seq_count)
    pairs = gather_hops(qkv[:, query_width:], seq_hops).reshape(SLOT, 2 * pair_width)
    distance = jnp.arange(SLOT, dtype=jnp.int32)
    key_place = (seq_here ^ (distance // rows)) * rows + distance % rows
    kpos = jnp.where(key_place < lengths[0], key_place - seq_here * rows, far_place)[None, :]
    mixed = attend_forward(kpos, qkv, pairs)
    resid = flat + product(mixed, out_w)
    normed_two, factor_two = norm_rows(resid, gain_two)
    normed_two_low = normed_two.astype(low)

    core = hops_a[-1]
    slow_a, slow_b = hops_a[:-1], hops_b[:-1]
    near_rows = plane * rows // 2

    def spread(block):
        part_a = gather_hops(block[: rows // 2], slow_a)
        part_b = gather_hops(block[rows // 2 :], slow_b)
        near = jnp.stack([part_a, part_b]).reshape(near_rows, width)
        far = swap(near, core)
        return (near, far, jnp.concatenate([near, far], axis=0))

    def hop_core(partial):
        other = swap(partial[near_rows:], core)
        near = (partial[:near_rows].astype(full) + other.astype(full)).astype(low)
        near = near.reshape(2, plane // 2, rows // 2, width)
        return (near[0], near[1])

    def hop_slow(parts, stage):
        return tuple(reduce_hop(part, hops[stage]) for part, hops in zip(parts, (slow_a, slow_b)))

    def hop_last(parts):
        got = [reduce_hops(part, hops[:1]) for part, hops in zip(parts, (slow_a, slow_b))]
        return jnp.concatenate(got, axis=0)

    stages = list(range(1, len(slow_a)))[::-1]
    grad_all = spread(upstream_low)[2]
    rows_near, rows_far, rows_all = spread(normed_two_low)
    both_near = product(rows_near, units_w)
    both_far = product(rows_far, units_w)
    hidden, units_grad = hidden_units(both_near, both_far, grad_all, down_w)
    down_grad = product_left(hidden, grad_all).astype(low)
    units_grad, down_grad = lax.optimization_barrier((units_grad, down_grad))
    down_grad = down_grad[:ff_here]
    partial = product_right(units_grad, units_w).astype(low)
    down_line = line_reduce(down_grad.reshape(outer, ff_own, width))
    back = hop_core(partial)
    rows_late, grad_late = lax.optimization_barrier((rows_all, units_grad, back, down_grad))[:2]
    units_w_grad = product_left(rows_late, grad_late).astype(low)
    units_line = line_reduce(units_w_grad.reshape(outer, INNER * share, 2 * ff_pad))
    for stage in stages:
        back = hop_slow(back, stage)
    hidden_late = after(hidden, back, units_w_grad)
    partial = product(hidden_late, down_w).astype(low)
    normed_two_grad = hop_last(back)

    upstream = upstream_low.astype(full)
    resid_norm_grad, gain_two_grad = norm_back(resid, factor_two, gain_two, normed_two_grad)
    resid_grad = upstream + resid_norm_grad
    attn_grad = resid_grad.astype(low)
    mixed_grad = product_right(attn_grad, out_w).astype(low)
    out_w_grad = product_left(mixed, attn_grad).astype(low)
    query_grad, key_part, value_part = attend_backward(
        kpos, cosine, sine, qkv, pairs, mixed_grad
    )
    forth = hop_core(after(partial, normed_two_grad))
    for stage in stages:
        forth = hop_slow(forth, stage)
    forth = hop_last(lax.optimization_barrier((*forth, query_grad))[:2])
    layer_out = jnp.where(keep, resid + forth, 0.0).astype(low)
    layer_out = layer_out.reshape(slot_count, rows, width)

    blocks = units_line.reshape(INNER, share, 2 * ff_pad)

    def plane_swap(distance, seq_distance):
        block = to_place(blocks, inner_here ^ distance)
        if not distance and not seq_distance:
            return block
        pairs = [
            (w * seq_count + q, (w ^ distance) * seq_count + (q ^ seq_distance))
            for w in range(wt_count)
            for q in range(seq_count)
        ]
        return lax.ppermute(block, ("wt", "seq"), pairs)

    units_got = [
        jnp.stack([plane_swap(a, b) for a in range(INNER)]) for b in range(seq_count)
    ]
    down_out = seq_gather(down_line)
    down_out = down_out.reshape(seq_count * ff_own, width).astype(full)
    pair_part = jnp.concatenate([key_part, value_part], axis=1)
    pair_sum = reduce_hops(
        pair_part.reshape(seq_count, rows, 2 * pair_width).astype(low), seq_hops
    )
    key_rot_grad = pair_sum[:, :pair_width].reshape(rows, KV_HEADS, HEAD_DIM)
    turned = jnp.concatenate([key_rot_grad[..., half:], key_rot_grad[..., :half]], axis=-1)
    key_grad = key_rot_grad * cosine[:, None, :] - turned * sine[:, None, :]
    head_grad = jnp.concatenate(
        [query_grad, key_grad.reshape(rows, pair_width).astype(low),
         pair_sum[:, pair_width:].astype(low)],
        axis=1,
    )
    head_w_grad = product_left(normed_low, head_grad).astype(low)
    head_b_grad = jnp.sum(head_grad.astype(full), axis=0)
    normed_grad = product_right(head_grad, head_w)
    factor_one = lax.rsqrt(jnp.mean(flat * flat, axis=-1, keepdims=True) + epsilon)
    input_norm_grad, gain_one_grad = norm_back(flat, factor_one, gain_one, normed_grad)
    input_grad = (resid_grad + input_norm_grad).astype(low).reshape(slot_count, rows, width)

    edges = [0, share, share + bias_q]
    edges += [edges[-1] + bias_k, edges[-1] + 2 * bias_k]

    def parts(vector):
        return vector.reshape(wt_count, -1)

    small_grad = jnp.concatenate(
        [
            parts(gain_one_grad),
            parts(head_b_grad[:query_width]),
            parts(head_b_grad[query_width : query_width + pair_width]),
            parts(head_b_grad[query_width + pair_width :]),
            parts(gain_two_grad),
        ],
        axis=1,
    ).astype(low)
    small_grad = jnp.pad(small_grad, ((0, 0), (0, 256 * seq_count - small_grad.shape[1])))
    small_grad = jnp.pad(small_grad[:, None, :], ((0, 0), (0, 15), (0, 0)))

    def by_owner(partial):
        return partial.reshape(outer, INNER, -1, partial.shape[-1])

    out_w_out, heads_out, small_out = reduce_shares(
        by_owner(out_w_grad),
        by_owner(head_w_grad),
        by_owner(small_grad),
    )
    small_out = small_out[0]
    gate_out, up_out = join_units(info, jnp.stack(units_got), outer, ff_own)
    return (
        layer_out,
        input_grad,
        small_out[: edges[1]],
        heads_out[:, :query_width],
        small_out[edges[1] : edges[2]],
        heads_out[:, query_width : query_width + pair_width],
        small_out[edges[2] : edges[3]],
        heads_out[:, query_width + pair_width :],
        small_out[edges[3] : edges[4]],
        out_w_out,
        small_out[edges[4] : edges[4] + ffn_gain.shape[0]],
        gate_out,
        up_out,
        down_out,
    )


def solution(mesh):
    by_wt = P("wt")
    by_row = P("wt", None)
    by_token = P("wt", "seq", None)
    return jax.shard_map(
        body,
        mesh=mesh,
        in_specs=(
            by_token, by_wt, by_wt, by_row, by_wt, by_row, by_wt, by_row, by_wt, by_row,
            by_wt, by_row, by_row, by_row, by_token,
        ),
        out_specs=(
            by_token, by_token, by_wt, by_row, by_wt, by_row, by_wt, by_row, by_wt, by_row,
            by_wt, by_row, by_row, by_row,
        ),
        check_vma=False,
    )
```
